32 devices in a mesh: blocks: 8 (over z, x), gz: 4 (over y, core).
Axes of the slice: x: 2, y: 2, z: 4, core: 2. Of those that a mesh axis runs over, the one named last changes fastest.
Arguments:
- coarse_field: float32 [4, 128, 3, 4096], P('gz', 'blocks'), may hold values from -6 to 6
- coarse_velocity: float32 [4, 128, 3, 4096], P('gz', 'blocks'), may hold values from -15 to 15
- fine_field: float32 [4, 96, 3, 4096], P('gz', 'blocks'), may hold values from -6 to 6
- fine_velocity: float32 [4, 96, 3, 4096], P('gz', 'blocks'), may hold values from -15 to 15
- pairs: int32 [4, 32, 6], P('gz', 'blocks'), may hold values from 0 to 15, as said below
Outputs:
- coarse_new: float32 [4, 128, 3, 4096], P('gz', 'blocks')
- fine_new: float32 [4, 96, 3, 4096], P('gz', 'blocks')
- face_jump: float32 [4, 32, 256], P('gz', 'blocks')
The draws below stay inside these ranges and needn't reach their ends.
Inputs may be any that keep to these rules, and one draw needn't show every extreme that they name: `pairs`: Columns: fine slot below 12, face axis 0 to 2, owner device below 8, coarse slot below 16, quadrant row and column 0 or 1. No two rows of a device name the same fine slot and face axis, and no two rows of a group name the same coarse block, face axis and quadrant. The rows of one device name one owner device at most 2 times, and exactly 2 times for some owner; rows of one device that name the same owner differ in face axis; some owner is named 2 times by every device of its group. Each face axis stands in 1 to 2 of a device's rows.
All inputs are finite; a program needn't handle non-finite values.
Results may differ from the reference program's by a relative error of at most 0.0003.
Values sent between devices are 32-bit elements; how exact they have to be, the bound alone decides.
A program may use at most 256 MiB of HBM per device.

```python
import jax
import jax.numpy as jnp
from jax import lax

EDGE = 16
HALF = 8
CB = 16
FB = 12
PAIRS_DEV = 4
COARSE_ALL = 128
FINE_ALL = 96
N_BLOCKS = 8
N_GZ = 4


def velocity_law(key, count):
    shape = (N_GZ, count * N_BLOCKS, 3, EDGE ** 3)
    group = jnp.arange(N_GZ)[:, None]
    device = jnp.arange(count * N_BLOCKS)[None, :] // count
    position = (device * N_GZ + group).astype(jnp.float32)
    scale = 1.0 + 2.0 * position / max(N_BLOCKS * N_GZ - 1, 1)
    first = jax.random.fold_in(key, 0)
    base = jax.random.truncated_normal(first, -5.0, 5.0, shape, jnp.float32)
    return (base * scale[:, :, None, None]).astype(jnp.float32)


def draw_coarse_velocity(key, part):
    return velocity_law(jax.random.fold_in(key, 3), CB)


def draw_fine_velocity(key, part):
    return velocity_law(jax.random.fold_in(key, 5), FB)


def source_rows(source_key, forced):
    first, second, third, fourth = jax.random.split(source_key, 4)
    order = jax.random.permutation(first, N_BLOCKS)
    spot = jnp.sum(jnp.arange(N_BLOCKS) * (order == forced).astype(jnp.int32))
    swapped = order.at[spot].set(order[0]).at[0].set(forced)
    doubles = jax.random.randint(second, (), 1, PAIRS_DEV // 2 + 1)
    rotate = jax.random.randint(third, (), 0, 3)
    place = jnp.arange(N_BLOCKS)
    counts = jnp.where(place < doubles, 2, jnp.where(place < PAIRS_DEV - doubles, 1, 0))
    starts = jnp.cumsum(counts) - counts
    rank = jnp.arange(PAIRS_DEV)
    link = jnp.sum((starts[None, :] <= rank[:, None]).astype(jnp.int32), axis=1) - 1
    owner = swapped[link]
    face = (rank + rotate) % 3
    within = rank // 3
    slot_tables = jax.vmap(lambda sub: jax.random.permutation(sub, FB))(jax.random.split(fourth, 3))
    fine_slot = slot_tables[face, within]
    return (owner.astype(jnp.int32), face.astype(jnp.int32), fine_slot.astype(jnp.int32))


def one_group(group_key):
    first, second, third, fourth = jax.random.split(group_key, 4)
    forced = jax.random.randint(first, (), 0, N_BLOCKS)
    owner, face, fine_slot = jax.vmap(lambda sub: source_rows(sub, forced))(jax.random.split(second, N_BLOCKS))
    target = owner * 3 + face
    hits = jnp.sum((target[:, :, None] == jnp.arange(N_BLOCKS * 3)[None, None, :]).astype(jnp.int32), axis=1)
    before = jnp.cumsum(hits, axis=0) - hits
    index = jnp.take_along_axis(before, target, axis=1)
    key_tables = jax.vmap(lambda sub: jax.random.permutation(sub, 4 * CB))(jax.random.split(third, N_BLOCKS * 3))
    value = key_tables[target, index]
    columns = jnp.stack([fine_slot, face, owner, value // 4, value // 2 % 2, value % 2], axis=-1)
    orders = jax.vmap(lambda sub: jax.random.permutation(sub, PAIRS_DEV))(jax.random.split(fourth, N_BLOCKS))
    shuffled = jnp.take_along_axis(columns, orders[:, :, None], axis=1)
    return shuffled.reshape(N_BLOCKS * PAIRS_DEV, 6).astype(jnp.int32)


def draw_pairs(key, part):
    base = jax.random.fold_in(key, 11)
    group_keys = jax.vmap(lambda index: jax.random.fold_in(base, index))(jnp.arange(N_GZ))
    return jax.vmap(one_group)(group_keys)


def block_scale(rng, dims, shards, smallest, top_value):
    level, own = 1.0, jax.random.fold_in(rng, 6)
    for dim, parts in shards:
        heights = jnp.exp(jax.random.uniform(jax.random.fold_in(own, dim), (parts,), jnp.float32, smallest / len(shards), top_value / len(shards)))
        level = level * jnp.repeat(heights, dims[dim] // parts).reshape([-1 if axis == dim else 1 for axis in range(len(dims))])
    return level


def gaussian(rng, extent, deviation, reach, shards=(), kind=jnp.bfloat16):
    result = jax.random.normal(rng, extent, jnp.float32) * deviation
    if len(shards) > 0:
        result = block_scale(rng, extent, shards, -0.22, 0.18) * result
    return jnp.clip(result, min=-reach, max=reach).astype(kind)


def setup_inputs(seed: int = 0) -> dict:
    seeds = jax.random.split(jax.random.key(seed), 6)
    coarse_field = gaussian(seeds[0], (N_GZ, COARSE_ALL, 3, EDGE ** 3), 1.0, 6.0, ((0, 4), (1, 8)), jnp.float32)
    coarse_velocity = draw_coarse_velocity(jax.random.fold_in(seeds[5], 71), 0)
    fine_field = gaussian(seeds[2], (N_GZ, FINE_ALL, 3, EDGE ** 3), 1.0, 6.0, ((0, 4), (1, 8)), jnp.float32)
    fine_velocity = draw_fine_velocity(jax.random.fold_in(seeds[5], 71), 0)
    pairs = draw_pairs(jax.random.fold_in(seeds[5], 71), 0)
    return dict(coarse_field=coarse_field, coarse_velocity=coarse_velocity, fine_field=fine_field, fine_velocity=fine_velocity, pairs=pairs)


TANGENT = ((1, 2), (0, 2), (0, 1))

def cube(values):
    return values.reshape(values.shape[:-1] + (EDGE, EDGE, EDGE))

def centred(field):
    return [0.5 * (field[along] + jnp.roll(field[along], -1, axis=along)) for along in range(3)]

def cell_speed(field, velocity):
    centre = centred(field)
    speed_v = jnp.sqrt(velocity[0] * velocity[0] + velocity[1] * velocity[1] + velocity[2] * velocity[2])
    speed_b = jnp.sqrt(centre[0] * centre[0] + centre[1] * centre[1] + centre[2] * centre[2])
    return jnp.max(speed_v + speed_b)

def edge_fields(field, velocity):
    field_x, field_y, field_z = centred(field)
    vel_x, vel_y, vel_z = (velocity[0], velocity[1], velocity[2])
    cell_x = -(vel_y * field_z - vel_z * field_y)
    cell_y = -(vel_z * field_x - vel_x * field_z)
    cell_z = -(vel_x * field_y - vel_y * field_x)

    def corner(values, first, second):
        rolled = jnp.roll(values, 1, axis=first)
        return 0.25 * (values + rolled + jnp.roll(values, 1, axis=second) + jnp.roll(rolled, 1, axis=second))
    return [corner(cell_x, 1, 2), corner(cell_y, 0, 2), corner(cell_z, 0, 1)]

def faraday(field, emf, factor):

    def ahead(values, along):
        return jnp.roll(values, -1, axis=along) - values
    emf_x, emf_y, emf_z = emf
    new_x = field[0] - factor * (ahead(emf_z, 1) - ahead(emf_y, 2))
    new_y = field[1] - factor * (ahead(emf_x, 2) - ahead(emf_z, 0))
    new_z = field[2] - factor * (ahead(emf_y, 0) - ahead(emf_x, 1))
    return jnp.stack([new_x, new_y, new_z])

def put_plane(values, normal, plane_new):
    shape = [1, 1, 1]
    shape[normal] = EDGE
    first = (jnp.arange(EDGE) == 0).reshape(shape)
    return jnp.where(first, jnp.expand_dims(plane_new, normal), values)

def restrict(planes):
    first = 0.5 * (planes[:, 0, 0::2, 0::2] + planes[:, 0, 1::2, 0::2])
    second = 0.5 * (planes[:, 1, 0::2, 0::2] + planes[:, 1, 0::2, 1::2])
    return jnp.stack([first, second], axis=1)

def reference(coarse_field, coarse_velocity, fine_field, fine_velocity, pairs):
    coarse_flat = coarse_field.reshape(-1, 3, EDGE ** 3)
    coarse_vel = coarse_velocity.reshape(-1, 3, EDGE ** 3)
    fine_flat = fine_field.reshape(-1, 3, EDGE ** 3)
    fine_vel = fine_velocity.reshape(-1, 3, EDGE ** 3)
    speeds_c = lax.map(lambda item: cell_speed(cube(item[0]), cube(item[1])), (coarse_flat, coarse_vel))
    speeds_f = lax.map(lambda item: cell_speed(cube(item[0]), cube(item[1])), (fine_flat, fine_vel))
    top_speed = jnp.maximum(jnp.max(speeds_c), jnp.max(speeds_f))
    time_step = 0.2 / top_speed

    def fine_step(item):
        field = cube(item[0])
        emf = edge_fields(field, cube(item[1]))
        updated = faraday(field, emf, time_step / 0.5)
        tangents = jnp.stack([jnp.stack([jnp.take(emf[TANGENT[normal][0]], 0, axis=normal), jnp.take(emf[TANGENT[normal][1]], 0, axis=normal)]) for normal in range(3)])
        normals = jnp.stack([jnp.take(updated[normal], 0, axis=normal) for normal in range(3)])
        return (updated.reshape(3, EDGE ** 3), tangents, normals)
    fine_out, fine_tangents, fine_normals = lax.map(fine_step, (fine_flat, fine_vel))
    pair_rows = pairs.reshape(-1, 6).astype(jnp.int32)
    count = pair_rows.shape[0]
    group = (jnp.arange(count, dtype=jnp.int32) // (PAIRS_DEV * N_BLOCKS)).astype(jnp.int32)
    source = (jnp.arange(count, dtype=jnp.int32) % (PAIRS_DEV * N_BLOCKS) // PAIRS_DEV).astype(jnp.int32)
    fine_block = (group * (FB * N_BLOCKS) + source * FB + pair_rows[:, 0]).astype(jnp.int32)
    face_dir = pair_rows[:, 1]
    coarse_block = (group * (CB * N_BLOCKS) + pair_rows[:, 2] * CB + pair_rows[:, 3]).astype(jnp.int32)
    quad_row = pair_rows[:, 4]
    quad_col = pair_rows[:, 5]
    restricted = restrict(fine_tangents[fine_block, face_dir])
    span = jnp.arange(HALF, dtype=jnp.int32)
    rows_idx = (quad_row[:, None, None, None] * HALF + span[None, None, :, None]).astype(jnp.int32)
    cols_idx = (quad_col[:, None, None, None] * HALF + span[None, None, None, :]).astype(jnp.int32)
    comp_idx = jnp.arange(2, dtype=jnp.int32)[None, :, None, None]
    blocks_all = coarse_flat.shape[0]
    replaced = jnp.zeros((blocks_all, 3, 2, EDGE, EDGE), jnp.float32)
    replaced = replaced.at[coarse_block[:, None, None, None], face_dir[:, None, None, None], comp_idx, rows_idx, cols_idx].set(restricted)
    hit_mask = jnp.zeros((blocks_all, 3, EDGE, EDGE), jnp.float32)
    hit_mask = hit_mask.at[coarse_block[:, None, None], face_dir[:, None, None], rows_idx[:, 0], cols_idx[:, 0]].set(jnp.ones((count, HALF, HALF), jnp.float32))

    def coarse_step(item):
        field = cube(item[0])
        emf = edge_fields(field, cube(item[1]))
        for normal in range(3):
            for which in range(2):
                along = TANGENT[normal][which]
                plane_now = jnp.take(emf[along], 0, axis=normal)
                plane_new = jnp.where(item[3][normal] > 0.5, item[2][normal, which], plane_now)
                emf[along] = put_plane(emf[along], normal, plane_new)
        updated = faraday(field, emf, time_step / 1.0)
        normals = jnp.stack([jnp.take(updated[normal], 0, axis=normal) for normal in range(3)])
        return (updated.reshape(3, EDGE ** 3), normals)
    coarse_out, coarse_normals = lax.map(coarse_step, (coarse_flat, coarse_vel, replaced, hit_mask))
    quadrant = coarse_normals[coarse_block[:, None, None], face_dir[:, None, None], rows_idx[:, 0], cols_idx[:, 0]]
    prolonged = jnp.repeat(jnp.repeat(quadrant, 2, axis=1), 2, axis=2)
    face_jump = fine_normals[fine_block, face_dir] - prolonged
    return (coarse_out.reshape(coarse_field.shape), fine_out.reshape(fine_field.shape), face_jump.reshape(N_GZ, PAIRS_DEV * N_BLOCKS, EDGE * EDGE))
```

```python
import functools

import jax
import jax.numpy as jnp
from jax import lax
from jax.experimental import pallas as pl
from jax.experimental.pallas import tpu as pltpu
from jax.sharding import PartitionSpec as P

EDGE = 16
HALF = 8
CAP = 2
LANES = 128
ROWS = 8
TILES = EDGE**3 // LANES
SPAN = 3 * TILES
TINY = 1.2e-38
BIG = 1e30
EMPTY = 3e38
TANGENT = ((1, 2), (0, 2), (0, 1))
MESH = pl.DeviceIdType.MESH
COARSE_STEP = 8
FINE_STEP = 4


def take(values, index):
    return jnp.take_along_axis(values, index, axis=1, mode="promise_in_bounds")


def largest_step(count, most):
    return max(n for n in range(1, most + 1) if count % n == 0)


def kernel(
    peers,
    groups,
    coarse_count,
    fine_count,
    pair_count,
    pairs_hbm,
    cb_hbm,
    cv_hbm,
    fb_hbm,
    fv_hbm,
    cb,
    curl_c,
    fb,
    curl_f,
    jump_a,
    jump_b,
    step_out,
    pairs,
    cv,
    fv,
    emf_c,
    emf_p,
    plane_e,
    plane_b,
    plane_n,
    held_ref,
    own_a,
    own_b,
    picked,
    rows1,
    send1,
    recv1,
    send2,
    recv2,
    gmax,
    gmax_in,
    load_sem,
    s1_sem,
    r1_sem,
    s2_sem,
    r2_sem,
    sg_sem,
    rg_sem,
):
    me = lax.axis_index("blocks")
    mg = lax.axis_index("gz")
    few = peers <= 8
    coarse_groups = coarse_count // ROWS
    pair_rows = ROWS * -(-pair_count // ROWS)

    def each_peer(body):
        lax.fori_loop(1, peers, lambda k, _: (body(lax.rem(me + k, peers)), 0)[1], 0, unroll=few)

    def each_group(body):
        for k in range(1, groups):
            body(lax.rem(mg + k, groups))

    barrier = pltpu.get_barrier_semaphore()
    each_peer(
        lambda p: pl.semaphore_signal(barrier, inc=1, device_id=(p, mg), device_id_type=MESH)
    )
    loads = [
        pltpu.make_async_copy(src, dst, load_sem.at[n])
        for n, (src, dst) in enumerate(((fb_hbm, fb), (fv_hbm, fv), (cb_hbm, cb), (cv_hbm, cv)))
    ]
    listed = pltpu.make_async_copy(pairs_hbm, pairs, load_sem.at[4])
    listed.start()
    for load in loads:
        load.start()
    each_group(
        lambda g: pl.semaphore_signal(barrier, inc=1, device_id=(me, g), device_id_type=MESH)
    )

    lane = lax.broadcasted_iota(jnp.int32, (ROWS, LANES), 1)
    sub = lax.broadcasted_iota(jnp.int32, (ROWS, LANES), 0)
    zero = jnp.zeros((ROWS, LANES), jnp.float32)
    row16 = lane // EDGE
    k_of = lane % EDGE
    k8 = lane % HALF
    first_y = lane < EDGE
    last_y = lane >= LANES - EDGE
    first_z = k_of == 0
    last_z = k_of == EDGE - 1
    first_x = sub == 0
    last_x = sub == ROWS - 1

    def roll(v, shift):
        return v if shift % LANES == 0 else pltpu.roll(v, shift % LANES, 1)

    def back_y(pair):
        low, high = roll(pair[0], EDGE), roll(pair[1], EDGE)
        return jnp.where(first_y, high, low), jnp.where(first_y, low, high)

    def ahead_y(pair):
        low, high = roll(pair[0], -EDGE), roll(pair[1], -EDGE)
        return jnp.where(last_y, high, low), jnp.where(last_y, low, high)

    def back_z(pair):
        return tuple(jnp.where(first_z, roll(v, 1 - EDGE), roll(v, 1)) for v in pair)

    def ahead_z(pair):
        return tuple(jnp.where(last_z, roll(v, EDGE - 1), roll(v, -1)) for v in pair)

    def add(a, b):
        return tuple(x + y for x, y in zip(a, b))

    def sub2(a, b):
        return tuple(x - y for x, y in zip(a, b))

    def mul(a, b):
        return tuple(x * y for x, y in zip(a, b))

    def quad(f):
        return lambda q: f(q[:2]) + f(q[2:])

    def back_x(q):
        r = [pltpu.roll(v, 1, 0) for v in q]
        return tuple(jnp.where(first_x, r[n ^ 2], r[n]) for n in range(4))

    def ahead_x(q):
        r = [pltpu.roll(v, ROWS - 1, 0) for v in q]
        return tuple(jnp.where(last_x, r[n ^ 2], r[n]) for n in range(4))

    def top_of(v, c):
        out = []
        for n in range(len(v[0])):
            vv = (v[0][n] * v[0][n] + v[1][n] * v[1][n]) + v[2][n] * v[2][n]
            cc = (c[0][n] * c[0][n] + c[1][n] * c[1][n]) + c[2][n] * c[2][n]
            root_v = vv * lax.rsqrt(jnp.maximum(vv, TINY))
            root_c = cc * lax.rsqrt(jnp.maximum(cc, TINY))
            out.append(root_v + 0.5 * root_c)
        return functools.reduce(jnp.maximum, out)

    def cells(v, c):
        return (
            sub2(mul(v[2], c[1]), mul(v[1], c[2])),
            sub2(mul(v[0], c[2]), mul(v[2], c[0])),
            sub2(mul(v[1], c[0]), mul(v[0], c[1])),
        )

    def fine_read(ref, base):
        return tuple(
            tuple(
                ref[pl.ds(base + c * TILES + 2 * HALF * ih + h, ROWS, stride=2), :]
                for ih in range(2)
                for h in range(2)
            )
            for c in range(3)
        )

    def fine_put(ref, base, values):
        for c in range(3):
            for ih in range(2):
                for h in range(2):
                    ref[pl.ds(base + c * TILES + 2 * HALF * ih + h, ROWS, stride=2), :] = values[c][
                        2 * ih + h
                    ]

    def fine_edges(b, v):
        c = (add(b[0], ahead_x(b[0])), add(b[1], quad(ahead_y)(b[1])), add(b[2], quad(ahead_z)(b[2])))
        cell = cells(v, c)
        part_x = add(cell[0], quad(back_y)(cell[0]))
        part_y = add(cell[1], quad(back_z)(cell[1]))
        part_z = add(cell[2], quad(back_y)(cell[2]))
        e = (
            add(part_x, quad(back_z)(part_x)),
            add(part_y, back_x(part_y)),
            add(part_z, back_x(part_z)),
        )
        return e, c

    def fine_curl(e):
        return (
            sub2(sub2(quad(ahead_y)(e[2]), e[2]), sub2(quad(ahead_z)(e[1]), e[1])),
            sub2(sub2(quad(ahead_z)(e[0]), e[0]), sub2(ahead_x(e[2]), e[2])),
            sub2(sub2(ahead_x(e[1]), e[1]), sub2(quad(ahead_y)(e[0]), e[0])),
        )

    def by_axis(d, values):
        return jnp.where(d == 0, values[0], jnp.where(d == 1, values[1], values[2]))

    def sum_rows(v):
        return jnp.sum(v, axis=0, keepdims=True)

    listed.wait()
    loads[0].wait()
    loads[1].wait()

    half_lane = 32 * (row16 % 4)
    index_r = (half_lane + 2 * k8, 2 * k8, half_lane)
    target_r = (jnp.zeros_like(lane), row16, k8)

    def pair_edges(r):
        base = pairs[r, 0] * SPAN
        fine_put(emf_p, r * SPAN, fine_edges(fine_read(fb, base), fine_read(fv, base))[0])

    def pair_restrict(r):
        d = pairs[r, 1]
        index, target = by_axis(d, index_r), by_axis(d, target_r)
        upper = lane >= jnp.where(d == 1, LANES, 64)
        for which in range(2):
            axis = jnp.where(d == 0, 1, 0) if which == 0 else jnp.where(d == 2, 1, 2)
            base = r * SPAN + axis * TILES
            got = []
            for h in range(2):
                here = emf_p[pl.ds(base + h, ROWS, stride=4), :]
                if which == 0:
                    there = jnp.where(
                        d == 0, roll(here, -EDGE), emf_p[pl.ds(base + h + 2, ROWS, stride=4), :]
                    )
                else:
                    there = jnp.where(d == 2, roll(here, -EDGE), roll(here, -1))
                got.append(take(0.5 * (here + there), index))
            value = jnp.where(upper, got[1], got[0])
            rows1[pl.ds(4 * r + which, 1), :] = sum_rows(jnp.where(sub == target, value, 0.0))
        code = (pairs[r, 3] * 6 + d * 2 + pairs[r, 4]).astype(jnp.float32)
        key = jnp.where((lane[:1] // HALF) % 2 == pairs[r, 5], code, -1.0)
        rows1[pl.ds(4 * r + 2, 1), :] = key

    def each_pair(body):
        if pair_count <= 4:
            for r in range(pair_count):
                body(r)
        else:
            lax.fori_loop(0, pair_count, lambda r, _: (body(r), 0)[1], 0)

    each_pair(pair_edges)
    each_pair(pair_restrict)

    slot_of = [pairs[r, 0] for r in range(pair_count)]
    face_of = [pairs[r, 1] for r in range(pair_count)]
    owner_of = [pairs[r, 2] for r in range(pair_count)]
    rank_of = []
    for r in range(pair_count):
        rank = jnp.int32(0)
        for q in range(r):
            rank = rank + jnp.where(owner_of[q] == owner_of[r], 1, 0)
        rank_of.append(rank)

    def build(p, carry):
        message = jnp.full((ROWS, LANES), -1.0, jnp.float32)
        for r in range(pair_count):
            here = jnp.where(owner_of[r] == p, rank_of[r], ROWS)
            for n, row in enumerate((2 * here, 2 * here + 1, 2 * CAP + here)):
                message = jnp.where(
                    sub == row, jnp.broadcast_to(rows1[4 * r + n : 4 * r + n + 1, :], (ROWS, LANES)), message
                )
        slot(send1, p)[...] = message
        return carry

    def slot(ref, p):
        return ref.at[pl.ds(pl.multiple_of(p * ROWS, ROWS), ROWS)]

    lax.fori_loop(0, peers, build, 0, unroll=few)

    pl.semaphore_wait(barrier, peers - 1 + groups - 1)

    def out1(p):
        return pltpu.make_async_remote_copy(
            src_ref=slot(send1, p), dst_ref=slot(recv1, me), send_sem=s1_sem,
            recv_sem=r1_sem, device_id=(p, mg), device_id_type=MESH,
        )

    def out2(p):
        return pltpu.make_async_remote_copy(
            src_ref=slot(send2, p), dst_ref=slot(recv2, me), send_sem=s2_sem,
            recv_sem=r2_sem, device_id=(p, mg), device_id_type=MESH,
        )

    def outg(g):
        return pltpu.make_async_remote_copy(
            src_ref=gmax, dst_ref=slot(gmax_in, mg), send_sem=sg_sem,
            recv_sem=rg_sem, device_id=(me, g), device_id_type=MESH,
        )

    def drain(ref, sem, count):
        part = ref.at[pl.ds(0, ROWS * count)]
        pltpu.make_async_copy(part, part, sem).wait()

    each_peer(lambda p: out1(p).start())

    loads[2].wait()
    loads[3].wait()

    def column(tile):
        return pl.ds(pl.multiple_of(tile * LANES, LANES), LANES)

    def blocked(ref, g):
        def read(c, i):
            return tuple(ref[c, ROWS * g : ROWS * g + ROWS, column(2 * i + h)] for h in range(2))

        return read

    def blocked_put(ref, g):
        def put(c, i, pair):
            for h in range(2):
                ref[c, ROWS * g : ROWS * g + ROWS, column(2 * i + h)] = pair[h]

        return put


    def coarse_step(n, carry):
        parts, best = carry
        parts = list(parts)
        for u in range(COARSE_STEP):
            i = n * COARSE_STEP + u
            after = lax.rem(i + 1, EDGE)
            for g in range(coarse_groups):
                field, velocity, put = blocked(cb, g), blocked(cv, g), blocked_put(emf_c, g)
                b = [field(c, i) for c in range(3)]
                v = [velocity(c, i) for c in range(3)]
                c = (add(b[0], field(0, after)), add(b[1], ahead_y(b[1])), add(b[2], ahead_z(b[2])))
                cell = cells(v, c)
                part_x = add(cell[0], back_y(cell[0]))
                part_y = add(cell[1], back_z(cell[1]))
                part_z = add(cell[2], back_y(cell[2]))
                put(0, i, add(part_x, back_z(part_x)))
                put(1, i, add(part_y, parts[g][0]))
                put(2, i, add(part_z, parts[g][1]))
                parts[g] = (part_y, part_z)
                best = jnp.maximum(best, top_of(v, c))
        return tuple(parts), best

    nothing = ((zero, zero), (zero, zero))
    parts, best = lax.fori_loop(
        0, EDGE // COARSE_STEP, coarse_step, ((nothing,) * coarse_groups, zero)
    )
    for g in range(coarse_groups):
        read, put = blocked(emf_c, g), blocked_put(emf_c, g)
        for c in range(2):
            put(1 + c, 0, add(read(1 + c, 0), parts[g][c]))

    fine_step = largest_step(fine_count, FINE_STEP)

    def fine_bulk(n, best):
        for u in range(fine_step):
            base = (n * fine_step + u) * SPAN
            b, v = fine_read(fb, base), fine_read(fv, base)
            e, c = fine_edges(b, v)
            fine_put(curl_f, base, fine_curl(e))
            best = jnp.maximum(best, top_of(v, c))
        return best

    best = lax.fori_loop(0, fine_count // fine_step, fine_bulk, best)
    gmax[...] = best
    each_group(lambda g: outg(g).start())


    def packed(read, c, d, q1):
        if d == 0:
            return read(c, 0)[q1]
        out = zero
        for m in range(HALF):
            tiles = read(c, q1 * HALF + m)
            if d == 1:
                out = jnp.where(row16 == m, roll(tiles[0], EDGE * m), out)
            else:
                for q2 in range(2):
                    out = jnp.where(k_of == HALF * q2 + m, roll(tiles[q2], HALF * q2 + m), out)
        return out

    def plane_slot(n, g):
        at = (n * coarse_groups + g) * ROWS
        return slice(at, at + ROWS)

    for g in range(coarse_groups):
        for d in range(3):
            for q1 in range(2):
                plane_b[plane_slot(2 * d + q1, g), :] = packed(blocked(cb, g), d, d, q1)
                for which in range(2):
                    plane_e[plane_slot(4 * d + 2 * which + q1, g), :] = packed(
                        blocked(emf_c, g), TANGENT[d][which], d, q1
                    )

    def row_of(ref, n):
        return jnp.broadcast_to(ref[pl.ds(n, 1), :], (ROWS, LANES))

    slot(recv1, me)[...] = slot(send1, me)[...]
    drain(recv1, r1_sem, peers - 1)

    base_code = [((sub + ROWS * g) * 6).astype(jnp.float32) for g in range(coarse_groups)]
    empty = jnp.full((ROWS, LANES), EMPTY, jnp.float32)
    for g in range(coarse_groups):

        def collect(p, held, g=g):
            for c in range(CAP):
                code = row_of(recv1, p * ROWS + 2 * CAP + c) - base_code[g]
                values = [row_of(recv1, p * ROWS + 2 * c + which) for which in range(2)]
                held = [
                    jnp.where(code == float(2 * (n // 4) + n % 2), values[n // 2 % 2], held[n])
                    for n in range(12)
                ]
            return held

        held = lax.fori_loop(0, peers, collect, [empty] * 12, unroll=few)
        for n in range(12):
            held_ref[plane_slot(n, g), :] = held[n]

    spread = row16
    squeeze = EDGE * k8

    def ahead_i(pair):
        turned = [roll(v, -1) for v in pair]
        wrapped = [roll(v, HALF - 1) for v in pair]
        return tuple(jnp.where(k8 == HALF - 1, wrapped[1 - q], turned[q]) for q in range(2))

    def ahead_j(pair):
        return tuple(
            jnp.where(
                last_y,
                jnp.where(k_of < HALF, roll(v, LANES - EDGE - HALF), roll(v, LANES - HALF)),
                roll(v, -EDGE),
            )
            for v in pair
        )

    for g in range(coarse_groups):
        hold = [held_ref[plane_slot(n, g), :] for n in range(12)]
        sent = [[(hold[4 * d + 2 * w], hold[4 * d + 2 * w + 1]) for w in range(2)] for d in range(3)]
        now = [
            [
                [
                    jnp.where(
                        sent[d][w][q] < BIG, sent[d][w][q], plane_e[plane_slot(4 * d + 2 * w + q, g), :]
                    )
                    for q in range(2)
                ]
                for w in range(2)
            ]
            for d in range(3)
        ]
        for q in range(2):
            over = take(sent[2][0][q], spread)
            now[1][0][q] = jnp.where((over < BIG) & first_z, over, now[1][0][q])
            under = take(sent[1][0][q], squeeze)
            free = (sent[2][0][q] >= BIG) & (lane < HALF) & (under < BIG)
            now[2][0][q] = jnp.where(free, under, now[2][0][q])
            over = roll(sent[2][1][0], -HALF * q)
            now[0][0][q] = jnp.where((over < BIG) & first_z, over, now[0][0][q])
            under = roll(sent[0][0][q], HALF * q)
            free = (sent[2][1][0] >= BIG) & (k_of == HALF * q) & (under < BIG)
            now[2][1][0] = jnp.where(free, under, now[2][1][0])
        over, under = sent[1][1][0], sent[0][1][0]
        now[0][1][0] = jnp.where((over < BIG) & first_y, over, now[0][1][0])
        now[1][1][0] = jnp.where((over >= BIG) & first_y & (under < BIG), under, now[1][1][0])
        for d in range(3):
            one, two = now[d]
            if d < 2:
                ahead_one, ahead_two = ahead_y(two), ahead_z(one)
            else:
                ahead_one, ahead_two = ahead_i(two), ahead_j(one)
            left, right = sub2(ahead_one, two), sub2(ahead_two, one)
            curl = sub2(right, left) if d == 1 else sub2(left, right)
            for q in range(2):
                plane_n[plane_slot(2 * d + q, g), :] = curl[q]

    drain(gmax_in, rg_sem, groups - 1)
    for k in range(1, groups):
        best = jnp.maximum(best, slot(gmax_in, lax.rem(mg + k, groups))[...])
    top_row = jnp.broadcast_to(jnp.max(best, axis=0, keepdims=True), (ROWS, LANES))

    def answer(p, carry):
        rows = top_row
        for c in range(CAP):
            key = row_of(recv1, p * ROWS + 2 * CAP + c)
            curl_acc, field_acc = zero, zero
            for g in range(coarse_groups):
                code = key - base_code[g]
                for n in range(6):
                    hit = code == float(n)
                    curl_acc = jnp.where(hit, plane_n[plane_slot(n, g), :], curl_acc)
                    field_acc = jnp.where(hit, plane_b[plane_slot(n, g), :], field_acc)
            rows = jnp.where(sub == c, sum_rows(curl_acc), rows)
            rows = jnp.where(sub == CAP + c, sum_rows(field_acc), rows)
        slot(send2, p)[...] = rows
        return carry

    lax.fori_loop(0, peers, answer, 0, unroll=few)
    each_peer(lambda p: out2(p).start())

    for g in range(coarse_groups):
        for d in range(3):
            for which in range(2):
                axis = TANGENT[d][which]
                for q1 in range(2):
                    value = held_ref[plane_slot(4 * d + 2 * which + q1, g), :]

                    def patch(tile, shift, mask, value=value, axis=axis, g=g):
                        where = (axis, slice(ROWS * g, ROWS * g + ROWS), slice(tile * LANES, tile * LANES + LANES))
                        turned = roll(value, shift)
                        put = turned < BIG
                        if mask is not None:
                            put = put & mask
                        emf_c[where] = jnp.where(put, turned, emf_c[where])

                    if d == 0:
                        patch(q1, 0, None)
                        continue
                    for m in range(HALF):
                        tile = 2 * (q1 * HALF + m)
                        if d == 1:
                            patch(tile, -EDGE * m, first_y)
                        else:
                            for q2 in range(2):
                                patch(tile + q2, -(HALF * q2 + m), first_z)


    def curl_step(n, carry):
        for u in range(4):
            i = 4 * n + u
            after = lax.rem(i + 1, EDGE)
            for g in range(coarse_groups):
                read, put = blocked(emf_c, g), blocked_put(curl_c, g)
                e_x, e_y, e_z = read(0, i), read(1, i), read(2, i)
                put(0, i, sub2(sub2(ahead_y(e_z), e_z), sub2(ahead_z(e_y), e_y)))
                put(1, i, sub2(sub2(ahead_z(e_x), e_x), sub2(read(2, after), e_z)))
                put(2, i, sub2(sub2(read(1, after), e_y), sub2(ahead_y(e_x), e_x)))
        return carry

    lax.fori_loop(0, EDGE // 4, curl_step, 0)

    index_n = (lane, k_of, EDGE * k8)
    target_n = (jnp.zeros_like(lane), row16, row16)

    def pair_normal(r):
        d = pairs[r, 1]
        base = pairs[r, 0] * SPAN + d * TILES
        index, target = by_axis(d, index_n), by_axis(d, target_n)
        upper = k_of >= jnp.where(d == 2, HALF, EDGE)
        for n, ref in enumerate((fb, curl_f)):
            for h in range(2):
                start = base + jnp.where(d == 0, h, 2 * HALF * h)
                got = [take(ref[pl.ds(start + s, ROWS, stride=2), :], index) for s in range(2)]
                value = jnp.where(upper, got[1], got[0])
                picked[pl.ds((2 * n + h) * pair_rows + r, 1), :] = sum_rows(
                    jnp.where(sub == target, value, 0.0)
                )

    each_pair(pair_normal)

    slot(recv2, me)[...] = slot(send2, me)[...]
    drain(recv2, r2_sem, peers - 1)
    top = lax.fori_loop(
        0, peers, lambda p, t: jnp.maximum(t, row_of(recv2, p * ROWS + 2 * CAP)), zero, unroll=few
    )
    step_out[...] = jnp.broadcast_to(0.125 * (0.2 / jnp.max(top, axis=1, keepdims=True)), (ROWS, LANES))
    for r in range(pair_count):
        row = owner_of[r] * ROWS + rank_of[r]
        own_a[r : r + 1, :] = recv2[pl.ds(row, 1), :]
        own_b[r : r + 1, :] = recv2[pl.ds(row + CAP, 1), :]
    for s in range(0, pair_count, ROWS):
        turned, column_of = jnp.zeros_like(lane), jnp.zeros_like(lane)
        for r in range(s, min(s + ROWS, pair_count)):
            turned = jnp.where(sub == r - s, face_of[r], turned)
            column_of = jnp.where(sub == r - s, pairs[r, 5], column_of)
        for h in range(2):
            m, n = 4 * h + lane // 32, k_of // 2
            index = jnp.where(turned == 2, EDGE * n + m, EDGE * m + n) + HALF * column_of
            curl, field = take(own_a[s : s + ROWS, :], index), take(own_b[s : s + ROWS, :], index)
            side = slice(h * LANES, (h + 1) * LANES)
            fine = [picked[n * pair_rows + s : n * pair_rows + s + ROWS, :] for n in (h, 2 + h)]
            jump_a[s : s + ROWS, side] = fine[0] - field
            jump_b[s : s + ROWS, side] = 2.0 * fine[1] - curl
    drain(send1, s1_sem, peers - 1)
    drain(send2, s2_sem, peers - 1)
    drain(gmax_in, sg_sem, groups - 1)


def store(cb, curl_c, fb, curl_f, jump_a, jump_b, step, out_c, out_f, out_j, new_c, new_f, new_j, sems):
    by = step[0:1, 0:1]
    copies = []
    for c in range(3):
        new_c[c] = cb[c] - by * curl_c[c]
        copies.append(pltpu.make_async_copy(new_c.at[c], out_c.at[c], sems.at[len(copies)]))
        copies[-1].start()
    rows = fb.shape[0]
    for n in range(2):
        part = pl.ds(n * (rows // 2), rows // 2)
        new_f[part, :] = fb[part, :] - (2.0 * by) * curl_f[part, :]
        copies.append(pltpu.make_async_copy(new_f.at[part], out_f.at[part], sems.at[len(copies)]))
        copies[-1].start()
    count = out_j.shape[0]
    new_j[...] = (jump_a[...] - by * jump_b[...])[:count]
    copies.append(pltpu.make_async_copy(new_j, out_j, sems.at[len(copies)]))
    copies[-1].start()
    for copy in copies:
        copy.wait()


def on_device(peers, groups, coarse_field, coarse_velocity, fine_field, fine_velocity, pairs):
    coarse_count, fine_count = coarse_field.shape[1], fine_field.shape[1]
    pair_count = pairs.shape[1]
    cells = EDGE**3
    flat_rows = fine_count * SPAN

    def coarse_view(x):
        return jnp.transpose(x[0], (1, 0, 2))

    def fine_view(x):
        return x.reshape(flat_rows, LANES)

    pair_rows = ROWS * -(-pair_count // ROWS)
    operands = [
        pltpu.with_memory_space_constraint(x, pltpu.HBM)
        for x in (
            pairs[0],
            coarse_view(coarse_field),
            coarse_view(coarse_velocity),
            fine_view(fine_field),
            fine_view(fine_velocity),
        )
    ]
    f32 = jnp.float32
    dma = pltpu.SemaphoreType.DMA
    vmem = pltpu.VMEM
    anywhere = pl.BlockSpec(memory_space=pltpu.HBM)
    inside = pl.BlockSpec(memory_space=pltpu.VMEM)
    coarse_shape, fine_shape = (3, coarse_count, cells), (flat_rows, LANES)
    shapes = (
        coarse_shape,
        coarse_shape,
        fine_shape,
        fine_shape,
        (pair_rows, EDGE * EDGE),
        (pair_rows, EDGE * EDGE),
        (ROWS, LANES),
    )
    results = pl.pallas_call(
        functools.partial(kernel, peers, groups, coarse_count, fine_count, pair_count),
        out_shape=tuple(jax.ShapeDtypeStruct(s, f32) for s in shapes),
        in_specs=[anywhere] * 5,
        out_specs=(inside,) * len(shapes),
        scratch_shapes=[
            pltpu.SMEM(pairs.shape[1:], jnp.int32),
            vmem(coarse_shape, f32),
            vmem(fine_shape, f32),
            vmem(coarse_shape, f32),
            vmem((pair_count * SPAN, LANES), f32),
            vmem((12 * coarse_count, LANES), f32),
            vmem((6 * coarse_count, LANES), f32),
            vmem((6 * coarse_count, LANES), f32),
            vmem((12 * coarse_count, LANES), f32),
            vmem((pair_rows, LANES), f32),
            vmem((pair_rows, LANES), f32),
            vmem((4 * pair_rows, LANES), f32),
            vmem((4 * pair_rows, LANES), f32),
            vmem((peers * ROWS, LANES), f32),
            vmem((peers * ROWS, LANES), f32),
            vmem((peers * ROWS, LANES), f32),
            vmem((peers * ROWS, LANES), f32),
            vmem((ROWS, LANES), f32),
            vmem((groups * ROWS, LANES), f32),
            dma((5,)),
            dma,
            dma,
            dma,
            dma,
            dma,
            dma,
        ],
        compiler_params=pltpu.CompilerParams(
            collective_id=0, has_side_effects=True, vmem_limit_bytes=32 * 1024 * 1024
        ),
    )(*operands)
    coarse_out, fine_out, jump = pl.pallas_call(
        store,
        out_shape=(
            jax.ShapeDtypeStruct(coarse_shape, f32),
            jax.ShapeDtypeStruct(fine_shape, f32),
            jax.ShapeDtypeStruct((pair_count, EDGE * EDGE), f32),
        ),
        in_specs=[inside] * len(shapes),
        out_specs=(anywhere,) * 3,
        scratch_shapes=[
            vmem(coarse_shape, f32),
            vmem(fine_shape, f32),
            vmem((pair_count, EDGE * EDGE), f32),
            dma((6,)),
        ],
    )(*(pltpu.with_memory_space_constraint(x, pltpu.VMEM) for x in results))
    return (
        jnp.transpose(coarse_out, (1, 0, 2))[None],
        fine_out.reshape(1, fine_count, 3, cells),
        jump[None],
    )


def solution(mesh):
    spec = P("gz", "blocks", None, None)
    flat = P("gz", "blocks", None)
    return jax.shard_map(
        functools.partial(on_device, mesh.shape["blocks"], mesh.shape["gz"]),
        mesh=mesh,
        in_specs=(spec, spec, spec, spec, flat),
        out_specs=(spec, spec, flat),
        check_vma=False,
    )
```

```python
import functools

import jax
import jax.numpy as jnp
from jax import lax
from jax.experimental import pallas as pl
from jax.experimental.pallas import tpu as pltpu
from jax.sharding import PartitionSpec as P

EDGE = 16
HALF = 8
CAP = 2
LANES = 128
ROWS = 8
TILES = EDGE**3 // LANES
SPAN = 3 * TILES
TINY = 1.2e-38
BIG = 1e30
EMPTY = 3e38
TANGENT = ((1, 2), (0, 2), (0, 1))
MESH = pl.DeviceIdType.MESH
CHUNK = 4
CHUNKS = EDGE // CHUNK
FINE_STEP = 4
SPEED_STEP = 6


def take(values, index):
    return jnp.take_along_axis(values, index, axis=1, mode="promise_in_bounds")


def largest_step(count, most):
    return max(n for n in range(1, most + 1) if count % n == 0)


def kernel(
    peers,
    groups,
    coarse_count,
    fine_count,
    pair_count,
    pairs_hbm,
    cb_hbm,
    cv_hbm,
    fb_hbm,
    fv_hbm,
    cb,
    curl_c,
    fb,
    curl_f,
    jump_a,
    jump_b,
    step_out,
    pairs,
    cv,
    fv,
    emf_c,
    emf_p,
    centred,
    halfway,
    plane_e,
    plane_b,
    plane_n,
    held_ref,
    own_a,
    own_b,
    picked,
    rows1,
    send1,
    recv1,
    send2,
    recv2,
    gmax,
    gmax_in,
    load_sem,
    s1_sem,
    r1_sem,
    s2_sem,
    r2_sem,
    sg_sem,
    rg_sem,
):
    me = lax.axis_index("blocks")
    mg = lax.axis_index("gz")
    few = peers <= 8
    coarse_groups = coarse_count // ROWS
    pair_rows = ROWS * -(-pair_count // ROWS)

    def each_peer(body):
        lax.fori_loop(1, peers, lambda k, _: (body(lax.rem(me + k, peers)), 0)[1], 0, unroll=few)

    def each_group(body):
        for k in range(1, groups):
            body(lax.rem(mg + k, groups))

    barrier = pltpu.get_barrier_semaphore()
    each_peer(
        lambda p: pl.semaphore_signal(barrier, inc=1, device_id=(p, mg), device_id_type=MESH)
    )
    loads = [
        pltpu.make_async_copy(src, dst, load_sem.at[n])
        for n, (src, dst) in enumerate(((fb_hbm, fb), (fv_hbm, fv), (cb_hbm, cb), (cv_hbm, cv)))
    ]
    listed = pltpu.make_async_copy(pairs_hbm, pairs, load_sem.at[4])
    listed.start()
    for load in loads:
        load.start()
    each_group(
        lambda g: pl.semaphore_signal(barrier, inc=1, device_id=(me, g), device_id_type=MESH)
    )

    lane = lax.broadcasted_iota(jnp.int32, (ROWS, LANES), 1)
    sub = lax.broadcasted_iota(jnp.int32, (ROWS, LANES), 0)
    zero = jnp.zeros((ROWS, LANES), jnp.float32)
    row16 = lane // EDGE
    k_of = lane % EDGE
    k8 = lane % HALF
    first_y = lane < EDGE
    last_y = lane >= LANES - EDGE
    first_z = k_of == 0
    last_z = k_of == EDGE - 1
    first_x = sub == 0
    last_x = sub == ROWS - 1

    def roll(v, shift):
        return v if shift % LANES == 0 else pltpu.roll(v, shift % LANES, 1)

    def back_y(pair):
        low, high = roll(pair[0], EDGE), roll(pair[1], EDGE)
        return jnp.where(first_y, high, low), jnp.where(first_y, low, high)

    def ahead_y(pair):
        low, high = roll(pair[0], -EDGE), roll(pair[1], -EDGE)
        return jnp.where(last_y, high, low), jnp.where(last_y, low, high)

    def back_z(pair):
        return tuple(jnp.where(first_z, roll(v, 1 - EDGE), roll(v, 1)) for v in pair)

    def ahead_z(pair):
        return tuple(jnp.where(last_z, roll(v, EDGE - 1), roll(v, -1)) for v in pair)

    def add(a, b):
        return tuple(x + y for x, y in zip(a, b))

    def sub2(a, b):
        return tuple(x - y for x, y in zip(a, b))

    def mul(a, b):
        return tuple(x * y for x, y in zip(a, b))

    def quad(f):
        return lambda q: f(q[:2]) + f(q[2:])

    def back_x(q):
        r = [pltpu.roll(v, 1, 0) for v in q]
        return tuple(jnp.where(first_x, r[n ^ 2], r[n]) for n in range(4))

    def ahead_x(q):
        r = [pltpu.roll(v, ROWS - 1, 0) for v in q]
        return tuple(jnp.where(last_x, r[n ^ 2], r[n]) for n in range(4))

    def top_of(v, c):
        out = []
        for n in range(len(v[0])):
            vv = (v[0][n] * v[0][n] + v[1][n] * v[1][n]) + v[2][n] * v[2][n]
            cc = (c[0][n] * c[0][n] + c[1][n] * c[1][n]) + c[2][n] * c[2][n]
            root_v = vv * lax.rsqrt(jnp.maximum(vv, TINY))
            root_c = cc * lax.rsqrt(jnp.maximum(cc, TINY))
            out.append(root_v + 0.5 * root_c)
        return functools.reduce(jnp.maximum, out)

    def cells(v, c):
        return (
            sub2(mul(v[2], c[1]), mul(v[1], c[2])),
            sub2(mul(v[0], c[2]), mul(v[2], c[0])),
            sub2(mul(v[1], c[0]), mul(v[0], c[1])),
        )

    def fine_read(ref, base):
        return tuple(
            tuple(
                ref[pl.ds(base + c * TILES + 2 * HALF * ih + h, ROWS, stride=2), :]
                for ih in range(2)
                for h in range(2)
            )
            for c in range(3)
        )

    def fine_put(ref, base, values):
        for c in range(3):
            for ih in range(2):
                for h in range(2):
                    ref[pl.ds(base + c * TILES + 2 * HALF * ih + h, ROWS, stride=2), :] = values[c][
                        2 * ih + h
                    ]

    def fine_centre(b):
        return (add(b[0], ahead_x(b[0])), add(b[1], quad(ahead_y)(b[1])), add(b[2], quad(ahead_z)(b[2])))

    def fine_edges(b, v):
        cell = cells(v, fine_centre(b))
        part_x = add(cell[0], quad(back_y)(cell[0]))
        part_y = add(cell[1], quad(back_z)(cell[1]))
        part_z = add(cell[2], quad(back_y)(cell[2]))
        return (
            add(part_x, quad(back_z)(part_x)),
            add(part_y, back_x(part_y)),
            add(part_z, back_x(part_z)),
        )

    def fine_curl(e):
        return (
            sub2(sub2(quad(ahead_y)(e[2]), e[2]), sub2(quad(ahead_z)(e[1]), e[1])),
            sub2(sub2(quad(ahead_z)(e[0]), e[0]), sub2(ahead_x(e[2]), e[2])),
            sub2(sub2(ahead_x(e[1]), e[1]), sub2(quad(ahead_y)(e[0]), e[0])),
        )

    def by_axis(d, values):
        return jnp.where(d == 0, values[0], jnp.where(d == 1, values[1], values[2]))

    def sum_rows(v):
        return jnp.sum(v, axis=0, keepdims=True)

    listed.wait()
    loads[0].wait()
    loads[1].wait()

    half_lane = 32 * (row16 % 4)
    index_r = (half_lane + 2 * k8, 2 * k8, half_lane)
    target_r = (jnp.zeros_like(lane), row16, k8)

    def pair_edges(r):
        base = pairs[r, 0] * SPAN
        fine_put(emf_p, r * SPAN, fine_edges(fine_read(fb, base), fine_read(fv, base)))

    def pair_restrict(r):
        d = pairs[r, 1]
        index, target = by_axis(d, index_r), by_axis(d, target_r)
        upper = lane >= jnp.where(d == 1, LANES, 64)
        for which in range(2):
            axis = jnp.where(d == 0, 1, 0) if which == 0 else jnp.where(d == 2, 1, 2)
            base = r * SPAN + axis * TILES
            got = []
            for h in range(2):
                here = emf_p[pl.ds(base + h, ROWS, stride=4), :]
                if which == 0:
                    there = jnp.where(
                        d == 0, roll(here, -EDGE), emf_p[pl.ds(base + h + 2, ROWS, stride=4), :]
                    )
                else:
                    there = jnp.where(d == 2, roll(here, -EDGE), roll(here, -1))
                got.append(take(0.5 * (here + there), index))
            value = jnp.where(upper, got[1], got[0])
            rows1[pl.ds(4 * r + which, 1), :] = sum_rows(jnp.where(sub == target, value, 0.0))
        code = (pairs[r, 3] * 6 + d * 2 + pairs[r, 4]).astype(jnp.float32)
        key = jnp.where((lane[:1] // HALF) % 2 == pairs[r, 5], code, -1.0)
        rows1[pl.ds(4 * r + 2, 1), :] = key

    def each_pair(body):
        if pair_count <= 4:
            for r in range(pair_count):
                body(r)
        else:
            lax.fori_loop(0, pair_count, lambda r, _: (body(r), 0)[1], 0)

    each_pair(pair_edges)
    each_pair(pair_restrict)

    slot_of = [pairs[r, 0] for r in range(pair_count)]
    face_of = [pairs[r, 1] for r in range(pair_count)]
    owner_of = [pairs[r, 2] for r in range(pair_count)]
    rank_of = []
    for r in range(pair_count):
        rank = jnp.int32(0)
        for q in range(r):
            rank = rank + jnp.where(owner_of[q] == owner_of[r], 1, 0)
        rank_of.append(rank)

    def build(p, carry):
        message = jnp.full((ROWS, LANES), -1.0, jnp.float32)
        for r in range(pair_count):
            here = jnp.where(owner_of[r] == p, rank_of[r], ROWS)
            for n, row in enumerate((2 * here, 2 * here + 1, 2 * CAP + here)):
                message = jnp.where(
                    sub == row, jnp.broadcast_to(rows1[4 * r + n : 4 * r + n + 1, :], (ROWS, LANES)), message
                )
        slot(send1, p)[...] = message
        return carry

    def slot(ref, p):
        return ref.at[pl.ds(pl.multiple_of(p * ROWS, ROWS), ROWS)]

    lax.fori_loop(0, peers, build, 0, unroll=few)

    loads[2].wait()
    loads[3].wait()

    def column(tile):
        return pl.ds(pl.multiple_of(tile * LANES, LANES), LANES)

    def blocked(ref, g):
        def read(c, i):
            return tuple(ref[c, ROWS * g : ROWS * g + ROWS, column(2 * i + h)] for h in range(2))

        return read

    def blocked_put(ref, g):
        def put(c, i, pair):
            for h in range(2):
                ref[c, ROWS * g : ROWS * g + ROWS, column(2 * i + h)] = pair[h]

        return put


    def at(n, u, g, h):
        return pl.ds((((n * CHUNK + u) * coarse_groups + g) * 2 + h) * ROWS, ROWS)

    def each_plane(body):
        for u in range(CHUNK):
            for g in range(coarse_groups):
                body(u, g)

    def centre(chunk):
        def plane(u, g):
            i = chunk * CHUNK + u
            field = blocked(cb, g)
            b = [field(c, i) for c in range(3)]
            c = (
                add(b[0], field(0, lax.rem(i + 1, EDGE))),
                add(b[1], ahead_y(b[1])),
                add(b[2], ahead_z(b[2])),
            )
            for n in range(3):
                for h in range(2):
                    centred[at(n, u, g, h), :] = c[n][h]

        each_plane(plane)

    def coarse_step(t, carry):
        parts, best = carry
        parts = list(parts)

        def last(u, g):
            part_x = tuple(halfway[at(0, u, g, h), :] for h in range(2))
            i = lax.rem(t + CHUNKS - 2, CHUNKS) * CHUNK + u
            blocked_put(emf_c, g)(0, i, add(part_x, back_z(part_x)))

        each_plane(last)
        tops = []

        def middle(u, g):
            i = lax.rem(t + CHUNKS - 1, CHUNKS) * CHUNK + u
            put = blocked_put(emf_c, g)
            c = [tuple(centred[at(n, u, g, h), :] for h in range(2)) for n in range(3)]
            v = [blocked(cv, g)(n, i) for n in range(3)]
            cell = cells(v, c)
            part_x = add(cell[0], back_y(cell[0]))
            part_y = add(cell[1], back_z(cell[1]))
            part_z = add(cell[2], back_y(cell[2]))
            for h in range(2):
                halfway[at(0, u, g, h), :] = part_x[h]
            put(1, i, add(part_y, parts[g][0]))
            put(2, i, add(part_z, parts[g][1]))
            parts[g] = (part_y, part_z)
            tops.append(top_of(v, c))

        each_plane(middle)
        centre(lax.rem(t, CHUNKS))
        return tuple(parts), functools.reduce(jnp.maximum, tops, best)

    centre(CHUNKS - 1)
    nothing = ((zero, zero), (zero, zero))
    best = lax.fori_loop(0, CHUNKS + 2, coarse_step, ((nothing,) * coarse_groups, zero))[1]

    speed_step = largest_step(fine_count, SPEED_STEP)

    def fine_top(n, best):
        for u in range(speed_step):
            base = (n * speed_step + u) * SPAN
            b, v = fine_read(fb, base), fine_read(fv, base)
            best = jnp.maximum(best, top_of(v, fine_centre(b)))
        return best

    best = lax.fori_loop(0, fine_count // speed_step, fine_top, best)
    gmax[...] = best

    pl.semaphore_wait(barrier, peers - 1 + groups - 1)

    def out1(p):
        return pltpu.make_async_remote_copy(
            src_ref=slot(send1, p), dst_ref=slot(recv1, me), send_sem=s1_sem,
            recv_sem=r1_sem, device_id=(p, mg), device_id_type=MESH,
        )

    def out2(p):
        return pltpu.make_async_remote_copy(
            src_ref=slot(send2, p), dst_ref=slot(recv2, me), send_sem=s2_sem,
            recv_sem=r2_sem, device_id=(p, mg), device_id_type=MESH,
        )

    def outg(g):
        return pltpu.make_async_remote_copy(
            src_ref=gmax, dst_ref=slot(gmax_in, mg), send_sem=sg_sem,
            recv_sem=rg_sem, device_id=(me, g), device_id_type=MESH,
        )

    def drain(ref, sem, count):
        part = ref.at[pl.ds(0, ROWS * count)]
        pltpu.make_async_copy(part, part, sem).wait()

    each_group(lambda g: outg(g).start())
    each_peer(lambda p: out1(p).start())

    fine_step = largest_step(fine_count, FINE_STEP)

    def fine_bulk(n, carry):
        for u in range(fine_step):
            base = (n * fine_step + u) * SPAN
            fine_put(curl_f, base, fine_curl(fine_edges(fine_read(fb, base), fine_read(fv, base))))
        return carry

    lax.fori_loop(0, fine_count // fine_step, fine_bulk, 0)


    def packed(read, c, d, q1):
        if d == 0:
            return read(c, 0)[q1]
        out = zero
        for m in range(HALF):
            tiles = read(c, q1 * HALF + m)
            if d == 1:
                out = jnp.where(row16 == m, roll(tiles[0], EDGE * m), out)
            else:
                for q2 in range(2):
                    out = jnp.where(k_of == HALF * q2 + m, roll(tiles[q2], HALF * q2 + m), out)
        return out

    def plane_slot(n, g):
        at = (n * coarse_groups + g) * ROWS
        return slice(at, at + ROWS)

    for g in range(coarse_groups):
        for d in range(3):
            for q1 in range(2):
                plane_b[plane_slot(2 * d + q1, g), :] = packed(blocked(cb, g), d, d, q1)
                for which in range(2):
                    plane_e[plane_slot(4 * d + 2 * which + q1, g), :] = packed(
                        blocked(emf_c, g), TANGENT[d][which], d, q1
                    )

    def row_of(ref, n):
        return jnp.broadcast_to(ref[pl.ds(n, 1), :], (ROWS, LANES))

    slot(recv1, me)[...] = slot(send1, me)[...]
    drain(recv1, r1_sem, peers - 1)

    base_code = [((sub + ROWS * g) * 6).astype(jnp.float32) for g in range(coarse_groups)]
    empty = jnp.full((ROWS, LANES), EMPTY, jnp.float32)
    for g in range(coarse_groups):

        def collect(p, held, g=g):
            for c in range(CAP):
                code = row_of(recv1, p * ROWS + 2 * CAP + c) - base_code[g]
                values = [row_of(recv1, p * ROWS + 2 * c + which) for which in range(2)]
                held = [
                    jnp.where(code == float(2 * (n // 4) + n % 2), values[n // 2 % 2], held[n])
                    for n in range(12)
                ]
            return held

        held = lax.fori_loop(0, peers, collect, [empty] * 12, unroll=few)
        for n in range(12):
            held_ref[plane_slot(n, g), :] = held[n]

    spread = row16
    squeeze = EDGE * k8

    def ahead_i(pair):
        turned = [roll(v, -1) for v in pair]
        wrapped = [roll(v, HALF - 1) for v in pair]
        return tuple(jnp.where(k8 == HALF - 1, wrapped[1 - q], turned[q]) for q in range(2))

    def ahead_j(pair):
        return tuple(
            jnp.where(
                last_y,
                jnp.where(k_of < HALF, roll(v, LANES - EDGE - HALF), roll(v, LANES - HALF)),
                roll(v, -EDGE),
            )
            for v in pair
        )

    for g in range(coarse_groups):
        hold = [held_ref[plane_slot(n, g), :] for n in range(12)]
        sent = [[(hold[4 * d + 2 * w], hold[4 * d + 2 * w + 1]) for w in range(2)] for d in range(3)]
        now = [
            [
                [
                    jnp.where(
                        sent[d][w][q] < BIG, sent[d][w][q], plane_e[plane_slot(4 * d + 2 * w + q, g), :]
                    )
                    for q in range(2)
                ]
                for w in range(2)
            ]
            for d in range(3)
        ]
        for q in range(2):
            over = take(sent[2][0][q], spread)
            now[1][0][q] = jnp.where((over < BIG) & first_z, over, now[1][0][q])
            under = take(sent[1][0][q], squeeze)
            free = (sent[2][0][q] >= BIG) & (lane < HALF) & (under < BIG)
            now[2][0][q] = jnp.where(free, under, now[2][0][q])
            over = roll(sent[2][1][0], -HALF * q)
            now[0][0][q] = jnp.where((over < BIG) & first_z, over, now[0][0][q])
            under = roll(sent[0][0][q], HALF * q)
            free = (sent[2][1][0] >= BIG) & (k_of == HALF * q) & (under < BIG)
            now[2][1][0] = jnp.where(free, under, now[2][1][0])
        over, under = sent[1][1][0], sent[0][1][0]
        now[0][1][0] = jnp.where((over < BIG) & first_y, over, now[0][1][0])
        now[1][1][0] = jnp.where((over >= BIG) & first_y & (under < BIG), under, now[1][1][0])
        for d in range(3):
            one, two = now[d]
            if d < 2:
                ahead_one, ahead_two = ahead_y(two), ahead_z(one)
            else:
                ahead_one, ahead_two = ahead_i(two), ahead_j(one)
            left, right = sub2(ahead_one, two), sub2(ahead_two, one)
            curl = sub2(right, left) if d == 1 else sub2(left, right)
            for q in range(2):
                plane_n[plane_slot(2 * d + q, g), :] = curl[q]

    drain(gmax_in, rg_sem, groups - 1)
    for k in range(1, groups):
        best = jnp.maximum(best, slot(gmax_in, lax.rem(mg + k, groups))[...])
    top_row = jnp.broadcast_to(jnp.max(best, axis=0, keepdims=True), (ROWS, LANES))

    def answer(p, carry):
        rows = top_row
        for c in range(CAP):
            key = row_of(recv1, p * ROWS + 2 * CAP + c)
            curl_acc, field_acc = zero, zero
            for g in range(coarse_groups):
                code = key - base_code[g]
                for n in range(6):
                    hit = code == float(n)
                    curl_acc = jnp.where(hit, plane_n[plane_slot(n, g), :], curl_acc)
                    field_acc = jnp.where(hit, plane_b[plane_slot(n, g), :], field_acc)
            rows = jnp.where(sub == c, sum_rows(curl_acc), rows)
            rows = jnp.where(sub == CAP + c, sum_rows(field_acc), rows)
        slot(send2, p)[...] = rows
        return carry

    lax.fori_loop(0, peers, answer, 0, unroll=few)
    each_peer(lambda p: out2(p).start())

    for g in range(coarse_groups):
        for d in range(3):
            for which in range(2):
                axis = TANGENT[d][which]
                for q1 in range(2):
                    value = held_ref[plane_slot(4 * d + 2 * which + q1, g), :]

                    def patch(tile, shift, mask, value=value, axis=axis, g=g):
                        where = (axis, slice(ROWS * g, ROWS * g + ROWS), slice(tile * LANES, tile * LANES + LANES))
                        turned = roll(value, shift)
                        put = turned < BIG
                        if mask is not None:
                            put = put & mask
                        emf_c[where] = jnp.where(put, turned, emf_c[where])

                    if d == 0:
                        patch(q1, 0, None)
                        continue
                    for m in range(HALF):
                        tile = 2 * (q1 * HALF + m)
                        if d == 1:
                            patch(tile, -EDGE * m, first_y)
                        else:
                            for q2 in range(2):
                                patch(tile + q2, -(HALF * q2 + m), first_z)


    def curl_step(n, carry):
        for u in range(4):
            i = 4 * n + u
            after = lax.rem(i + 1, EDGE)
            for g in range(coarse_groups):
                read, put = blocked(emf_c, g), blocked_put(curl_c, g)
                e_x, e_y, e_z = read(0, i), read(1, i), read(2, i)
                put(0, i, sub2(sub2(ahead_y(e_z), e_z), sub2(ahead_z(e_y), e_y)))
                put(1, i, sub2(sub2(ahead_z(e_x), e_x), sub2(read(2, after), e_z)))
                put(2, i, sub2(sub2(read(1, after), e_y), sub2(ahead_y(e_x), e_x)))
        return carry

    lax.fori_loop(0, EDGE // 4, curl_step, 0)

    index_n = (lane, k_of, EDGE * k8)
    target_n = (jnp.zeros_like(lane), row16, row16)

    def pair_normal(r):
        d = pairs[r, 1]
        base = pairs[r, 0] * SPAN + d * TILES
        index, target = by_axis(d, index_n), by_axis(d, target_n)
        upper = k_of >= jnp.where(d == 2, HALF, EDGE)
        for n, ref in enumerate((fb, curl_f)):
            for h in range(2):
                start = base + jnp.where(d == 0, h, 2 * HALF * h)
                got = [take(ref[pl.ds(start + s, ROWS, stride=2), :], index) for s in range(2)]
                value = jnp.where(upper, got[1], got[0])
                picked[pl.ds((2 * n + h) * pair_rows + r, 1), :] = sum_rows(
                    jnp.where(sub == target, value, 0.0)
                )

    each_pair(pair_normal)

    slot(recv2, me)[...] = slot(send2, me)[...]
    drain(recv2, r2_sem, peers - 1)
    top = lax.fori_loop(
        0, peers, lambda p, t: jnp.maximum(t, row_of(recv2, p * ROWS + 2 * CAP)), zero, unroll=few
    )
    step_out[...] = jnp.broadcast_to(0.125 * (0.2 / jnp.max(top, axis=1, keepdims=True)), (ROWS, LANES))
    for r in range(pair_count):
        row = owner_of[r] * ROWS + rank_of[r]
        own_a[r : r + 1, :] = recv2[pl.ds(row, 1), :]
        own_b[r : r + 1, :] = recv2[pl.ds(row + CAP, 1), :]
    for s in range(0, pair_count, ROWS):
        turned, column_of = jnp.zeros_like(lane), jnp.zeros_like(lane)
        for r in range(s, min(s + ROWS, pair_count)):
            turned = jnp.where(sub == r - s, face_of[r], turned)
            column_of = jnp.where(sub == r - s, pairs[r, 5], column_of)
        for h in range(2):
            m, n = 4 * h + lane // 32, k_of // 2
            index = jnp.where(turned == 2, EDGE * n + m, EDGE * m + n) + HALF * column_of
            curl, field = take(own_a[s : s + ROWS, :], index), take(own_b[s : s + ROWS, :], index)
            side = slice(h * LANES, (h + 1) * LANES)
            fine = [picked[n * pair_rows + s : n * pair_rows + s + ROWS, :] for n in (h, 2 + h)]
            jump_a[s : s + ROWS, side] = fine[0] - field
            jump_b[s : s + ROWS, side] = 2.0 * fine[1] - curl
    drain(send1, s1_sem, peers - 1)
    drain(send2, s2_sem, peers - 1)
    drain(gmax_in, sg_sem, groups - 1)


def store(cb, curl_c, fb, curl_f, jump_a, jump_b, step, out_c, out_f, out_j, new_c, new_f, new_j, sems):
    by = step[0:1, 0:1]
    copies = []
    for c in range(3):
        new_c[c] = cb[c] - by * curl_c[c]
        copies.append(pltpu.make_async_copy(new_c.at[c], out_c.at[c], sems.at[len(copies)]))
        copies[-1].start()
    rows = fb.shape[0]
    for n in range(2):
        part = pl.ds(n * (rows // 2), rows // 2)
        new_f[part, :] = fb[part, :] - (2.0 * by) * curl_f[part, :]
        copies.append(pltpu.make_async_copy(new_f.at[part], out_f.at[part], sems.at[len(copies)]))
        copies[-1].start()
    count = out_j.shape[0]
    new_j[...] = (jump_a[...] - by * jump_b[...])[:count]
    copies.append(pltpu.make_async_copy(new_j, out_j, sems.at[len(copies)]))
    copies[-1].start()
    for copy in copies:
        copy.wait()


def on_device(peers, groups, coarse_field, coarse_velocity, fine_field, fine_velocity, pairs):
    coarse_count, fine_count = coarse_field.shape[1], fine_field.shape[1]
    pair_count = pairs.shape[1]
    cells = EDGE**3
    flat_rows = fine_count * SPAN

    def coarse_view(x):
        return jnp.transpose(x[0], (1, 0, 2))

    def fine_view(x):
        return x.reshape(flat_rows, LANES)

    pair_rows = ROWS * -(-pair_count // ROWS)
    operands = [
        pltpu.with_memory_space_constraint(x, pltpu.HBM)
        for x in (
            pairs[0],
            coarse_view(coarse_field),
            coarse_view(coarse_velocity),
            fine_view(fine_field),
            fine_view(fine_velocity),
        )
    ]
    f32 = jnp.float32
    dma = pltpu.SemaphoreType.DMA
    vmem = pltpu.VMEM
    anywhere = pl.BlockSpec(memory_space=pltpu.HBM)
    inside = pl.BlockSpec(memory_space=pltpu.VMEM)
    coarse_shape, fine_shape = (3, coarse_count, cells), (flat_rows, LANES)
    shapes = (
        coarse_shape,
        coarse_shape,
        fine_shape,
        fine_shape,
        (pair_rows, EDGE * EDGE),
        (pair_rows, EDGE * EDGE),
        (ROWS, LANES),
    )
    results = pl.pallas_call(
        functools.partial(kernel, peers, groups, coarse_count, fine_count, pair_count),
        out_shape=tuple(jax.ShapeDtypeStruct(s, f32) for s in shapes),
        in_specs=[anywhere] * 5,
        out_specs=(inside,) * len(shapes),
        scratch_shapes=[
            pltpu.SMEM(pairs.shape[1:], jnp.int32),
            vmem(coarse_shape, f32),
            vmem(fine_shape, f32),
            vmem(coarse_shape, f32),
            vmem((pair_count * SPAN, LANES), f32),
            vmem((6 * CHUNK * coarse_count, LANES), f32),
            vmem((2 * CHUNK * coarse_count, LANES), f32),
            vmem((12 * coarse_count, LANES), f32),
            vmem((6 * coarse_count, LANES), f32),
            vmem((6 * coarse_count, LANES), f32),
            vmem((12 * coarse_count, LANES), f32),
            vmem((pair_rows, LANES), f32),
            vmem((pair_rows, LANES), f32),
            vmem((4 * pair_rows, LANES), f32),
            vmem((4 * pair_rows, LANES), f32),
            vmem((peers * ROWS, LANES), f32),
            vmem((peers * ROWS, LANES), f32),
            vmem((peers * ROWS, LANES), f32),
            vmem((peers * ROWS, LANES), f32),
            vmem((ROWS, LANES), f32),
            vmem((groups * ROWS, LANES), f32),
            dma((5,)),
            dma,
            dma,
            dma,
            dma,
            dma,
            dma,
        ],
        compiler_params=pltpu.CompilerParams(
            collective_id=0, has_side_effects=True, vmem_limit_bytes=32 * 1024 * 1024
        ),
    )(*operands)
    coarse_out, fine_out, jump = pl.pallas_call(
        store,
        out_shape=(
            jax.ShapeDtypeStruct(coarse_shape, f32),
            jax.ShapeDtypeStruct(fine_shape, f32),
            jax.ShapeDtypeStruct((pair_count, EDGE * EDGE), f32),
        ),
        in_specs=[inside] * len(shapes),
        out_specs=(anywhere,) * 3,
        scratch_shapes=[
            vmem(coarse_shape, f32),
            vmem(fine_shape, f32),
            vmem((pair_count, EDGE * EDGE), f32),
            dma((6,)),
        ],
    )(*(pltpu.with_memory_space_constraint(x, pltpu.VMEM) for x in results))
    return (
        jnp.transpose(coarse_out, (1, 0, 2))[None],
        fine_out.reshape(1, fine_count, 3, cells),
        jump[None],
    )


def solution(mesh):
    spec = P("gz", "blocks", None, None)
    flat = P("gz", "blocks", None)
    return jax.shard_map(
        functools.partial(on_device, mesh.shape["blocks"], mesh.shape["gz"]),
        mesh=mesh,
        in_specs=(spec, spec, spec, spec, flat),
        out_specs=(spec, spec, flat),
        check_vma=False,
    )
```

```python
import functools

import jax
import jax.numpy as jnp
from jax import lax
from jax.experimental import pallas as pl
from jax.experimental.pallas import tpu as pltpu
from jax.sharding import PartitionSpec as P

EDGE = 16
HALF = 8
CAP = 2
LANES = 128
ROWS = 8
TILES = EDGE**3 // LANES
SPAN = 3 * TILES
TINY = 1.2e-38
BIG = 1e30
EMPTY = 3e38
TANGENT = ((1, 2), (0, 2), (0, 1))
MESH = pl.DeviceIdType.MESH
TOP_CHUNK = 4
CHUNK = 4
CHUNKS = EDGE // CHUNK
FINE_STEP = 4
SPEED_STEP = 6


def take(values, index):
    return jnp.take_along_axis(values, index, axis=1, mode="promise_in_bounds")


def largest_step(count, most):
    return max(n for n in range(1, most + 1) if count % n == 0)


def kernel(
    peers,
    groups,
    coarse_count,
    fine_count,
    pair_count,
    pairs_hbm,
    cb_hbm,
    cv_hbm,
    fb_hbm,
    fv_hbm,
    cb,
    curl_c,
    fb,
    curl_f,
    picked,
    own_a,
    own_b,
    index_out,
    step_out,
    pairs,
    cv,
    fv,
    emf_c,
    emf_p,
    centred,
    halfway,
    plane_e,
    plane_b,
    plane_n,
    held_ref,
    top_rows,
    rows1,
    send1,
    recv1,
    send2,
    recv2,
    gmax,
    gmax_in,
    load_sem,
    s1_sem,
    r1_sem,
    s2_sem,
    r2_sem,
    sg_sem,
    rg_sem,
):
    me = lax.axis_index("blocks")
    mg = lax.axis_index("gz")
    few = peers <= 8
    coarse_groups = coarse_count // ROWS
    pair_rows = ROWS * -(-pair_count // ROWS)

    paired = peers & (peers - 1) == 0
    bits = [1 << n for n in range(peers.bit_length() - 1)]

    def target(k):
        if not paired:
            return lax.rem(me + k, peers)
        p = me
        for bit in bits:
            p = p + lax.rem(k // bit, 2) * bit * (1 - 2 * lax.rem(me // bit, 2))
        return p

    def source(k):
        return target(k) if paired else lax.rem(me + peers - k, peers)

    def each_step(first, last, body, carry=0):
        def step(n, carry):
            return body(last - 1 - n, carry)

        return lax.fori_loop(0, last - first, step, carry, unroll=few)

    def each_peer(body):
        each_step(1, peers, lambda k, _: (body(target(k)), 0)[1])

    def each_group(body):
        for k in range(1, groups):
            body(lax.rem(mg + k, groups))

    barrier = pltpu.get_barrier_semaphore()
    each_peer(
        lambda p: pl.semaphore_signal(barrier, inc=1, device_id=(p, mg), device_id_type=MESH)
    )
    loads = [
        pltpu.make_async_copy(src, dst, load_sem.at[n])
        for n, (src, dst) in enumerate(((fb_hbm, fb), (fv_hbm, fv), (cb_hbm, cb), (cv_hbm, cv)))
    ]
    listed = pltpu.make_async_copy(pairs_hbm, pairs, load_sem.at[4])
    listed.start()
    for load in loads:
        load.start()
    each_group(
        lambda g: pl.semaphore_signal(barrier, inc=1, device_id=(me, g), device_id_type=MESH)
    )

    lane = lax.broadcasted_iota(jnp.int32, (ROWS, LANES), 1)
    sub = lax.broadcasted_iota(jnp.int32, (ROWS, LANES), 0)
    zero = jnp.zeros((ROWS, LANES), jnp.float32)
    row16 = lane // EDGE
    k_of = lane % EDGE
    k8 = lane % HALF
    first_y = lane < EDGE
    last_y = lane >= LANES - EDGE
    first_z = k_of == 0
    last_z = k_of == EDGE - 1
    first_x = sub == 0
    last_x = sub == ROWS - 1

    def roll(v, shift):
        return v if shift % LANES == 0 else pltpu.roll(v, shift % LANES, 1)

    def back_y(pair):
        low, high = roll(pair[0], EDGE), roll(pair[1], EDGE)
        return jnp.where(first_y, high, low), jnp.where(first_y, low, high)

    def ahead_y(pair):
        low, high = roll(pair[0], -EDGE), roll(pair[1], -EDGE)
        return jnp.where(last_y, high, low), jnp.where(last_y, low, high)

    def back_z(pair):
        return tuple(jnp.where(first_z, roll(v, 1 - EDGE), roll(v, 1)) for v in pair)

    def ahead_z(pair):
        return tuple(jnp.where(last_z, roll(v, EDGE - 1), roll(v, -1)) for v in pair)

    def add(a, b):
        return tuple(x + y for x, y in zip(a, b))

    def sub2(a, b):
        return tuple(x - y for x, y in zip(a, b))

    def mul(a, b):
        return tuple(x * y for x, y in zip(a, b))

    def quad(f):
        return lambda q: f(q[:2]) + f(q[2:])

    def back_x(q):
        r = [pltpu.roll(v, 1, 0) for v in q]
        return tuple(jnp.where(first_x, r[n ^ 2], r[n]) for n in range(4))

    def ahead_x(q):
        r = [pltpu.roll(v, ROWS - 1, 0) for v in q]
        return tuple(jnp.where(last_x, r[n ^ 2], r[n]) for n in range(4))

    def top_of(v, c):
        out = []
        for n in range(len(v[0])):
            vv = (v[0][n] * v[0][n] + v[1][n] * v[1][n]) + v[2][n] * v[2][n]
            cc = (c[0][n] * c[0][n] + c[1][n] * c[1][n]) + c[2][n] * c[2][n]
            root_v = vv * lax.rsqrt(jnp.maximum(vv, TINY))
            root_c = cc * lax.rsqrt(jnp.maximum(cc, TINY))
            out.append(root_v + 0.5 * root_c)
        return functools.reduce(jnp.maximum, out)

    def cells(v, c):
        return (
            sub2(mul(v[2], c[1]), mul(v[1], c[2])),
            sub2(mul(v[0], c[2]), mul(v[2], c[0])),
            sub2(mul(v[1], c[0]), mul(v[0], c[1])),
        )

    def fine_read(ref, base):
        return tuple(
            tuple(
                ref[pl.ds(base + c * TILES + 2 * HALF * ih + h, ROWS, stride=2), :]
                for ih in range(2)
                for h in range(2)
            )
            for c in range(3)
        )

    def fine_put(ref, base, values):
        for c in range(3):
            for ih in range(2):
                for h in range(2):
                    ref[pl.ds(base + c * TILES + 2 * HALF * ih + h, ROWS, stride=2), :] = values[c][
                        2 * ih + h
                    ]

    def fine_centre(b):
        return (add(b[0], ahead_x(b[0])), add(b[1], quad(ahead_y)(b[1])), add(b[2], quad(ahead_z)(b[2])))

    def fine_edges(b, v):
        cell = cells(v, fine_centre(b))
        part_x = add(cell[0], quad(back_y)(cell[0]))
        part_y = add(cell[1], quad(back_z)(cell[1]))
        part_z = add(cell[2], quad(back_y)(cell[2]))
        return (
            add(part_x, quad(back_z)(part_x)),
            add(part_y, back_x(part_y)),
            add(part_z, back_x(part_z)),
        )

    def fine_curl(e):
        return (
            sub2(sub2(quad(ahead_y)(e[2]), e[2]), sub2(quad(ahead_z)(e[1]), e[1])),
            sub2(sub2(quad(ahead_z)(e[0]), e[0]), sub2(ahead_x(e[2]), e[2])),
            sub2(sub2(ahead_x(e[1]), e[1]), sub2(quad(ahead_y)(e[0]), e[0])),
        )

    def by_axis(d, values):
        return jnp.where(d == 0, values[0], jnp.where(d == 1, values[1], values[2]))

    def sum_rows(v):
        return jnp.sum(v, axis=0, keepdims=True)

    listed.wait()
    loads[0].wait()
    loads[1].wait()

    half_lane = 32 * (row16 % 4)
    index_r = (half_lane + 2 * k8, 2 * k8, half_lane)
    target_r = (jnp.zeros_like(lane), row16, k8)

    def pair_edges(r):
        base = pairs[r, 0] * SPAN
        fine_put(emf_p, r * SPAN, fine_edges(fine_read(fb, base), fine_read(fv, base)))

    def pair_restrict(r):
        d = pairs[r, 1]
        index, target = by_axis(d, index_r), by_axis(d, target_r)
        upper = lane >= jnp.where(d == 1, LANES, 64)
        for which in range(2):
            axis = jnp.where(d == 0, 1, 0) if which == 0 else jnp.where(d == 2, 1, 2)
            base = r * SPAN + axis * TILES
            got = []
            for h in range(2):
                here = emf_p[pl.ds(base + h, ROWS, stride=4), :]
                if which == 0:
                    there = jnp.where(
                        d == 0, roll(here, -EDGE), emf_p[pl.ds(base + h + 2, ROWS, stride=4), :]
                    )
                else:
                    there = jnp.where(d == 2, roll(here, -EDGE), roll(here, -1))
                got.append(take(0.5 * (here + there), index))
            value = jnp.where(upper, got[1], got[0])
            rows1[pl.ds(4 * r + which, 1), :] = sum_rows(jnp.where(sub == target, value, 0.0))
        code = (pairs[r, 3] * 6 + d * 2 + pairs[r, 4]).astype(jnp.float32)
        key = jnp.where((lane[:1] // HALF) % 2 == pairs[r, 5], code, -1.0)
        rows1[pl.ds(4 * r + 2, 1), :] = key

    def each_pair(body):
        if pair_count <= 4:
            for r in range(pair_count):
                body(r)
        else:
            lax.fori_loop(0, pair_count, lambda r, _: (body(r), 0)[1], 0)

    each_pair(pair_edges)
    each_pair(pair_restrict)

    slot_of = [pairs[r, 0] for r in range(pair_count)]
    face_of = [pairs[r, 1] for r in range(pair_count)]
    owner_of = [pairs[r, 2] for r in range(pair_count)]
    rank_of = []
    for r in range(pair_count):
        rank = jnp.int32(0)
        for q in range(r):
            rank = rank + jnp.where(owner_of[q] == owner_of[r], 1, 0)
        rank_of.append(rank)

    def build(p, carry):
        message = jnp.full((ROWS, LANES), -1.0, jnp.float32)
        for r in range(pair_count):
            here = jnp.where(owner_of[r] == p, rank_of[r], ROWS)
            for n, row in enumerate((2 * here, 2 * here + 1, 2 * CAP + here)):
                message = jnp.where(
                    sub == row, jnp.broadcast_to(rows1[4 * r + n : 4 * r + n + 1, :], (ROWS, LANES)), message
                )
        slot(send1, p)[...] = message
        return carry

    def slot(ref, p):
        return ref.at[pl.ds(pl.multiple_of(p * ROWS, ROWS), ROWS)]

    lax.fori_loop(0, peers, build, 0, unroll=few)

    def column(tile):
        return pl.ds(pl.multiple_of(tile * LANES, LANES), LANES)

    def blocked(ref, g):
        def read(c, i):
            return tuple(ref[c, ROWS * g : ROWS * g + ROWS, column(2 * i + h)] for h in range(2))

        return read

    def blocked_put(ref, g):
        def put(c, i, pair):
            for h in range(2):
                ref[c, ROWS * g : ROWS * g + ROWS, column(2 * i + h)] = pair[h]

        return put

    speed_step = largest_step(fine_count, SPEED_STEP)

    def fine_top(n, best):
        for u in range(speed_step):
            base = (n * speed_step + u) * SPAN
            b, v = fine_read(fb, base), fine_read(fv, base)
            best = jnp.maximum(best, top_of(v, fine_centre(b)))
        return best

    best = lax.fori_loop(0, fine_count // speed_step, fine_top, zero)

    loads[2].wait()
    loads[3].wait()


    def at(n, i, g, h):
        row = (((n * coarse_groups + g) * EDGE + i) * 2 + h) * ROWS
        return pl.ds(row if isinstance(row, int) else pl.multiple_of(row, ROWS), ROWS)

    def each_plane(chunk, planes, body):
        for u in range(planes):
            for g in range(coarse_groups):
                body(chunk * planes + u, g)

    def coarse_top(n, best):
        tops = []

        def plane(i, g):
            field = blocked(cb, g)
            b = [field(c, i) for c in range(3)]
            c = (
                add(b[0], field(0, lax.rem(i + 1, EDGE))),
                add(b[1], ahead_y(b[1])),
                add(b[2], ahead_z(b[2])),
            )
            for k in range(3):
                for h in range(2):
                    centred[at(k, i, g, h), :] = c[k][h]
            tops.append(top_of([blocked(cv, g)(k, i) for k in range(3)], c))

        each_plane(n, TOP_CHUNK, plane)
        return functools.reduce(jnp.maximum, tops, best)

    best = lax.fori_loop(0, EDGE // TOP_CHUNK, coarse_top, best)
    gmax[...] = best

    pl.semaphore_wait(barrier, peers - 1 + groups - 1)

    def out1(k):
        p = target(k)
        return pltpu.make_async_remote_copy(
            src_ref=slot(send1, p), dst_ref=slot(recv1, me), send_sem=s1_sem,
            recv_sem=r1_sem.at[k // (peers - 1)], device_id=(p, mg), device_id_type=MESH,
        )

    def out2(p):
        return pltpu.make_async_remote_copy(
            src_ref=slot(send2, p), dst_ref=slot(recv2, me), send_sem=s2_sem,
            recv_sem=r2_sem, device_id=(p, mg), device_id_type=MESH,
        )

    def outg(g):
        return pltpu.make_async_remote_copy(
            src_ref=gmax, dst_ref=slot(gmax_in, mg), send_sem=sg_sem,
            recv_sem=rg_sem, device_id=(me, g), device_id_type=MESH,
        )

    def drain(ref, sem, count):
        part = ref.at[pl.ds(0, ROWS * count)]
        pltpu.make_async_copy(part, part, sem).wait()

    each_group(lambda g: outg(g).start())
    each_step(1, peers, lambda k, _: (out1(k).start(), 0)[1])


    def coarse_step(t, parts):
        parts = list(parts)

        def last(i, g):
            part_x = tuple(halfway[at(0, i, g, h), :] for h in range(2))
            blocked_put(emf_c, g)(0, i, add(part_x, back_z(part_x)))

        def first(i, g):
            put = blocked_put(emf_c, g)
            c = [tuple(centred[at(n, i, g, h), :] for h in range(2)) for n in range(3)]
            cell = cells([blocked(cv, g)(n, i) for n in range(3)], c)
            part_x = add(cell[0], back_y(cell[0]))
            part_y = add(cell[1], back_z(cell[1]))
            part_z = add(cell[2], back_y(cell[2]))
            for h in range(2):
                halfway[at(0, i, g, h), :] = part_x[h]
            put(1, i, add(part_y, parts[g][0]))
            put(2, i, add(part_z, parts[g][1]))
            parts[g] = (part_y, part_z)

        each_plane(lax.rem(t + CHUNKS - 1, CHUNKS), CHUNK, last)
        each_plane(lax.rem(t, CHUNKS), CHUNK, first)
        return tuple(parts)

    nothing = ((zero, zero), (zero, zero))
    lax.fori_loop(0, CHUNKS + 1, coarse_step, (nothing,) * coarse_groups)


    def packed(read, c, d, q1):
        if d == 0:
            return read(c, 0)[q1]
        out = zero
        for m in range(HALF):
            tiles = read(c, q1 * HALF + m)
            if d == 1:
                out = jnp.where(row16 == m, roll(tiles[0], EDGE * m), out)
            else:
                for q2 in range(2):
                    out = jnp.where(k_of == HALF * q2 + m, roll(tiles[q2], HALF * q2 + m), out)
        return out

    def plane_slot(n, g):
        at = (n * coarse_groups + g) * ROWS
        return slice(at, at + ROWS)

    for g in range(coarse_groups):
        for d in range(3):
            for q1 in range(2):
                plane_b[plane_slot(2 * d + q1, g), :] = packed(blocked(cb, g), d, d, q1)
                for which in range(2):
                    plane_e[plane_slot(4 * d + 2 * which + q1, g), :] = packed(
                        blocked(emf_c, g), TANGENT[d][which], d, q1
                    )

    fine_step = largest_step(fine_count, FINE_STEP)

    def fine_bulk(n, carry):
        for u in range(fine_step):
            base = (n * fine_step + u) * SPAN
            fine_put(curl_f, base, fine_curl(fine_edges(fine_read(fb, base), fine_read(fv, base))))
        return carry

    lax.fori_loop(0, fine_count // fine_step, fine_bulk, 0)

    def row_of(ref, n):
        return jnp.broadcast_to(ref[pl.ds(n, 1), :], (ROWS, LANES))

    base_code = [((sub + ROWS * g) * 6).astype(jnp.float32) for g in range(coarse_groups)]
    empty = jnp.full((ROWS, LANES), EMPTY, jnp.float32)

    def collect(p, held):
        held = list(held)
        for c in range(CAP):
            key = row_of(recv1, p * ROWS + 2 * CAP + c)
            values = [row_of(recv1, p * ROWS + 2 * c + which) for which in range(2)]
            for g in range(coarse_groups):
                code = key - base_code[g]
                held[g] = tuple(
                    jnp.where(code == float(2 * (n // 4) + n % 2), values[n // 2 % 2], held[g][n])
                    for n in range(12)
                )
        return tuple(held)

    slot(recv1, me)[...] = slot(send1, me)[...]
    drain(recv1, r1_sem.at[0], peers - 2)
    held = collect(me, ((empty,) * 12,) * coarse_groups)
    held = each_step(1, peers - 1, lambda k, held: collect(source(k), held), held)
    for g in range(coarse_groups):
        for n in range(12):
            held_ref[plane_slot(n, g), :] = held[g][n]
    drain(gmax_in, rg_sem, groups - 1)
    for k in range(1, groups):
        best = jnp.maximum(best, slot(gmax_in, lax.rem(mg + k, groups))[...])
    top = jnp.max(jnp.max(best, axis=0, keepdims=True), axis=1, keepdims=True)
    top_rows[...] = jnp.broadcast_to(top, (ROWS, LANES))
    drain(recv1, r1_sem.at[1], 1)
    held = tuple(
        tuple(held_ref[plane_slot(n, g), :] for n in range(12)) for g in range(coarse_groups)
    )
    held = collect(source(jnp.int32(peers - 1)), held)
    spread = row16
    squeeze = EDGE * k8
    upper8 = k_of >= HALF

    def known(v):
        return v < BIG

    def chosen(v, other):
        return jnp.where(known(v), v, other)

    for g in range(coarse_groups):
        for n in range(12):
            held_ref[plane_slot(n, g), :] = held[g][n]
        sent = [[[held[g][4 * d + 2 * w + q] for q in range(2)] for w in range(2)] for d in range(3)]
        base = [
            [
                [chosen(sent[d][w][q], plane_e[plane_slot(4 * d + 2 * w + q, g), :]) for q in range(2)]
                for w in range(2)
            ]
            for d in range(3)
        ]
        now = [[list(base[d][w]) for w in range(2)] for d in range(3)]
        ahead = [[[None] * 2 for w in range(2)] for d in range(3)]
        for q in range(2):
            over = roll(sent[2][1][0], -HALF * q)
            now[0][0][q] = jnp.where(first_z, chosen(over, base[0][0][q]), base[0][0][q])
            wrap = chosen(roll(sent[2][1][0], EDGE - 1 - HALF * q), roll(base[0][0][q], EDGE - 1))
            ahead[0][0][q] = jnp.where(last_z, wrap, roll(base[0][0][q], -1))

            over = take(sent[2][0][q], spread)
            now[1][0][q] = jnp.where(first_z, chosen(over, base[1][0][q]), base[1][0][q])
            wrap = chosen(over, roll(base[1][0][q], EDGE - 1))
            ahead[1][0][q] = jnp.where(last_z, wrap, roll(base[1][0][q], -1))

            under = take(sent[1][0][q], squeeze)
            free = known(under) & (sent[2][0][q] >= BIG) & (lane < HALF)
            now[2][0][q] = jnp.where(free, under, base[2][0][q])
            free = known(under) & (roll(sent[2][0][q], LANES - HALF) >= BIG)
            wrap = jnp.where(free, under, roll(base[2][0][q], LANES - HALF))
            wrap = jnp.where(upper8, wrap, roll(base[2][0][q], LANES - EDGE - HALF))
            ahead[2][0][q] = jnp.where(last_y, wrap, roll(base[2][0][q], -EDGE))

        over, under = sent[1][1][0], sent[0][1][0]
        now[0][1][0] = jnp.where(first_y, chosen(over, base[0][1][0]), base[0][1][0])
        free = known(under) & (over >= BIG) & first_y
        now[1][1][0] = jnp.where(free, under, base[1][1][0])
        over, under = roll(over, -EDGE), roll(under, -EDGE)
        turned = [[roll(base[d][1][q], -EDGE) for q in range(2)] for d in range(2)]
        wrap = (chosen(over, turned[0][0]), jnp.where(known(under) & (over >= BIG), under, turned[1][0]))
        for d in range(2):
            ahead[d][1] = [
                jnp.where(last_y, turned[d][1], turned[d][0]),
                jnp.where(last_y, wrap[d], turned[d][1]),
            ]

        under = jnp.where(upper8, roll(sent[0][0][1], HALF), sent[0][0][0])
        free = known(under) & (sent[2][1][0] >= BIG) & (k8 == 0)
        now[2][1][0] = jnp.where(free, under, base[2][1][0])
        under = jnp.where(upper8, roll(sent[0][0][1], EDGE - 1), roll(sent[0][0][0], HALF - 1))
        free = known(under) & (roll(sent[2][1][0], HALF - 1) >= BIG)
        turned = [roll(base[2][1][q], HALF - 1) for q in range(2)]
        wrap = (turned[1], jnp.where(free, under, turned[0]))
        for q in range(2):
            ahead[2][1][q] = jnp.where(k8 == HALF - 1, wrap[q], roll(base[2][1][q], -1))

        for d in range(3):
            left, right = sub2(ahead[d][1], now[d][1]), sub2(ahead[d][0], now[d][0])
            curl = sub2(right, left) if d == 1 else sub2(left, right)
            for q in range(2):
                plane_n[plane_slot(2 * d + q, g), :] = curl[q]


    def answer(p):
        rows = top_rows[...]
        for c in range(CAP):
            key = row_of(recv1, p * ROWS + 2 * CAP + c)
            curl_acc, field_acc = zero, zero
            for g in range(coarse_groups):
                code = key - base_code[g]
                for n in range(6):
                    hit = code == float(n)
                    curl_acc = jnp.where(hit, plane_n[plane_slot(n, g), :], curl_acc)
                    field_acc = jnp.where(hit, plane_b[plane_slot(n, g), :], field_acc)
            rows = jnp.where(sub == c, sum_rows(curl_acc), rows)
            rows = jnp.where(sub == CAP + c, sum_rows(field_acc), rows)
        slot(send2, p)[...] = rows

    def reply(k, carry):
        answer(target(k))
        out2(target(k)).start()
        return carry

    each_step(1, peers, reply)
    answer(me)
    for g in range(coarse_groups):
        for d in range(3):
            for which in range(2):
                axis = TANGENT[d][which]
                for q1 in range(2):
                    value = held_ref[plane_slot(4 * d + 2 * which + q1, g), :]

                    def patch(tile, shift, mask, value=value, axis=axis, g=g):
                        where = (axis, slice(ROWS * g, ROWS * g + ROWS), slice(tile * LANES, tile * LANES + LANES))
                        turned = roll(value, shift)
                        put = turned < BIG
                        if mask is not None:
                            put = put & mask
                        emf_c[where] = jnp.where(put, turned, emf_c[where])

                    if d == 0:
                        patch(q1, 0, None)
                        continue
                    for m in range(HALF):
                        tile = 2 * (q1 * HALF + m)
                        if d == 1:
                            patch(tile, -EDGE * m, first_y)
                        else:
                            for q2 in range(2):
                                patch(tile + q2, -(HALF * q2 + m), first_z)


    def curl_step(n, carry):
        for u in range(4):
            i = 4 * n + u
            after = lax.rem(i + 1, EDGE)
            for g in range(coarse_groups):
                read, put = blocked(emf_c, g), blocked_put(curl_c, g)
                e_x, e_y, e_z = read(0, i), read(1, i), read(2, i)
                put(0, i, sub2(sub2(ahead_y(e_z), e_z), sub2(ahead_z(e_y), e_y)))
                put(1, i, sub2(sub2(ahead_z(e_x), e_x), sub2(read(2, after), e_z)))
                put(2, i, sub2(sub2(read(1, after), e_y), sub2(ahead_y(e_x), e_x)))
        return carry

    lax.fori_loop(0, EDGE // 4, curl_step, 0)

    index_n = (lane, k_of, EDGE * k8)
    target_n = (jnp.zeros_like(lane), row16, row16)

    def pair_normal(r):
        d = pairs[r, 1]
        base = pairs[r, 0] * SPAN + d * TILES
        index, target = by_axis(d, index_n), by_axis(d, target_n)
        upper = k_of >= jnp.where(d == 2, HALF, EDGE)
        for n, ref in enumerate((fb, curl_f)):
            for h in range(2):
                start = base + jnp.where(d == 0, h, 2 * HALF * h)
                got = [take(ref[pl.ds(start + s, ROWS, stride=2), :], index) for s in range(2)]
                value = jnp.where(upper, got[1], got[0])
                picked[pl.ds((2 * n + h) * pair_rows + r, 1), :] = sum_rows(
                    jnp.where(sub == target, value, 0.0)
                )

    each_pair(pair_normal)

    for s in range(0, pair_count, ROWS):
        turned, column_of = jnp.zeros_like(lane), jnp.zeros_like(lane)
        for r in range(s, min(s + ROWS, pair_count)):
            turned = jnp.where(sub == r - s, face_of[r], turned)
            column_of = jnp.where(sub == r - s, pairs[r, 5], column_of)
        for h in range(2):
            m, n = 4 * h + lane // 32, k_of // 2
            index_out[h * pair_rows + s : h * pair_rows + s + ROWS, :] = (
                jnp.where(turned == 2, EDGE * n + m, EDGE * m + n) + HALF * column_of
            )

    slot(recv2, me)[...] = slot(send2, me)[...]
    drain(recv2, r2_sem, peers - 1)
    for r in range(pair_count):
        row = owner_of[r] * ROWS + rank_of[r]
        own_a[r : r + 1, :] = recv2[pl.ds(row, 1), :]
        own_b[r : r + 1, :] = recv2[pl.ds(row + CAP, 1), :]
    top = lax.fori_loop(
        0, peers, lambda p, t: jnp.maximum(t, row_of(recv2, p * ROWS + 2 * CAP)), zero, unroll=few
    )
    step_out[...] = 0.125 * (0.2 / top)
    drain(send1, s1_sem, peers - 1)
    drain(send2, s2_sem, peers - 1)
    drain(gmax_in, sg_sem, groups - 1)


def store(
    cb, curl_c, fb, curl_f, picked, own_a, own_b, index, step, out_c, out_f, out_j, new_c, new_f, new_j, sems
):
    by = step[0:1, 0:1]
    copies = []

    def send(src, dst):
        copies.append(pltpu.make_async_copy(src, dst, sems.at[len(copies)]))
        copies[-1].start()

    for c in range(3):
        new_c[c] = cb[c] - by * curl_c[c]
        send(new_c.at[c], out_c.at[c])
    rows = fb.shape[0]
    for n in range(2):
        part = pl.ds(n * (rows // 2), rows // 2)
        new_f[part, :] = fb[part, :] - (2.0 * by) * curl_f[part, :]
        send(new_f.at[part], out_f.at[part])
    count, pair_rows = out_j.shape[0], own_a.shape[0]
    for s in range(0, count, ROWS):
        for h in range(2):
            fine, curl, column = [
                ref[n * pair_rows + s : n * pair_rows + s + ROWS, :]
                for ref, n in ((picked, h), (picked, 2 + h), (index, h))
            ]
            fine = fine - (2.0 * by) * curl
            coarse = own_b[s : s + ROWS, :] - by * own_a[s : s + ROWS, :]
            new_j[s : s + ROWS, h * LANES : (h + 1) * LANES] = fine - take(coarse, column)
    send(new_j.at[pl.ds(0, count)], out_j)
    for copy in copies:
        copy.wait()


def on_device(peers, groups, coarse_field, coarse_velocity, fine_field, fine_velocity, pairs):
    coarse_count, fine_count = coarse_field.shape[1], fine_field.shape[1]
    pair_count = pairs.shape[1]
    cells = EDGE**3
    flat_rows = fine_count * SPAN

    def coarse_view(x):
        return jnp.transpose(x[0], (1, 0, 2))

    def fine_view(x):
        return x.reshape(flat_rows, LANES)

    pair_rows = ROWS * -(-pair_count // ROWS)
    operands = [
        pltpu.with_memory_space_constraint(x, pltpu.HBM)
        for x in (
            pairs[0],
            coarse_view(coarse_field),
            coarse_view(coarse_velocity),
            fine_view(fine_field),
            fine_view(fine_velocity),
        )
    ]
    f32 = jnp.float32
    dma = pltpu.SemaphoreType.DMA
    vmem = pltpu.VMEM
    anywhere = pl.BlockSpec(memory_space=pltpu.HBM)
    inside = pl.BlockSpec(memory_space=pltpu.VMEM)
    coarse_shape, fine_shape = (3, coarse_count, cells), (flat_rows, LANES)
    shapes = (
        coarse_shape,
        coarse_shape,
        fine_shape,
        fine_shape,
        (4 * pair_rows, LANES),
        (pair_rows, LANES),
        (pair_rows, LANES),
        (2 * pair_rows, LANES),
        (ROWS, LANES),
    )
    kinds = [f32] * 7 + [jnp.int32, f32]
    results = pl.pallas_call(
        functools.partial(kernel, peers, groups, coarse_count, fine_count, pair_count),
        out_shape=tuple(jax.ShapeDtypeStruct(s, k) for s, k in zip(shapes, kinds)),
        in_specs=[anywhere] * 5,
        out_specs=(inside,) * len(shapes),
        scratch_shapes=[
            pltpu.SMEM(pairs.shape[1:], jnp.int32),
            vmem(coarse_shape, f32),
            vmem(fine_shape, f32),
            vmem(coarse_shape, f32),
            vmem((pair_count * SPAN, LANES), f32),
            vmem((6 * EDGE * coarse_count, LANES), f32),
            vmem((2 * EDGE * coarse_count, LANES), f32),
            vmem((12 * coarse_count, LANES), f32),
            vmem((6 * coarse_count, LANES), f32),
            vmem((6 * coarse_count, LANES), f32),
            vmem((12 * coarse_count, LANES), f32),
            vmem((ROWS, LANES), f32),
            vmem((4 * pair_rows, LANES), f32),
            vmem((peers * ROWS, LANES), f32),
            vmem((peers * ROWS, LANES), f32),
            vmem((peers * ROWS, LANES), f32),
            vmem((peers * ROWS, LANES), f32),
            vmem((ROWS, LANES), f32),
            vmem((groups * ROWS, LANES), f32),
            dma((5,)),
            dma,
            dma((2,)),
            dma,
            dma,
            dma,
            dma,
        ],
        compiler_params=pltpu.CompilerParams(
            collective_id=0, has_side_effects=True, vmem_limit_bytes=32 * 1024 * 1024
        ),
    )(*operands)
    coarse_out, fine_out, jump = pl.pallas_call(
        store,
        out_shape=(
            jax.ShapeDtypeStruct(coarse_shape, f32),
            jax.ShapeDtypeStruct(fine_shape, f32),
            jax.ShapeDtypeStruct((pair_count, EDGE * EDGE), f32),
        ),
        in_specs=[inside] * len(shapes),
        out_specs=(anywhere,) * 3,
        scratch_shapes=[
            vmem(coarse_shape, f32),
            vmem(fine_shape, f32),
            vmem((pair_rows, EDGE * EDGE), f32),
            dma((6,)),
        ],
    )(*(pltpu.with_memory_space_constraint(x, pltpu.VMEM) for x in results))
    return (
        jnp.transpose(coarse_out, (1, 0, 2))[None],
        fine_out.reshape(1, fine_count, 3, cells),
        jump[None],
    )


def solution(mesh):
    spec = P("gz", "blocks", None, None)
    flat = P("gz", "blocks", None)
    return jax.shard_map(
        functools.partial(on_device, mesh.shape["blocks"], mesh.shape["gz"]),
        mesh=mesh,
        in_specs=(spec, spec, spec, spec, flat),
        out_specs=(spec, spec, flat),
        check_vma=False,
    )
```

```python
import functools

import jax
import jax.numpy as jnp
from jax import lax
from jax.experimental import pallas as pl
from jax.experimental.pallas import tpu as pltpu
from jax.sharding import PartitionSpec as P

EDGE = 16
HALF = 8
CAP = 2
LANES = 128
ROWS = 8
TILES = EDGE**3 // LANES
SPAN = 3 * TILES
TINY = 1.2e-38
BIG = 1e30
EMPTY = 3e38
TANGENT = ((1, 2), (0, 2), (0, 1))
MESH = pl.DeviceIdType.MESH
TOP_CHUNK = 4
CHUNK = 4
CHUNKS = EDGE // CHUNK
FINE_STEP = 4
SPEED_STEP = 6


def take(values, index):
    return jnp.take_along_axis(values, index, axis=1, mode="promise_in_bounds")


def largest_step(count, most):
    return max(n for n in range(1, most + 1) if count % n == 0)


def kernel(
    peers,
    groups,
    coarse_count,
    fine_count,
    pair_count,
    pairs_hbm,
    cb_hbm,
    cv_hbm,
    fb_hbm,
    fv_hbm,
    curl_c,
    curl_f,
    fine_face,
    own_a,
    own_b,
    index_out,
    step_out,
    pairs,
    cb,
    cv,
    fb,
    fv,
    emf_c,
    emf_p,
    centred,
    halfway,
    plane_e,
    plane_b,
    plane_n,
    held_ref,
    picked,
    tops,
    rows1,
    send1,
    recv1,
    send2,
    recv2,
    gmax,
    gmax_in,
    load_sem,
    sent_sem,
    r1_sem,
    r2_sem,
    rg_sem,
    rt_sem,
):
    me = lax.axis_index("blocks")
    mg = lax.axis_index("gz")
    few = peers <= 8
    coarse_groups = coarse_count // ROWS
    pair_rows = ROWS * -(-pair_count // ROWS)

    paired = peers & (peers - 1) == 0
    flips = []
    for n in range(peers.bit_length() - 1):
        bit = 1 << n
        flips.append((bit, bit * (1 - 2 * lax.rem(lax.div(me, bit), 2))))

    def target(k):
        if not paired:
            return lax.rem(me + k, peers)
        return sum((lax.rem(lax.div(k, bit), 2) * flip for bit, flip in flips), me)

    def source(k):
        return target(k) if paired else lax.rem(me + peers - k, peers)

    def each_step(first, last, body, carry=0):
        if few:
            for k in range(last - 1, first - 1, -1):
                carry = body(k, carry)
            return carry
        return lax.fori_loop(0, last - first, lambda n, c: body(last - 1 - n, c), carry)

    def each_peer(body):
        each_step(1, peers, lambda k, _: (body(target(k)), 0)[1])

    def each_group(body):
        for k in range(1, groups):
            body(lax.rem(mg + k, groups))

    barrier = pltpu.get_barrier_semaphore()
    each_peer(
        lambda p: pl.semaphore_signal(barrier, inc=1, device_id=(p, mg), device_id_type=MESH)
    )
    loads = [
        pltpu.make_async_copy(src, dst, load_sem.at[n])
        for n, (src, dst) in enumerate(((fb_hbm, fb), (fv_hbm, fv), (cb_hbm, cb), (cv_hbm, cv)))
    ]
    listed = pltpu.make_async_copy(pairs_hbm, pairs, load_sem.at[4])
    listed.start()
    for load in loads:
        load.start()
    each_group(
        lambda g: pl.semaphore_signal(barrier, inc=1, device_id=(me, g), device_id_type=MESH)
    )

    lane = lax.broadcasted_iota(jnp.int32, (ROWS, LANES), 1)
    sub = lax.broadcasted_iota(jnp.int32, (ROWS, LANES), 0)
    zero = jnp.zeros((ROWS, LANES), jnp.float32)
    row16 = lane // EDGE
    k_of = lane % EDGE
    k8 = lane % HALF
    first_y = lane < EDGE
    last_y = lane >= LANES - EDGE
    first_z = k_of == 0
    last_z = k_of == EDGE - 1
    first_x = sub == 0
    last_x = sub == ROWS - 1

    def roll(v, shift):
        return v if shift % LANES == 0 else pltpu.roll(v, shift % LANES, 1)

    def back_y(pair):
        low, high = roll(pair[0], EDGE), roll(pair[1], EDGE)
        return jnp.where(first_y, high, low), jnp.where(first_y, low, high)

    def ahead_y(pair):
        low, high = roll(pair[0], -EDGE), roll(pair[1], -EDGE)
        return jnp.where(last_y, high, low), jnp.where(last_y, low, high)

    def back_z(pair):
        return tuple(jnp.where(first_z, roll(v, 1 - EDGE), roll(v, 1)) for v in pair)

    def ahead_z(pair):
        return tuple(jnp.where(last_z, roll(v, EDGE - 1), roll(v, -1)) for v in pair)

    def add(a, b):
        return tuple(x + y for x, y in zip(a, b))

    def sub2(a, b):
        return tuple(x - y for x, y in zip(a, b))

    def mul(a, b):
        return tuple(x * y for x, y in zip(a, b))

    def quad(f):
        return lambda q: f(q[:2]) + f(q[2:])

    def back_x(q):
        r = [pltpu.roll(v, 1, 0) for v in q]
        return tuple(jnp.where(first_x, r[n ^ 2], r[n]) for n in range(4))

    def ahead_x(q):
        r = [pltpu.roll(v, ROWS - 1, 0) for v in q]
        return tuple(jnp.where(last_x, r[n ^ 2], r[n]) for n in range(4))

    def top_of(v, c):
        out = []
        for n in range(len(v[0])):
            vv = (v[0][n] * v[0][n] + v[1][n] * v[1][n]) + v[2][n] * v[2][n]
            cc = (c[0][n] * c[0][n] + c[1][n] * c[1][n]) + c[2][n] * c[2][n]
            root_v = vv * lax.rsqrt(jnp.maximum(vv, TINY))
            root_c = cc * lax.rsqrt(jnp.maximum(cc, TINY))
            out.append(root_v + 0.5 * root_c)
        return functools.reduce(jnp.maximum, out)

    def cells(v, c):
        return (
            sub2(mul(v[2], c[1]), mul(v[1], c[2])),
            sub2(mul(v[0], c[2]), mul(v[2], c[0])),
            sub2(mul(v[1], c[0]), mul(v[0], c[1])),
        )

    def fine_read(ref, base):
        return tuple(
            tuple(
                ref[pl.ds(base + c * TILES + 2 * HALF * ih + h, ROWS, stride=2), :]
                for ih in range(2)
                for h in range(2)
            )
            for c in range(3)
        )

    def fine_put(ref, base, values):
        for c in range(3):
            for ih in range(2):
                for h in range(2):
                    ref[pl.ds(base + c * TILES + 2 * HALF * ih + h, ROWS, stride=2), :] = values[c][
                        2 * ih + h
                    ]

    def fine_centre(b):
        return (add(b[0], ahead_x(b[0])), add(b[1], quad(ahead_y)(b[1])), add(b[2], quad(ahead_z)(b[2])))

    def fine_edges(b, v):
        cell = cells(v, fine_centre(b))
        part_x = add(cell[0], quad(back_y)(cell[0]))
        part_y = add(cell[1], quad(back_z)(cell[1]))
        part_z = add(cell[2], quad(back_y)(cell[2]))
        return (
            add(part_x, quad(back_z)(part_x)),
            add(part_y, back_x(part_y)),
            add(part_z, back_x(part_z)),
        )

    def fine_curl(e):
        return (
            sub2(sub2(quad(ahead_y)(e[2]), e[2]), sub2(quad(ahead_z)(e[1]), e[1])),
            sub2(sub2(quad(ahead_z)(e[0]), e[0]), sub2(ahead_x(e[2]), e[2])),
            sub2(sub2(ahead_x(e[1]), e[1]), sub2(quad(ahead_y)(e[0]), e[0])),
        )

    def by_axis(d, values):
        return jnp.where(d == 0, values[0], jnp.where(d == 1, values[1], values[2]))

    def sum_rows(v):
        return jnp.sum(v, axis=0, keepdims=True)

    listed.wait()
    loads[0].wait()
    loads[1].wait()

    half_lane = 32 * (row16 % 4)
    index_r = (half_lane + 2 * k8, 2 * k8, half_lane)
    target_r = (jnp.zeros_like(lane), row16, k8)

    def pair_edges(r):
        base = pairs[r, 0] * SPAN
        fine_put(emf_p, r * SPAN, fine_edges(fine_read(fb, base), fine_read(fv, base)))

    def pair_restrict(r):
        d = pairs[r, 1]
        index, target = by_axis(d, index_r), by_axis(d, target_r)
        upper = lane >= jnp.where(d == 1, LANES, 64)
        for which in range(2):
            axis = jnp.where(d == 0, 1, 0) if which == 0 else jnp.where(d == 2, 1, 2)
            base = r * SPAN + axis * TILES
            got = []
            for h in range(2):
                here = emf_p[pl.ds(base + h, ROWS, stride=4), :]
                if which == 0:
                    there = jnp.where(
                        d == 0, roll(here, -EDGE), emf_p[pl.ds(base + h + 2, ROWS, stride=4), :]
                    )
                else:
                    there = jnp.where(d == 2, roll(here, -EDGE), roll(here, -1))
                got.append(take(0.5 * (here + there), index))
            value = jnp.where(upper, got[1], got[0])
            rows1[pl.ds(4 * r + which, 1), :] = sum_rows(jnp.where(sub == target, value, 0.0))
        code = (pairs[r, 3] * 6 + d * 2 + pairs[r, 4]).astype(jnp.float32)
        key = jnp.where((lane[:1] // HALF) % 2 == pairs[r, 5], code, -1.0)
        rows1[pl.ds(4 * r + 2, 1), :] = key

    def each_pair(body):
        if pair_count <= 4:
            for r in range(pair_count):
                body(r)
        else:
            lax.fori_loop(0, pair_count, lambda r, _: (body(r), 0)[1], 0)

    each_pair(pair_edges)
    each_pair(pair_restrict)

    slot_of = [pairs[r, 0] for r in range(pair_count)]
    face_of = [pairs[r, 1] for r in range(pair_count)]
    owner_of = [pairs[r, 2] for r in range(pair_count)]
    rank_of = []
    for r in range(pair_count):
        rank = jnp.int32(0)
        for q in range(r):
            rank = rank + jnp.where(owner_of[q] == owner_of[r], 1, 0)
        rank_of.append(rank)

    def build(p, carry):
        message = jnp.full((ROWS, LANES), -1.0, jnp.float32)
        for r in range(pair_count):
            here = jnp.where(owner_of[r] == p, rank_of[r], ROWS)
            for n, row in enumerate((2 * here, 2 * here + 1, 2 * CAP + here)):
                message = jnp.where(
                    sub == row, jnp.broadcast_to(rows1[4 * r + n : 4 * r + n + 1, :], (ROWS, LANES)), message
                )
        slot(send1, p)[...] = message
        return carry

    def slot(ref, p):
        return ref.at[pl.ds(pl.multiple_of(p * ROWS, ROWS), ROWS)]

    lax.fori_loop(0, peers, build, 0, unroll=few)

    def column(tile):
        return pl.ds(pl.multiple_of(tile * LANES, LANES), LANES)

    def blocked(ref, g):
        def read(c, i):
            return tuple(ref[c, ROWS * g : ROWS * g + ROWS, column(2 * i + h)] for h in range(2))

        return read

    def blocked_put(ref, g):
        def put(c, i, pair):
            for h in range(2):
                ref[c, ROWS * g : ROWS * g + ROWS, column(2 * i + h)] = pair[h]

        return put

    speed_step = largest_step(fine_count, SPEED_STEP)

    def fine_top(n, best):
        for u in range(speed_step):
            base = (n * speed_step + u) * SPAN
            b, v = fine_read(fb, base), fine_read(fv, base)
            best = jnp.maximum(best, top_of(v, fine_centre(b)))
        return best

    best = lax.fori_loop(0, fine_count // speed_step, fine_top, zero)

    loads[2].wait()
    loads[3].wait()


    def at(n, i, g, h):
        row = (((n * coarse_groups + g) * EDGE + i) * 2 + h) * ROWS
        return pl.ds(row if isinstance(row, int) else pl.multiple_of(row, ROWS), ROWS)

    def each_plane(chunk, planes, body):
        for u in range(planes):
            for g in range(coarse_groups):
                body(chunk * planes + u, g)

    def coarse_top(n, best):
        tops = []

        def plane(i, g):
            field = blocked(cb, g)
            b = [field(c, i) for c in range(3)]
            c = (
                add(b[0], field(0, lax.rem(i + 1, EDGE))),
                add(b[1], ahead_y(b[1])),
                add(b[2], ahead_z(b[2])),
            )
            for k in range(3):
                for h in range(2):
                    centred[at(k, i, g, h), :] = c[k][h]
            tops.append(top_of([blocked(cv, g)(k, i) for k in range(3)], c))

        each_plane(n, TOP_CHUNK, plane)
        return functools.reduce(jnp.maximum, tops, best)

    best = lax.fori_loop(0, EDGE // TOP_CHUNK, coarse_top, best)
    gmax[...] = jnp.max(best, axis=0, keepdims=True)

    pl.semaphore_wait(barrier, peers - 1 + groups - 1)

    def part(ref, p, rows):
        return ref.at[pl.ds(pl.multiple_of(p * ROWS, ROWS), rows)]

    def out1(k):
        p = target(k)
        return pltpu.make_async_remote_copy(
            src_ref=part(send1, p, 3 * CAP), dst_ref=part(recv1, me, 3 * CAP), send_sem=sent_sem,
            recv_sem=r1_sem.at[k // (peers - 1)], device_id=(p, mg), device_id_type=MESH,
        )

    def out2(p):
        return pltpu.make_async_remote_copy(
            src_ref=part(send2, p, 2 * CAP), dst_ref=part(recv2, me, 2 * CAP), send_sem=sent_sem,
            recv_sem=r2_sem, device_id=(p, mg), device_id_type=MESH,
        )

    def outg(g):
        return pltpu.make_async_remote_copy(
            src_ref=gmax, dst_ref=gmax_in.at[pl.ds(mg, 1)], send_sem=sent_sem,
            recv_sem=rg_sem, device_id=(me, g), device_id_type=MESH,
        )

    def outt(p):
        return pltpu.make_async_remote_copy(
            src_ref=tops.at[pl.ds(me, 1)], dst_ref=tops.at[pl.ds(me, 1)], send_sem=sent_sem,
            recv_sem=rt_sem, device_id=(p, mg), device_id_type=MESH,
        )

    def drain(ref, sem, rows):
        whole = ref.at[pl.ds(0, rows)]
        pltpu.make_async_copy(whole, whole, sem).wait()

    out1(peers - 1).start()
    each_group(lambda g: outg(g).start())
    each_step(1, peers - 1, lambda k, _: (out1(k).start(), 0)[1])


    def coarse_step(t, parts):
        parts = list(parts)

        def last(i, g):
            part_x = tuple(halfway[at(0, i, g, h), :] for h in range(2))
            blocked_put(emf_c, g)(0, i, add(part_x, back_z(part_x)))

        def first(i, g):
            put = blocked_put(emf_c, g)
            c = [tuple(centred[at(n, i, g, h), :] for h in range(2)) for n in range(3)]
            cell = cells([blocked(cv, g)(n, i) for n in range(3)], c)
            part_x = add(cell[0], back_y(cell[0]))
            part_y = add(cell[1], back_z(cell[1]))
            part_z = add(cell[2], back_y(cell[2]))
            for h in range(2):
                halfway[at(0, i, g, h), :] = part_x[h]
            put(1, i, add(part_y, parts[g][0]))
            put(2, i, add(part_z, parts[g][1]))
            parts[g] = (part_y, part_z)

        each_plane(lax.rem(t + CHUNKS - 1, CHUNKS), CHUNK, last)
        each_plane(lax.rem(t, CHUNKS), CHUNK, first)
        return tuple(parts)

    nothing = ((zero, zero), (zero, zero))
    lax.fori_loop(0, CHUNKS + 1, coarse_step, (nothing,) * coarse_groups)


    def packed(read, c, d, q1):
        if d == 0:
            return read(c, 0)[q1]
        out = zero
        for m in range(HALF):
            tiles = read(c, q1 * HALF + m)
            if d == 1:
                out = jnp.where(row16 == m, roll(tiles[0], EDGE * m), out)
            else:
                for q2 in range(2):
                    out = jnp.where(k_of == HALF * q2 + m, roll(tiles[q2], HALF * q2 + m), out)
        return out

    def plane_slot(n, g):
        at = (n * coarse_groups + g) * ROWS
        return slice(at, at + ROWS)

    for g in range(coarse_groups):
        for d in range(3):
            for q1 in range(2):
                plane_b[plane_slot(2 * d + q1, g), :] = packed(blocked(cb, g), d, d, q1)
                for which in range(2):
                    plane_e[plane_slot(4 * d + 2 * which + q1, g), :] = packed(
                        blocked(emf_c, g), TANGENT[d][which], d, q1
                    )

    fine_step = largest_step(fine_count, FINE_STEP)

    def fine_bulk(n, carry):
        for u in range(fine_step):
            base = (n * fine_step + u) * SPAN
            fine_put(curl_f, base, fine_curl(fine_edges(fine_read(fb, base), fine_read(fv, base))))
        return carry

    lax.fori_loop(0, fine_count // fine_step, fine_bulk, 0)

    def row_of(ref, n):
        return jnp.broadcast_to(ref[pl.ds(n, 1), :], (ROWS, LANES))

    base_code = [((sub + ROWS * g) * 6).astype(jnp.float32) for g in range(coarse_groups)]
    empty = jnp.full((ROWS, LANES), EMPTY, jnp.float32)

    def collect(p, held):
        held = list(held)
        for c in range(CAP):
            key = row_of(recv1, p * ROWS + 2 * CAP + c)
            values = [row_of(recv1, p * ROWS + 2 * c + which) for which in range(2)]
            for g in range(coarse_groups):
                code = key - base_code[g]
                held[g] = tuple(
                    jnp.where(code == float(2 * (n // 4) + n % 2), values[n // 2 % 2], held[g][n])
                    for n in range(12)
                )
        return tuple(held)

    slot(recv1, me)[...] = slot(send1, me)[...]
    drain(recv1, r1_sem.at[0], (peers - 2) * 3 * CAP)
    held = collect(me, ((empty,) * 12,) * coarse_groups)
    held = each_step(1, peers - 1, lambda k, held: collect(source(k), held), held)
    for g in range(coarse_groups):
        for n in range(12):
            held_ref[plane_slot(n, g), :] = held[g][n]
    drain(gmax_in, rg_sem, groups - 1)
    best = gmax[...]
    for k in range(1, groups):
        best = jnp.maximum(best, gmax_in[pl.ds(lax.rem(mg + k, groups), 1), :])
    tops[pl.ds(me, 1), :] = jnp.broadcast_to(jnp.max(best, axis=1, keepdims=True), (1, LANES))
    each_peer(lambda p: outt(p).start())
    drain(recv1, r1_sem.at[1], 3 * CAP)
    held = tuple(
        tuple(held_ref[plane_slot(n, g), :] for n in range(12)) for g in range(coarse_groups)
    )
    held = collect(source(jnp.int32(peers - 1)), held)
    spread = row16
    squeeze = EDGE * k8
    upper8 = k_of >= HALF

    def known(v):
        return v < BIG

    def chosen(v, other):
        return jnp.where(known(v), v, other)

    for g in range(coarse_groups):
        for n in range(12):
            held_ref[plane_slot(n, g), :] = held[g][n]
        sent = [[[held[g][4 * d + 2 * w + q] for q in range(2)] for w in range(2)] for d in range(3)]
        base = [
            [
                [chosen(sent[d][w][q], plane_e[plane_slot(4 * d + 2 * w + q, g), :]) for q in range(2)]
                for w in range(2)
            ]
            for d in range(3)
        ]
        now = [[list(base[d][w]) for w in range(2)] for d in range(3)]
        ahead = [[[None] * 2 for w in range(2)] for d in range(3)]
        for q in range(2):
            over = roll(sent[2][1][0], -HALF * q)
            now[0][0][q] = jnp.where(first_z, chosen(over, base[0][0][q]), base[0][0][q])
            wrap = chosen(roll(sent[2][1][0], EDGE - 1 - HALF * q), roll(base[0][0][q], EDGE - 1))
            ahead[0][0][q] = jnp.where(last_z, wrap, roll(base[0][0][q], -1))

            over = take(sent[2][0][q], spread)
            now[1][0][q] = jnp.where(first_z, chosen(over, base[1][0][q]), base[1][0][q])
            wrap = chosen(over, roll(base[1][0][q], EDGE - 1))
            ahead[1][0][q] = jnp.where(last_z, wrap, roll(base[1][0][q], -1))

            under = take(sent[1][0][q], squeeze)
            free = known(under) & (sent[2][0][q] >= BIG) & (lane < HALF)
            now[2][0][q] = jnp.where(free, under, base[2][0][q])
            free = known(under) & (roll(sent[2][0][q], LANES - HALF) >= BIG)
            wrap = jnp.where(free, under, roll(base[2][0][q], LANES - HALF))
            wrap = jnp.where(upper8, wrap, roll(base[2][0][q], LANES - EDGE - HALF))
            ahead[2][0][q] = jnp.where(last_y, wrap, roll(base[2][0][q], -EDGE))

        over, under = sent[1][1][0], sent[0][1][0]
        now[0][1][0] = jnp.where(first_y, chosen(over, base[0][1][0]), base[0][1][0])
        free = known(under) & (over >= BIG) & first_y
        now[1][1][0] = jnp.where(free, under, base[1][1][0])
        over, under = roll(over, -EDGE), roll(under, -EDGE)
        turned = [[roll(base[d][1][q], -EDGE) for q in range(2)] for d in range(2)]
        wrap = (chosen(over, turned[0][0]), jnp.where(known(under) & (over >= BIG), under, turned[1][0]))
        for d in range(2):
            ahead[d][1] = [
                jnp.where(last_y, turned[d][1], turned[d][0]),
                jnp.where(last_y, wrap[d], turned[d][1]),
            ]

        under = jnp.where(upper8, roll(sent[0][0][1], HALF), sent[0][0][0])
        free = known(under) & (sent[2][1][0] >= BIG) & (k8 == 0)
        now[2][1][0] = jnp.where(free, under, base[2][1][0])
        under = jnp.where(upper8, roll(sent[0][0][1], EDGE - 1), roll(sent[0][0][0], HALF - 1))
        free = known(under) & (roll(sent[2][1][0], HALF - 1) >= BIG)
        turned = [roll(base[2][1][q], HALF - 1) for q in range(2)]
        wrap = (turned[1], jnp.where(free, under, turned[0]))
        for q in range(2):
            ahead[2][1][q] = jnp.where(k8 == HALF - 1, wrap[q], roll(base[2][1][q], -1))

        for d in range(3):
            left, right = sub2(ahead[d][1], now[d][1]), sub2(ahead[d][0], now[d][0])
            curl = sub2(right, left) if d == 1 else sub2(left, right)
            for q in range(2):
                plane_n[plane_slot(2 * d + q, g), :] = curl[q]


    def answer(p):
        rows = zero
        for c in range(CAP):
            key = row_of(recv1, p * ROWS + 2 * CAP + c)
            curl_acc, field_acc = zero, zero
            for g in range(coarse_groups):
                code = key - base_code[g]
                for n in range(6):
                    hit = code == float(n)
                    curl_acc = jnp.where(hit, plane_n[plane_slot(n, g), :], curl_acc)
                    field_acc = jnp.where(hit, plane_b[plane_slot(n, g), :], field_acc)
            rows = jnp.where(sub == c, sum_rows(curl_acc), rows)
            rows = jnp.where(sub == CAP + c, sum_rows(field_acc), rows)
        slot(send2, p)[...] = rows

    def reply(k, carry):
        answer(target(k))
        out2(target(k)).start()
        return carry

    each_step(1, peers, reply)
    answer(me)
    for g in range(coarse_groups):
        for d in range(3):
            for which in range(2):
                axis = TANGENT[d][which]
                for q1 in range(2):
                    value = held_ref[plane_slot(4 * d + 2 * which + q1, g), :]

                    def patch(tile, shift, mask, value=value, axis=axis, g=g):
                        where = (axis, slice(ROWS * g, ROWS * g + ROWS), slice(tile * LANES, tile * LANES + LANES))
                        turned = roll(value, shift)
                        put = turned < BIG
                        if mask is not None:
                            put = put & mask
                        emf_c[where] = jnp.where(put, turned, emf_c[where])

                    if d == 0:
                        patch(q1, 0, None)
                        continue
                    for m in range(HALF):
                        tile = 2 * (q1 * HALF + m)
                        if d == 1:
                            patch(tile, -EDGE * m, first_y)
                        else:
                            for q2 in range(2):
                                patch(tile + q2, -(HALF * q2 + m), first_z)


    def curl_step(n, carry):
        for u in range(4):
            i = 4 * n + u
            after = lax.rem(i + 1, EDGE)
            for g in range(coarse_groups):
                read, put = blocked(emf_c, g), blocked_put(curl_c, g)
                e_x, e_y, e_z = read(0, i), read(1, i), read(2, i)
                put(0, i, sub2(sub2(ahead_y(e_z), e_z), sub2(ahead_z(e_y), e_y)))
                put(1, i, sub2(sub2(ahead_z(e_x), e_x), sub2(read(2, after), e_z)))
                put(2, i, sub2(sub2(read(1, after), e_y), sub2(ahead_y(e_x), e_x)))
        return carry

    lax.fori_loop(0, EDGE // 4, curl_step, 0)

    index_n = (lane, k_of, EDGE * k8)
    target_n = (jnp.zeros_like(lane), row16, row16)

    def pair_normal(r):
        d = pairs[r, 1]
        base = pairs[r, 0] * SPAN + d * TILES
        index, target = by_axis(d, index_n), by_axis(d, target_n)
        upper = k_of >= jnp.where(d == 2, HALF, EDGE)
        for n, ref in enumerate((fb, curl_f)):
            for h in range(2):
                start = base + jnp.where(d == 0, h, 2 * HALF * h)
                got = [take(ref[pl.ds(start + s, ROWS, stride=2), :], index) for s in range(2)]
                value = jnp.where(upper, got[1], got[0])
                picked[pl.ds((2 * n + h) * pair_rows + r, 1), :] = sum_rows(
                    jnp.where(sub == target, value, 0.0)
                )

    each_pair(pair_normal)

    for s in range(0, pair_count, ROWS):
        turned, column_of = jnp.zeros_like(lane), jnp.zeros_like(lane)
        for r in range(s, min(s + ROWS, pair_count)):
            turned = jnp.where(sub == r - s, face_of[r], turned)
            column_of = jnp.where(sub == r - s, pairs[r, 5], column_of)
        for h in range(2):
            m, n = 4 * h + lane // 32, k_of // 2
            index_out[h * pair_rows + s : h * pair_rows + s + ROWS, :] = (
                jnp.where(turned == 2, EDGE * n + m, EDGE * m + n) + HALF * column_of
            )

    drain(tops, rt_sem, peers - 1)
    by = jnp.broadcast_to(
        0.125 * (0.2 / jnp.max(tops[...], axis=0, keepdims=True)), (ROWS, LANES)
    )
    step_out[...] = by

    def finish_coarse(i, carry):
        for g in range(coarse_groups):
            field, curl, put = blocked(cb, g), blocked(curl_c, g), blocked_put(curl_c, g)
            for c in range(3):
                put(c, i, sub2(field(c, i), mul((by, by), curl(c, i))))
        return carry

    lax.fori_loop(0, EDGE, finish_coarse, 0, unroll=4)
    twice = 2.0 * by
    tiles = largest_step(fine_count * SPAN // ROWS, 36)

    def finish_fine(n, carry):
        for u in range(tiles):
            rows = pl.ds(pl.multiple_of((n * tiles + u) * ROWS, ROWS), ROWS)
            curl_f[rows, :] = fb[rows, :] - twice * curl_f[rows, :]
        return carry

    lax.fori_loop(0, fine_count * SPAN // ROWS // tiles, finish_fine, 0)
    for n in range(0, 2 * pair_rows, ROWS):
        far = slice(2 * pair_rows + n, 2 * pair_rows + n + ROWS)
        fine_face[n : n + ROWS, :] = picked[n : n + ROWS, :] - twice * picked[far, :]
    slot(recv2, me)[...] = slot(send2, me)[...]
    drain(recv2, r2_sem, (peers - 1) * 2 * CAP)
    for r in range(pair_count):
        row = owner_of[r] * ROWS + rank_of[r]
        own_a[r : r + 1, :] = recv2[pl.ds(row, 1), :]
        own_b[r : r + 1, :] = recv2[pl.ds(row + CAP, 1), :]
    drain(fb, sent_sem, (peers - 1) * (5 * CAP + 1) + groups - 1)


def store(new_c, new_f, fine_face, own_a, own_b, index, step, out_c, out_f, out_j, new_j, sems):
    copies = [
        pltpu.make_async_copy(src, dst, sems.at[n])
        for n, (src, dst) in enumerate(((new_c, out_c), (new_f, out_f)))
    ]
    for copy in copies:
        copy.start()
    count, pair_rows = out_j.shape[0], own_a.shape[0]
    for s in range(0, count, ROWS):
        coarse = own_b[s : s + ROWS, :] - step[...] * own_a[s : s + ROWS, :]
        for h in range(2):
            here = slice(h * pair_rows + s, h * pair_rows + s + ROWS)
            new_j[s : s + ROWS, h * LANES : (h + 1) * LANES] = fine_face[here, :] - take(
                coarse, index[here, :]
            )
    copies.append(pltpu.make_async_copy(new_j.at[pl.ds(0, count)], out_j, sems.at[2]))
    copies[-1].start()
    for copy in copies:
        copy.wait()


def on_device(peers, groups, coarse_field, coarse_velocity, fine_field, fine_velocity, pairs):
    coarse_count, fine_count = coarse_field.shape[1], fine_field.shape[1]
    pair_count = pairs.shape[1]
    cells = EDGE**3
    flat_rows = fine_count * SPAN

    def coarse_view(x):
        return jnp.transpose(x[0], (1, 0, 2))

    def fine_view(x):
        return x.reshape(flat_rows, LANES)

    pair_rows = ROWS * -(-pair_count // ROWS)
    operands = [
        pltpu.with_memory_space_constraint(x, pltpu.HBM)
        for x in (
            pairs[0],
            coarse_view(coarse_field),
            coarse_view(coarse_velocity),
            fine_view(fine_field),
            fine_view(fine_velocity),
        )
    ]
    f32 = jnp.float32
    dma = pltpu.SemaphoreType.DMA
    vmem = pltpu.VMEM
    anywhere = pl.BlockSpec(memory_space=pltpu.HBM)
    inside = pl.BlockSpec(memory_space=pltpu.VMEM)
    coarse_shape, fine_shape = (3, coarse_count, cells), (flat_rows, LANES)
    shapes = (
        coarse_shape,
        fine_shape,
        (2 * pair_rows, LANES),
        (pair_rows, LANES),
        (pair_rows, LANES),
        (2 * pair_rows, LANES),
        (ROWS, LANES),
    )
    kinds = [f32] * 5 + [jnp.int32, f32]
    results = pl.pallas_call(
        functools.partial(kernel, peers, groups, coarse_count, fine_count, pair_count),
        out_shape=tuple(jax.ShapeDtypeStruct(s, k) for s, k in zip(shapes, kinds)),
        in_specs=[anywhere] * 5,
        out_specs=(inside,) * len(shapes),
        scratch_shapes=[
            pltpu.SMEM(pairs.shape[1:], jnp.int32),
            vmem(coarse_shape, f32),
            vmem(coarse_shape, f32),
            vmem(fine_shape, f32),
            vmem(fine_shape, f32),
            vmem(coarse_shape, f32),
            vmem((pair_count * SPAN, LANES), f32),
            vmem((6 * EDGE * coarse_count, LANES), f32),
            vmem((2 * EDGE * coarse_count, LANES), f32),
            vmem((12 * coarse_count, LANES), f32),
            vmem((6 * coarse_count, LANES), f32),
            vmem((6 * coarse_count, LANES), f32),
            vmem((12 * coarse_count, LANES), f32),
            vmem((4 * pair_rows, LANES), f32),
            vmem((peers, LANES), f32),
            vmem((4 * pair_rows, LANES), f32),
            vmem((peers * ROWS, LANES), f32),
            vmem((peers * ROWS, LANES), f32),
            vmem((peers * ROWS, LANES), f32),
            vmem((peers * ROWS, LANES), f32),
            vmem((1, LANES), f32),
            vmem((groups, LANES), f32),
            dma((5,)),
            dma,
            dma((2,)),
            dma,
            dma,
            dma,
        ],
        compiler_params=pltpu.CompilerParams(
            collective_id=0, has_side_effects=True, vmem_limit_bytes=32 * 1024 * 1024
        ),
    )(*operands)
    coarse_out, fine_out, jump = pl.pallas_call(
        store,
        out_shape=(
            jax.ShapeDtypeStruct(coarse_shape, f32),
            jax.ShapeDtypeStruct(fine_shape, f32),
            jax.ShapeDtypeStruct((pair_count, EDGE * EDGE), f32),
        ),
        in_specs=[inside] * len(shapes),
        out_specs=(anywhere,) * 3,
        scratch_shapes=[
            vmem((pair_rows, EDGE * EDGE), f32),
            dma((3,)),
        ],
    )(*(pltpu.with_memory_space_constraint(x, pltpu.VMEM) for x in results))
    return (
        jnp.transpose(coarse_out, (1, 0, 2))[None],
        fine_out.reshape(1, fine_count, 3, cells),
        jump[None],
    )


def solution(mesh):
    spec = P("gz", "blocks", None, None)
    flat = P("gz", "blocks", None)
    return jax.shard_map(
        functools.partial(on_device, mesh.shape["blocks"], mesh.shape["gz"]),
        mesh=mesh,
        in_specs=(spec, spec, spec, spec, flat),
        out_specs=(spec, spec, flat),
        check_vma=False,
    )
```

```python
import functools

import jax
import jax.numpy as jnp
from jax import lax
from jax.experimental import pallas as pl
from jax.experimental.pallas import tpu as pltpu
from jax.sharding import PartitionSpec as P

EDGE = 16
HALF = 8
CAP = 2
LANES = 128
ROWS = 8
TILES = EDGE**3 // LANES
SPAN = 3 * TILES
TINY = 1.2e-38
BIG = 1e30
EMPTY = 3e38
TANGENT = ((1, 2), (0, 2), (0, 1))
MESH = pl.DeviceIdType.MESH
TOP_CHUNK = 4
CHUNK = 4
CHUNKS = EDGE // CHUNK
FINE_STEP = 4
SPEED_STEP = 6


def take(values, index):
    return jnp.take_along_axis(values, index, axis=1, mode="promise_in_bounds")


def largest_step(count, most):
    return max(n for n in range(1, most + 1) if count % n == 0)


def kernel(
    peers,
    groups,
    coarse_count,
    fine_count,
    pair_count,
    pairs_hbm,
    cb_hbm,
    cv_hbm,
    fb_hbm,
    fv_hbm,
    curl_c,
    curl_f,
    fine_face,
    own_a,
    own_b,
    index_out,
    step_out,
    pairs,
    cb,
    cv,
    fb,
    fv,
    emf_c,
    emf_p,
    centred,
    halfway,
    plane_e,
    plane_b,
    plane_n,
    held_ref,
    picked,
    tops,
    rows1,
    send1,
    recv1,
    relayed,
    send2,
    recv2,
    gmax,
    gmax_in,
    load_sem,
    sent_sem,
    s1_sem,
    bundle_sem,
    go_sem,
    r1_sem,
    r2_sem,
    rg_sem,
    rt_sem,
):
    me = lax.axis_index("blocks")
    mg = lax.axis_index("gz")
    few = peers <= 8
    coarse_groups = coarse_count // ROWS
    pair_rows = ROWS * -(-pair_count // ROWS)

    paired = peers & (peers - 1) == 0
    flips = []
    for n in range(peers.bit_length() - 1):
        bit = 1 << n
        flips.append((bit, bit * (1 - 2 * lax.rem(lax.div(me, bit), 2))))

    def target(k):
        if not paired:
            return lax.rem(me + k, peers)
        return sum((lax.rem(lax.div(k, bit), 2) * flip for bit, flip in flips), me)

    def source(k):
        return target(k) if paired else lax.rem(me + peers - k, peers)

    def each_step(first, last, body, carry=0):
        if few:
            for k in range(last - 1, first - 1, -1):
                carry = body(k, carry)
            return carry
        return lax.fori_loop(0, last - first, lambda n, c: body(last - 1 - n, c), carry)

    def each_peer(body):
        each_step(1, peers, lambda k, _: (body(target(k)), 0)[1])

    def each_group(body):
        for k in range(1, groups):
            body(lax.rem(mg + k, groups))

    barrier = pltpu.get_barrier_semaphore()
    relay = paired and few and peers > 2
    early = peers // 2 if relay else 0
    greeted = peers - 1 + groups - 1

    def greet(p):
        at = jnp.where(jnp.logical_and(p == 0, me > 1), 1, p) if relay else p
        pl.semaphore_signal(barrier, inc=1, device_id=(at, mg), device_id_type=MESH)

    each_peer(greet)
    loads = [
        pltpu.make_async_copy(src, dst, load_sem.at[n])
        for n, (src, dst) in enumerate(((fb_hbm, fb), (fv_hbm, fv), (cb_hbm, cb), (cv_hbm, cv)))
    ]
    listed = pltpu.make_async_copy(pairs_hbm, pairs, load_sem.at[4])
    listed.start()
    for load in loads:
        load.start()
    me_or_one = jnp.where(me == 0, 1, me) if relay else me
    each_group(
        lambda g: pl.semaphore_signal(barrier, inc=1, device_id=(me_or_one, g), device_id_type=MESH)
    )

    lane = lax.broadcasted_iota(jnp.int32, (ROWS, LANES), 1)
    sub = lax.broadcasted_iota(jnp.int32, (ROWS, LANES), 0)
    zero = jnp.zeros((ROWS, LANES), jnp.float32)
    row16 = lane // EDGE
    k_of = lane % EDGE
    k8 = lane % HALF
    first_y = lane < EDGE
    last_y = lane >= LANES - EDGE
    first_z = k_of == 0
    last_z = k_of == EDGE - 1
    first_x = sub == 0
    last_x = sub == ROWS - 1

    def roll(v, shift):
        return v if shift % LANES == 0 else pltpu.roll(v, shift % LANES, 1)

    def back_y(pair):
        low, high = roll(pair[0], EDGE), roll(pair[1], EDGE)
        return jnp.where(first_y, high, low), jnp.where(first_y, low, high)

    def ahead_y(pair):
        low, high = roll(pair[0], -EDGE), roll(pair[1], -EDGE)
        return jnp.where(last_y, high, low), jnp.where(last_y, low, high)

    def back_z(pair):
        return tuple(jnp.where(first_z, roll(v, 1 - EDGE), roll(v, 1)) for v in pair)

    def ahead_z(pair):
        return tuple(jnp.where(last_z, roll(v, EDGE - 1), roll(v, -1)) for v in pair)

    def add(a, b):
        return tuple(x + y for x, y in zip(a, b))

    def sub2(a, b):
        return tuple(x - y for x, y in zip(a, b))

    def mul(a, b):
        return tuple(x * y for x, y in zip(a, b))

    def quad(f):
        return lambda q: f(q[:2]) + f(q[2:])

    def back_x(q):
        r = [pltpu.roll(v, 1, 0) for v in q]
        return tuple(jnp.where(first_x, r[n ^ 2], r[n]) for n in range(4))

    def ahead_x(q):
        r = [pltpu.roll(v, ROWS - 1, 0) for v in q]
        return tuple(jnp.where(last_x, r[n ^ 2], r[n]) for n in range(4))

    def top_of(v, c):
        out = []
        for n in range(len(v[0])):
            vv = (v[0][n] * v[0][n] + v[1][n] * v[1][n]) + v[2][n] * v[2][n]
            cc = (c[0][n] * c[0][n] + c[1][n] * c[1][n]) + c[2][n] * c[2][n]
            root_v = vv * lax.rsqrt(jnp.maximum(vv, TINY))
            root_c = cc * lax.rsqrt(jnp.maximum(cc, TINY))
            out.append(root_v + 0.5 * root_c)
        return functools.reduce(jnp.maximum, out)

    def cells(v, c):
        return (
            sub2(mul(v[2], c[1]), mul(v[1], c[2])),
            sub2(mul(v[0], c[2]), mul(v[2], c[0])),
            sub2(mul(v[1], c[0]), mul(v[0], c[1])),
        )

    def fine_read(ref, base):
        return tuple(
            tuple(
                ref[pl.ds(base + c * TILES + 2 * HALF * ih + h, ROWS, stride=2), :]
                for ih in range(2)
                for h in range(2)
            )
            for c in range(3)
        )

    def fine_put(ref, base, values):
        for c in range(3):
            for ih in range(2):
                for h in range(2):
                    ref[pl.ds(base + c * TILES + 2 * HALF * ih + h, ROWS, stride=2), :] = values[c][
                        2 * ih + h
                    ]

    def fine_centre(b):
        return (add(b[0], ahead_x(b[0])), add(b[1], quad(ahead_y)(b[1])), add(b[2], quad(ahead_z)(b[2])))

    def fine_edges(b, v):
        cell = cells(v, fine_centre(b))
        part_x = add(cell[0], quad(back_y)(cell[0]))
        part_y = add(cell[1], quad(back_z)(cell[1]))
        part_z = add(cell[2], quad(back_y)(cell[2]))
        return (
            add(part_x, quad(back_z)(part_x)),
            add(part_y, back_x(part_y)),
            add(part_z, back_x(part_z)),
        )

    def fine_curl(e):
        return (
            sub2(sub2(quad(ahead_y)(e[2]), e[2]), sub2(quad(ahead_z)(e[1]), e[1])),
            sub2(sub2(quad(ahead_z)(e[0]), e[0]), sub2(ahead_x(e[2]), e[2])),
            sub2(sub2(ahead_x(e[1]), e[1]), sub2(quad(ahead_y)(e[0]), e[0])),
        )

    def by_axis(d, values):
        return jnp.where(d == 0, values[0], jnp.where(d == 1, values[1], values[2]))

    def sum_rows(v):
        return jnp.sum(v, axis=0, keepdims=True)

    def column(tile):
        return pl.ds(pl.multiple_of(tile * LANES, LANES), LANES)

    def blocked(ref, g):
        def read(c, i):
            return tuple(ref[c, ROWS * g : ROWS * g + ROWS, column(2 * i + h)] for h in range(2))

        return read

    def blocked_put(ref, g):
        def put(c, i, pair):
            for h in range(2):
                ref[c, ROWS * g : ROWS * g + ROWS, column(2 * i + h)] = pair[h]

        return put

    loads[0].wait()
    loads[1].wait()

    speed_step = largest_step(fine_count, SPEED_STEP)

    def fine_top(n, best):
        for u in range(speed_step):
            base = (n * speed_step + u) * SPAN
            b, v = fine_read(fb, base), fine_read(fv, base)
            best = jnp.maximum(best, top_of(v, fine_centre(b)))
        return best

    best = lax.fori_loop(0, fine_count // speed_step, fine_top, zero)

    loads[2].wait()
    loads[3].wait()


    def at(n, i, g, h):
        row = (((n * coarse_groups + g) * EDGE + i) * 2 + h) * ROWS
        return pl.ds(row if isinstance(row, int) else pl.multiple_of(row, ROWS), ROWS)

    def each_plane(chunk, planes, body):
        for u in range(planes):
            for g in range(coarse_groups):
                body(chunk * planes + u, g)

    def coarse_top(n, best):
        tops = []

        def plane(i, g):
            field = blocked(cb, g)
            b = [field(c, i) for c in range(3)]
            c = (
                add(b[0], field(0, lax.rem(i + 1, EDGE))),
                add(b[1], ahead_y(b[1])),
                add(b[2], ahead_z(b[2])),
            )
            for k in range(3):
                for h in range(2):
                    centred[at(k, i, g, h), :] = c[k][h]
            tops.append(top_of([blocked(cv, g)(k, i) for k in range(3)], c))

        each_plane(n, TOP_CHUNK, plane)
        return functools.reduce(jnp.maximum, tops, best)

    best = lax.fori_loop(0, EDGE // TOP_CHUNK, coarse_top, best)
    gmax[...] = jnp.max(best, axis=0, keepdims=True)

    def slot(ref, p):
        return ref.at[pl.ds(pl.multiple_of(p * ROWS, ROWS), ROWS)]

    def part(ref, p, rows):
        return ref.at[pl.ds(pl.multiple_of(p * ROWS, ROWS), rows)]

    def out1(k):
        p = target(k)
        return pltpu.make_async_remote_copy(
            src_ref=part(send1, p, 3 * CAP), dst_ref=part(recv1, me, 3 * CAP), send_sem=s1_sem,
            recv_sem=r1_sem.at[k // (peers - 1)], device_id=(p, mg), device_id_type=MESH,
        )

    def out2(p):
        return pltpu.make_async_remote_copy(
            src_ref=part(send2, p, 2 * CAP), dst_ref=part(recv2, me, 2 * CAP), send_sem=sent_sem,
            recv_sem=r2_sem, device_id=(p, mg), device_id_type=MESH,
        )

    def outg(g):
        return pltpu.make_async_remote_copy(
            src_ref=gmax, dst_ref=gmax_in.at[pl.ds(mg, 1)], send_sem=sent_sem,
            recv_sem=rg_sem, device_id=(me, g), device_id_type=MESH,
        )

    def outt(p):
        return pltpu.make_async_remote_copy(
            src_ref=tops.at[pl.ds(me, 1)], dst_ref=tops.at[pl.ds(me, 1)], send_sem=sent_sem,
            recv_sem=rt_sem, device_id=(p, mg), device_id_type=MESH,
        )

    def drain(ref, sem, rows):
        whole = ref.at[pl.ds(0, rows)]
        pltpu.make_async_copy(whole, whole, sem).wait()

    def out_bundle():
        rows = pl.ds(2 * ROWS, (peers - 2) * ROWS)
        return pltpu.make_async_remote_copy(
            src_ref=send1.at[rows], dst_ref=relayed.at[rows], send_sem=s1_sem,
            recv_sem=bundle_sem, device_id=(1, mg), device_id_type=MESH,
        )

    def out_relay(p):
        return pltpu.make_async_remote_copy(
            src_ref=part(relayed, p, 3 * CAP), dst_ref=part(recv1, 0, 3 * CAP), send_sem=s1_sem,
            recv_sem=r1_sem.at[p // (peers - 1)], device_id=(p, mg), device_id_type=MESH,
        )

    def send_all():
        each_step(1, peers, lambda k, _: (out1(k).start(), 0)[1])

    def send_group():
        each_group(lambda g: outg(g).start())


    @pl.when(me >= early)
    def _():
        pl.semaphore_wait(barrier, greeted)
        send_group()

    listed.wait()

    half_lane = 32 * (row16 % 4)
    index_r = (half_lane + 2 * k8, 2 * k8, half_lane)
    target_r = (jnp.zeros_like(lane), row16, k8)

    def pair_edges(r):
        base = pairs[r, 0] * SPAN
        fine_put(emf_p, r * SPAN, fine_edges(fine_read(fb, base), fine_read(fv, base)))

    def pair_restrict(r):
        d = pairs[r, 1]
        index, target = by_axis(d, index_r), by_axis(d, target_r)
        upper = lane >= jnp.where(d == 1, LANES, 64)
        for which in range(2):
            axis = jnp.where(d == 0, 1, 0) if which == 0 else jnp.where(d == 2, 1, 2)
            base = r * SPAN + axis * TILES
            got = []
            for h in range(2):
                here = emf_p[pl.ds(base + h, ROWS, stride=4), :]
                if which == 0:
                    there = jnp.where(
                        d == 0, roll(here, -EDGE), emf_p[pl.ds(base + h + 2, ROWS, stride=4), :]
                    )
                else:
                    there = jnp.where(d == 2, roll(here, -EDGE), roll(here, -1))
                got.append(take(0.5 * (here + there), index))
            value = jnp.where(upper, got[1], got[0])
            rows1[pl.ds(4 * r + which, 1), :] = sum_rows(jnp.where(sub == target, value, 0.0))
        code = (pairs[r, 3] * 6 + d * 2 + pairs[r, 4]).astype(jnp.float32)
        key = jnp.where((lane[:1] // HALF) % 2 == pairs[r, 5], code, -1.0)
        rows1[pl.ds(4 * r + 2, 1), :] = key

    def each_pair(body):
        if pair_count <= 4:
            for r in range(pair_count):
                body(r)
        else:
            lax.fori_loop(0, pair_count, lambda r, _: (body(r), 0)[1], 0)

    each_pair(pair_edges)
    each_pair(pair_restrict)

    slot_of = [pairs[r, 0] for r in range(pair_count)]
    face_of = [pairs[r, 1] for r in range(pair_count)]
    owner_of = [pairs[r, 2] for r in range(pair_count)]
    rank_of = []
    for r in range(pair_count):
        rank = jnp.int32(0)
        for q in range(r):
            rank = rank + jnp.where(owner_of[q] == owner_of[r], 1, 0)
        rank_of.append(rank)

    def build(p, carry):
        message = jnp.full((ROWS, LANES), -1.0, jnp.float32)
        for r in range(pair_count):
            here = jnp.where(owner_of[r] == p, rank_of[r], ROWS)
            for n, row in enumerate((2 * here, 2 * here + 1, 2 * CAP + here)):
                message = jnp.where(
                    sub == row, jnp.broadcast_to(rows1[4 * r + n : 4 * r + n + 1, :], (ROWS, LANES)), message
                )
        slot(send1, p)[...] = message
        return carry

    lax.fori_loop(0, peers, build, 0, unroll=few)

    if relay:

        @pl.when(me == 0)
        def _():
            pl.semaphore_wait(barrier, 1)
            out1(1).start()
            out_bundle().start()

        @pl.when(me == 1)
        def _():
            pl.semaphore_wait(barrier, greeted + groups - 1 + peers - 2)
            pl.semaphore_signal(go_sem, inc=1, device_id=(0, mg), device_id_type=MESH)
            rows = relayed.at[pl.ds(2 * ROWS, (peers - 2) * ROWS)]
            pltpu.make_async_copy(rows, rows, bundle_sem).wait()
            for p in range(peers - 1, 1, -1):
                out_relay(p).start()

        @pl.when(jnp.logical_and(me > 1, me < early))
        def _():
            pl.semaphore_wait(barrier, greeted)

        @pl.when(me > 0)
        def _():
            send_all()


        @pl.when(me == 0)
        def _():
            pl.semaphore_wait(go_sem, 1)

        @pl.when(me < early)
        def _():
            send_group()

    else:
        send_all()


    def coarse_step(t, parts):
        parts = list(parts)

        def last(i, g):
            part_x = tuple(halfway[at(0, i, g, h), :] for h in range(2))
            blocked_put(emf_c, g)(0, i, add(part_x, back_z(part_x)))

        def first(i, g):
            put = blocked_put(emf_c, g)
            c = [tuple(centred[at(n, i, g, h), :] for h in range(2)) for n in range(3)]
            cell = cells([blocked(cv, g)(n, i) for n in range(3)], c)
            part_x = add(cell[0], back_y(cell[0]))
            part_y = add(cell[1], back_z(cell[1]))
            part_z = add(cell[2], back_y(cell[2]))
            for h in range(2):
                halfway[at(0, i, g, h), :] = part_x[h]
            put(1, i, add(part_y, parts[g][0]))
            put(2, i, add(part_z, parts[g][1]))
            parts[g] = (part_y, part_z)

        each_plane(lax.rem(t + CHUNKS - 1, CHUNKS), CHUNK, last)
        each_plane(lax.rem(t, CHUNKS), CHUNK, first)
        return tuple(parts)

    nothing = ((zero, zero), (zero, zero))
    lax.fori_loop(0, CHUNKS + 1, coarse_step, (nothing,) * coarse_groups)


    def packed(read, c, d, q1):
        if d == 0:
            return read(c, 0)[q1]
        out = zero
        for m in range(HALF):
            tiles = read(c, q1 * HALF + m)
            if d == 1:
                out = jnp.where(row16 == m, roll(tiles[0], EDGE * m), out)
            else:
                for q2 in range(2):
                    out = jnp.where(k_of == HALF * q2 + m, roll(tiles[q2], HALF * q2 + m), out)
        return out

    def plane_slot(n, g):
        at = (n * coarse_groups + g) * ROWS
        return slice(at, at + ROWS)

    for g in range(coarse_groups):
        for d in range(3):
            for q1 in range(2):
                plane_b[plane_slot(2 * d + q1, g), :] = packed(blocked(cb, g), d, d, q1)
                for which in range(2):
                    plane_e[plane_slot(4 * d + 2 * which + q1, g), :] = packed(
                        blocked(emf_c, g), TANGENT[d][which], d, q1
                    )

    fine_step = largest_step(fine_count, FINE_STEP)

    def fine_bulk(n, carry):
        for u in range(fine_step):
            base = (n * fine_step + u) * SPAN
            fine_put(curl_f, base, fine_curl(fine_edges(fine_read(fb, base), fine_read(fv, base))))
        return carry

    lax.fori_loop(0, fine_count // fine_step, fine_bulk, 0)

    def row_of(ref, n):
        return jnp.broadcast_to(ref[pl.ds(n, 1), :], (ROWS, LANES))

    base_code = [((sub + ROWS * g) * 6).astype(jnp.float32) for g in range(coarse_groups)]
    empty = jnp.full((ROWS, LANES), EMPTY, jnp.float32)

    def collect(p, held):
        held = list(held)
        for c in range(CAP):
            key = row_of(recv1, p * ROWS + 2 * CAP + c)
            values = [row_of(recv1, p * ROWS + 2 * c + which) for which in range(2)]
            for g in range(coarse_groups):
                code = key - base_code[g]
                held[g] = tuple(
                    jnp.where(code == float(2 * (n // 4) + n % 2), values[n // 2 % 2], held[g][n])
                    for n in range(12)
                )
        return tuple(held)

    drain(gmax_in, rg_sem, groups - 1)
    best = gmax[...]
    for k in range(1, groups):
        best = jnp.maximum(best, gmax_in[pl.ds(lax.rem(mg + k, groups), 1), :])
    tops[pl.ds(me, 1), :] = jnp.broadcast_to(jnp.max(best, axis=1, keepdims=True), (1, LANES))
    each_peer(lambda p: outt(p).start())
    slot(recv1, me)[...] = slot(send1, me)[...]
    drain(recv1, r1_sem.at[0], (peers - 2) * 3 * CAP)
    held = collect(me, ((empty,) * 12,) * coarse_groups)
    held = each_step(1, peers - 1, lambda k, held: collect(source(k), held), held)
    for g in range(coarse_groups):
        for n in range(12):
            held_ref[plane_slot(n, g), :] = held[g][n]
    drain(recv1, r1_sem.at[1], 3 * CAP)
    held = tuple(
        tuple(held_ref[plane_slot(n, g), :] for n in range(12)) for g in range(coarse_groups)
    )
    held = collect(source(jnp.int32(peers - 1)), held)
    spread = row16
    squeeze = EDGE * k8
    upper8 = k_of >= HALF

    def known(v):
        return v < BIG

    def chosen(v, other):
        return jnp.where(known(v), v, other)

    for g in range(coarse_groups):
        for n in range(12):
            held_ref[plane_slot(n, g), :] = held[g][n]
        sent = [[[held[g][4 * d + 2 * w + q] for q in range(2)] for w in range(2)] for d in range(3)]
        base = [
            [
                [chosen(sent[d][w][q], plane_e[plane_slot(4 * d + 2 * w + q, g), :]) for q in range(2)]
                for w in range(2)
            ]
            for d in range(3)
        ]
        now = [[list(base[d][w]) for w in range(2)] for d in range(3)]
        ahead = [[[None] * 2 for w in range(2)] for d in range(3)]
        for q in range(2):
            over = roll(sent[2][1][0], -HALF * q)
            now[0][0][q] = jnp.where(first_z, chosen(over, base[0][0][q]), base[0][0][q])
            wrap = chosen(roll(sent[2][1][0], EDGE - 1 - HALF * q), roll(base[0][0][q], EDGE - 1))
            ahead[0][0][q] = jnp.where(last_z, wrap, roll(base[0][0][q], -1))

            over = take(sent[2][0][q], spread)
            now[1][0][q] = jnp.where(first_z, chosen(over, base[1][0][q]), base[1][0][q])
            wrap = chosen(over, roll(base[1][0][q], EDGE - 1))
            ahead[1][0][q] = jnp.where(last_z, wrap, roll(base[1][0][q], -1))

            under = take(sent[1][0][q], squeeze)
            free = known(under) & (sent[2][0][q] >= BIG) & (lane < HALF)
            now[2][0][q] = jnp.where(free, under, base[2][0][q])
            free = known(under) & (roll(sent[2][0][q], LANES - HALF) >= BIG)
            wrap = jnp.where(free, under, roll(base[2][0][q], LANES - HALF))
            wrap = jnp.where(upper8, wrap, roll(base[2][0][q], LANES - EDGE - HALF))
            ahead[2][0][q] = jnp.where(last_y, wrap, roll(base[2][0][q], -EDGE))

        over, under = sent[1][1][0], sent[0][1][0]
        now[0][1][0] = jnp.where(first_y, chosen(over, base[0][1][0]), base[0][1][0])
        free = known(under) & (over >= BIG) & first_y
        now[1][1][0] = jnp.where(free, under, base[1][1][0])
        over, under = roll(over, -EDGE), roll(under, -EDGE)
        turned = [[roll(base[d][1][q], -EDGE) for q in range(2)] for d in range(2)]
        wrap = (chosen(over, turned[0][0]), jnp.where(known(under) & (over >= BIG), under, turned[1][0]))
        for d in range(2):
            ahead[d][1] = [
                jnp.where(last_y, turned[d][1], turned[d][0]),
                jnp.where(last_y, wrap[d], turned[d][1]),
            ]

        under = jnp.where(upper8, roll(sent[0][0][1], HALF), sent[0][0][0])
        free = known(under) & (sent[2][1][0] >= BIG) & (k8 == 0)
        now[2][1][0] = jnp.where(free, under, base[2][1][0])
        under = jnp.where(upper8, roll(sent[0][0][1], EDGE - 1), roll(sent[0][0][0], HALF - 1))
        free = known(under) & (roll(sent[2][1][0], HALF - 1) >= BIG)
        turned = [roll(base[2][1][q], HALF - 1) for q in range(2)]
        wrap = (turned[1], jnp.where(free, under, turned[0]))
        for q in range(2):
            ahead[2][1][q] = jnp.where(k8 == HALF - 1, wrap[q], roll(base[2][1][q], -1))

        for d in range(3):
            left, right = sub2(ahead[d][1], now[d][1]), sub2(ahead[d][0], now[d][0])
            curl = sub2(right, left) if d == 1 else sub2(left, right)
            for q in range(2):
                plane_n[plane_slot(2 * d + q, g), :] = curl[q]


    def answer(p):
        rows = zero
        for c in range(CAP):
            key = row_of(recv1, p * ROWS + 2 * CAP + c)
            curl_acc, field_acc = zero, zero
            for g in range(coarse_groups):
                code = key - base_code[g]
                for n in range(6):
                    hit = code == float(n)
                    curl_acc = jnp.where(hit, plane_n[plane_slot(n, g), :], curl_acc)
                    field_acc = jnp.where(hit, plane_b[plane_slot(n, g), :], field_acc)
            rows = jnp.where(sub == c, sum_rows(curl_acc), rows)
            rows = jnp.where(sub == CAP + c, sum_rows(field_acc), rows)
        slot(send2, p)[...] = rows

    def reply(k, carry):
        answer(target(k))
        out2(target(k)).start()
        return carry

    each_step(1, peers, reply)
    answer(me)
    for g in range(coarse_groups):
        for d in range(3):
            for which in range(2):
                axis = TANGENT[d][which]
                for q1 in range(2):
                    value = held_ref[plane_slot(4 * d + 2 * which + q1, g), :]

                    def patch(tile, shift, mask, value=value, axis=axis, g=g):
                        where = (axis, slice(ROWS * g, ROWS * g + ROWS), slice(tile * LANES, tile * LANES + LANES))
                        turned = roll(value, shift)
                        put = turned < BIG
                        if mask is not None:
                            put = put & mask
                        emf_c[where] = jnp.where(put, turned, emf_c[where])

                    if d == 0:
                        patch(q1, 0, None)
                        continue
                    for m in range(HALF):
                        tile = 2 * (q1 * HALF + m)
                        if d == 1:
                            patch(tile, -EDGE * m, first_y)
                        else:
                            for q2 in range(2):
                                patch(tile + q2, -(HALF * q2 + m), first_z)


    def curl_step(n, carry):
        for u in range(4):
            i = 4 * n + u
            after = lax.rem(i + 1, EDGE)
            for g in range(coarse_groups):
                read, put = blocked(emf_c, g), blocked_put(curl_c, g)
                e_x, e_y, e_z = read(0, i), read(1, i), read(2, i)
                put(0, i, sub2(sub2(ahead_y(e_z), e_z), sub2(ahead_z(e_y), e_y)))
                put(1, i, sub2(sub2(ahead_z(e_x), e_x), sub2(read(2, after), e_z)))
                put(2, i, sub2(sub2(read(1, after), e_y), sub2(ahead_y(e_x), e_x)))
        return carry

    lax.fori_loop(0, EDGE // 4, curl_step, 0)

    index_n = (lane, k_of, EDGE * k8)
    target_n = (jnp.zeros_like(lane), row16, row16)

    def pair_normal(r):
        d = pairs[r, 1]
        base = pairs[r, 0] * SPAN + d * TILES
        index, target = by_axis(d, index_n), by_axis(d, target_n)
        upper = k_of >= jnp.where(d == 2, HALF, EDGE)
        for n, ref in enumerate((fb, curl_f)):
            for h in range(2):
                start = base + jnp.where(d == 0, h, 2 * HALF * h)
                got = [take(ref[pl.ds(start + s, ROWS, stride=2), :], index) for s in range(2)]
                value = jnp.where(upper, got[1], got[0])
                picked[pl.ds((2 * n + h) * pair_rows + r, 1), :] = sum_rows(
                    jnp.where(sub == target, value, 0.0)
                )

    each_pair(pair_normal)

    for s in range(0, pair_count, ROWS):
        turned, column_of = jnp.zeros_like(lane), jnp.zeros_like(lane)
        for r in range(s, min(s + ROWS, pair_count)):
            turned = jnp.where(sub == r - s, face_of[r], turned)
            column_of = jnp.where(sub == r - s, pairs[r, 5], column_of)
        for h in range(2):
            m, n = 4 * h + lane // 32, k_of // 2
            index_out[h * pair_rows + s : h * pair_rows + s + ROWS, :] = (
                jnp.where(turned == 2, EDGE * n + m, EDGE * m + n) + HALF * column_of
            )

    drain(tops, rt_sem, peers - 1)
    by = jnp.broadcast_to(
        0.125 * (0.2 / jnp.max(tops[...], axis=0, keepdims=True)), (ROWS, LANES)
    )
    step_out[...] = by

    for c in range(3):
        curl_c[c] = cb[c] - by[:1, :1] * curl_c[c]
    twice = 2.0 * by
    tiles = largest_step(fine_count * SPAN // ROWS, 36)

    def finish_fine(n, carry):
        for u in range(tiles):
            rows = pl.ds(pl.multiple_of((n * tiles + u) * ROWS, ROWS), ROWS)
            curl_f[rows, :] = fb[rows, :] - twice * curl_f[rows, :]
        return carry

    lax.fori_loop(0, fine_count * SPAN // ROWS // tiles, finish_fine, 0)
    for n in range(0, 2 * pair_rows, ROWS):
        far = slice(2 * pair_rows + n, 2 * pair_rows + n + ROWS)
        fine_face[n : n + ROWS, :] = picked[n : n + ROWS, :] - twice * picked[far, :]
    slot(recv2, me)[...] = slot(send2, me)[...]
    drain(recv2, r2_sem, (peers - 1) * 2 * CAP)
    for r in range(pair_count):
        row = owner_of[r] * ROWS + rank_of[r]
        own_a[r : r + 1, :] = recv2[pl.ds(row, 1), :]
        own_b[r : r + 1, :] = recv2[pl.ds(row + CAP, 1), :]
    drain(fb, sent_sem, (peers - 1) * (2 * CAP + 1) + groups - 1)
    if relay:

        @pl.when(me == 0)
        def _():
            drain(fb, s1_sem, 3 * CAP + (peers - 2) * ROWS)

        @pl.when(me == 1)
        def _():
            drain(fb, s1_sem, (2 * peers - 3) * 3 * CAP)

        @pl.when(me > 1)
        def _():
            drain(fb, s1_sem, (peers - 1) * 3 * CAP)

    else:
        drain(fb, s1_sem, (peers - 1) * 3 * CAP)


def store(new_c, new_f, fine_face, own_a, own_b, index, step, out_c, out_f, out_j, new_j, sems):
    copies = [
        pltpu.make_async_copy(src, dst, sems.at[n])
        for n, (src, dst) in enumerate(((new_c, out_c), (new_f, out_f)))
    ]
    for copy in copies:
        copy.start()
    count, pair_rows = out_j.shape[0], own_a.shape[0]
    for s in range(0, count, ROWS):
        coarse = own_b[s : s + ROWS, :] - step[...] * own_a[s : s + ROWS, :]
        for h in range(2):
            here = slice(h * pair_rows + s, h * pair_rows + s + ROWS)
            new_j[s : s + ROWS, h * LANES : (h + 1) * LANES] = fine_face[here, :] - take(
                coarse, index[here, :]
            )
    copies.append(pltpu.make_async_copy(new_j.at[pl.ds(0, count)], out_j, sems.at[2]))
    copies[-1].start()
    for copy in copies:
        copy.wait()


def on_device(peers, groups, coarse_field, coarse_velocity, fine_field, fine_velocity, pairs):
    coarse_count, fine_count = coarse_field.shape[1], fine_field.shape[1]
    pair_count = pairs.shape[1]
    cells = EDGE**3
    flat_rows = fine_count * SPAN

    def coarse_view(x):
        return jnp.transpose(x[0], (1, 0, 2))

    def fine_view(x):
        return x.reshape(flat_rows, LANES)

    pair_rows = ROWS * -(-pair_count // ROWS)
    operands = [
        pltpu.with_memory_space_constraint(x, pltpu.HBM)
        for x in (
            pairs[0],
            coarse_view(coarse_field),
            coarse_view(coarse_velocity),
            fine_view(fine_field),
            fine_view(fine_velocity),
        )
    ]
    f32 = jnp.float32
    dma = pltpu.SemaphoreType.DMA
    vmem = pltpu.VMEM
    anywhere = pl.BlockSpec(memory_space=pltpu.HBM)
    inside = pl.BlockSpec(memory_space=pltpu.VMEM)
    coarse_shape, fine_shape = (3, coarse_count, cells), (flat_rows, LANES)
    shapes = (
        coarse_shape,
        fine_shape,
        (2 * pair_rows, LANES),
        (pair_rows, LANES),
        (pair_rows, LANES),
        (2 * pair_rows, LANES),
        (ROWS, LANES),
    )
    kinds = [f32] * 5 + [jnp.int32, f32]
    results = pl.pallas_call(
        functools.partial(kernel, peers, groups, coarse_count, fine_count, pair_count),
        out_shape=tuple(jax.ShapeDtypeStruct(s, k) for s, k in zip(shapes, kinds)),
        in_specs=[anywhere] * 5,
        out_specs=(inside,) * len(shapes),
        scratch_shapes=[
            pltpu.SMEM(pairs.shape[1:], jnp.int32),
            vmem(coarse_shape, f32),
            vmem(coarse_shape, f32),
            vmem(fine_shape, f32),
            vmem(fine_shape, f32),
            vmem(coarse_shape, f32),
            vmem((pair_count * SPAN, LANES), f32),
            vmem((6 * EDGE * coarse_count, LANES), f32),
            vmem((2 * EDGE * coarse_count, LANES), f32),
            vmem((12 * coarse_count, LANES), f32),
            vmem((6 * coarse_count, LANES), f32),
            vmem((6 * coarse_count, LANES), f32),
            vmem((12 * coarse_count, LANES), f32),
            vmem((4 * pair_rows, LANES), f32),
            vmem((peers, LANES), f32),
            vmem((4 * pair_rows, LANES), f32),
            vmem((peers * ROWS, LANES), f32),
            vmem((peers * ROWS, LANES), f32),
            vmem((peers * ROWS, LANES), f32),
            vmem((peers * ROWS, LANES), f32),
            vmem((peers * ROWS, LANES), f32),
            vmem((1, LANES), f32),
            vmem((groups, LANES), f32),
            dma((5,)),
            dma,
            dma,
            dma,
            pltpu.SemaphoreType.REGULAR,
            dma((2,)),
            dma,
            dma,
            dma,
        ],
        compiler_params=pltpu.CompilerParams(
            collective_id=0, has_side_effects=True, vmem_limit_bytes=32 * 1024 * 1024
        ),
    )(*operands)
    coarse_out, fine_out, jump = pl.pallas_call(
        store,
        out_shape=(
            jax.ShapeDtypeStruct(coarse_shape, f32),
            jax.ShapeDtypeStruct(fine_shape, f32),
            jax.ShapeDtypeStruct((pair_count, EDGE * EDGE), f32),
        ),
        in_specs=[inside] * len(shapes),
        out_specs=(anywhere,) * 3,
        scratch_shapes=[
            vmem((pair_rows, EDGE * EDGE), f32),
            dma((3,)),
        ],
    )(*(pltpu.with_memory_space_constraint(x, pltpu.VMEM) for x in results))
    return (
        jnp.transpose(coarse_out, (1, 0, 2))[None],
        fine_out.reshape(1, fine_count, 3, cells),
        jump[None],
    )


def solution(mesh):
    spec = P("gz", "blocks", None, None)
    flat = P("gz", "blocks", None)
    return jax.shard_map(
        functools.partial(on_device, mesh.shape["blocks"], mesh.shape["gz"]),
        mesh=mesh,
        in_specs=(spec, spec, spec, spec, flat),
        out_specs=(spec, spec, flat),
        check_vma=False,
    )
```

```python
import functools

import jax
import jax.numpy as jnp
from jax import lax
from jax.experimental import pallas as pl
from jax.experimental.pallas import tpu as pltpu
from jax.sharding import PartitionSpec as P

EDGE = 16
HALF = 8
CAP = 2
LANES = 128
ROWS = 8
TILES = EDGE**3 // LANES
SPAN = 3 * TILES
TINY = 1.2e-38
BIG = 1e30
EMPTY = 3e38
TANGENT = ((1, 2), (0, 2), (0, 1))
MESH = pl.DeviceIdType.MESH
TOP_CHUNK = 4
CHUNK = 4
CHUNKS = EDGE // CHUNK
FINE_STEP = 4
SPEED_STEP = 6


def take(values, index):
    return jnp.take_along_axis(values, index, axis=1, mode="promise_in_bounds")


def largest_step(count, most):
    return max(n for n in range(1, most + 1) if count % n == 0)


def kernel(
    peers,
    groups,
    coarse_count,
    fine_count,
    pair_count,
    pairs_hbm,
    cb_hbm,
    cv_hbm,
    fb_hbm,
    fv_hbm,
    curl_c,
    curl_f,
    fine_face,
    own_a,
    own_b,
    index_out,
    step_out,
    pairs,
    cb,
    cv,
    fb,
    fv,
    emf_c,
    emf_p,
    centred,
    halfway,
    plane_e,
    plane_b,
    plane_n,
    held_ref,
    picked,
    tops,
    rows1,
    send1,
    recv1,
    relayed,
    send2,
    recv2,
    gmax,
    gmax_in,
    load_sem,
    sent_sem,
    s1_sem,
    bundle_sem,
    go_sem,
    r1_sem,
    r2_sem,
    rg_sem,
    rt_sem,
):
    me = lax.axis_index("blocks")
    mg = lax.axis_index("gz")
    few = peers <= 8
    coarse_groups = coarse_count // ROWS
    pair_rows = ROWS * -(-pair_count // ROWS)

    paired = peers & (peers - 1) == 0
    flips = []
    for n in range(peers.bit_length() - 1):
        bit = 1 << n
        flips.append((bit, bit * (1 - 2 * lax.rem(lax.div(me, bit), 2))))

    def target(k):
        if not paired:
            return lax.rem(me + k, peers)
        return sum((lax.rem(lax.div(k, bit), 2) * flip for bit, flip in flips), me)

    def source(k):
        return target(k) if paired else lax.rem(me + peers - k, peers)

    def each_step(first, last, body, carry=0):
        if few:
            for k in range(last - 1, first - 1, -1):
                carry = body(k, carry)
            return carry
        return lax.fori_loop(0, last - first, lambda n, c: body(last - 1 - n, c), carry)

    def each_peer(body):
        each_step(1, peers, lambda k, _: (body(target(k)), 0)[1])

    def each_group(body):
        for k in range(1, groups):
            body(lax.rem(mg + k, groups))

    barrier = pltpu.get_barrier_semaphore()
    relay = paired and few and peers > 2
    early = peers // 2 if relay else 0
    greeted = peers - 1 + groups - 1

    def greet(p):
        at = jnp.where(jnp.logical_and(p == 0, me > 1), 1, p) if relay else p
        pl.semaphore_signal(barrier, inc=1, device_id=(at, mg), device_id_type=MESH)

    each_peer(greet)
    loads = [
        pltpu.make_async_copy(src, dst, load_sem.at[n])
        for n, (src, dst) in enumerate(((fb_hbm, fb), (fv_hbm, fv), (cb_hbm, cb), (cv_hbm, cv)))
    ]
    listed = pltpu.make_async_copy(pairs_hbm, pairs, load_sem.at[4])
    listed.start()
    for load in loads:
        load.start()
    me_or_one = jnp.where(me == 0, 1, me) if relay else me
    each_group(
        lambda g: pl.semaphore_signal(barrier, inc=1, device_id=(me_or_one, g), device_id_type=MESH)
    )

    lane = lax.broadcasted_iota(jnp.int32, (ROWS, LANES), 1)
    sub = lax.broadcasted_iota(jnp.int32, (ROWS, LANES), 0)
    zero = jnp.zeros((ROWS, LANES), jnp.float32)
    row16 = lane // EDGE
    k_of = lane % EDGE
    k8 = lane % HALF
    first_y = lane < EDGE
    last_y = lane >= LANES - EDGE
    first_z = k_of == 0
    last_z = k_of == EDGE - 1
    first_x = sub == 0
    last_x = sub == ROWS - 1

    def roll(v, shift):
        return v if shift % LANES == 0 else pltpu.roll(v, shift % LANES, 1)

    def back_y(pair):
        low, high = roll(pair[0], EDGE), roll(pair[1], EDGE)
        return jnp.where(first_y, high, low), jnp.where(first_y, low, high)

    def ahead_y(pair):
        low, high = roll(pair[0], -EDGE), roll(pair[1], -EDGE)
        return jnp.where(last_y, high, low), jnp.where(last_y, low, high)

    def back_z(pair):
        return tuple(jnp.where(first_z, roll(v, 1 - EDGE), roll(v, 1)) for v in pair)

    def ahead_z(pair):
        return tuple(jnp.where(last_z, roll(v, EDGE - 1), roll(v, -1)) for v in pair)

    def add(a, b):
        return tuple(x + y for x, y in zip(a, b))

    def sub2(a, b):
        return tuple(x - y for x, y in zip(a, b))

    def mul(a, b):
        return tuple(x * y for x, y in zip(a, b))

    def quad(f):
        return lambda q: f(q[:2]) + f(q[2:])

    def back_x(q):
        r = [pltpu.roll(v, 1, 0) for v in q]
        return tuple(jnp.where(first_x, r[n ^ 2], r[n]) for n in range(4))

    def ahead_x(q):
        r = [pltpu.roll(v, ROWS - 1, 0) for v in q]
        return tuple(jnp.where(last_x, r[n ^ 2], r[n]) for n in range(4))

    def top_of(v, c):
        out = []
        for n in range(len(v[0])):
            vv = (v[0][n] * v[0][n] + v[1][n] * v[1][n]) + v[2][n] * v[2][n]
            cc = (c[0][n] * c[0][n] + c[1][n] * c[1][n]) + c[2][n] * c[2][n]
            root_v = vv * lax.rsqrt(jnp.maximum(vv, TINY))
            root_c = cc * lax.rsqrt(jnp.maximum(cc, TINY))
            out.append(root_v + 0.5 * root_c)
        return functools.reduce(jnp.maximum, out)

    def cells(v, c):
        return (
            sub2(mul(v[2], c[1]), mul(v[1], c[2])),
            sub2(mul(v[0], c[2]), mul(v[2], c[0])),
            sub2(mul(v[1], c[0]), mul(v[0], c[1])),
        )

    def fine_read(ref, base):
        return tuple(
            tuple(
                ref[pl.ds(base + c * TILES + 2 * HALF * ih + h, ROWS, stride=2), :]
                for ih in range(2)
                for h in range(2)
            )
            for c in range(3)
        )

    def fine_put(ref, base, values):
        for c in range(3):
            for ih in range(2):
                for h in range(2):
                    ref[pl.ds(base + c * TILES + 2 * HALF * ih + h, ROWS, stride=2), :] = values[c][
                        2 * ih + h
                    ]

    def fine_centre(b):
        return (add(b[0], ahead_x(b[0])), add(b[1], quad(ahead_y)(b[1])), add(b[2], quad(ahead_z)(b[2])))

    def fine_edges(b, v):
        cell = cells(v, fine_centre(b))
        part_x = add(cell[0], quad(back_y)(cell[0]))
        part_y = add(cell[1], quad(back_z)(cell[1]))
        part_z = add(cell[2], quad(back_y)(cell[2]))
        return (
            add(part_x, quad(back_z)(part_x)),
            add(part_y, back_x(part_y)),
            add(part_z, back_x(part_z)),
        )

    def fine_curl(e):
        return (
            sub2(sub2(quad(ahead_y)(e[2]), e[2]), sub2(quad(ahead_z)(e[1]), e[1])),
            sub2(sub2(quad(ahead_z)(e[0]), e[0]), sub2(ahead_x(e[2]), e[2])),
            sub2(sub2(ahead_x(e[1]), e[1]), sub2(quad(ahead_y)(e[0]), e[0])),
        )

    def by_axis(d, values):
        return jnp.where(d == 0, values[0], jnp.where(d == 1, values[1], values[2]))

    def sum_rows(v):
        return jnp.sum(v, axis=0, keepdims=True)

    def column(tile):
        return pl.ds(pl.multiple_of(tile * LANES, LANES), LANES)

    def blocked(ref, g):
        def read(c, i):
            return tuple(ref[c, ROWS * g : ROWS * g + ROWS, column(2 * i + h)] for h in range(2))

        return read

    def blocked_put(ref, g):
        def put(c, i, pair):
            for h in range(2):
                ref[c, ROWS * g : ROWS * g + ROWS, column(2 * i + h)] = pair[h]

        return put

    loads[0].wait()
    loads[1].wait()

    speed_step = largest_step(fine_count, SPEED_STEP)

    def fine_top(n, best):
        for u in range(speed_step):
            base = (n * speed_step + u) * SPAN
            b, v = fine_read(fb, base), fine_read(fv, base)
            best = jnp.maximum(best, top_of(v, fine_centre(b)))
        return best

    best = lax.fori_loop(0, fine_count // speed_step, fine_top, zero)

    loads[2].wait()
    loads[3].wait()


    def at(n, i, g, h):
        row = (((n * coarse_groups + g) * EDGE + i) * 2 + h) * ROWS
        return pl.ds(row if isinstance(row, int) else pl.multiple_of(row, ROWS), ROWS)

    def each_plane(chunk, planes, body):
        for u in range(planes):
            for g in range(coarse_groups):
                body(chunk * planes + u, g)

    def coarse_top(n, best):
        tops = []

        def plane(i, g):
            field = blocked(cb, g)
            b = [field(c, i) for c in range(3)]
            c = (
                add(b[0], field(0, lax.rem(i + 1, EDGE))),
                add(b[1], ahead_y(b[1])),
                add(b[2], ahead_z(b[2])),
            )
            for k in range(3):
                for h in range(2):
                    centred[at(k, i, g, h), :] = c[k][h]
            tops.append(top_of([blocked(cv, g)(k, i) for k in range(3)], c))

        each_plane(n, TOP_CHUNK, plane)
        return functools.reduce(jnp.maximum, tops, best)

    best = lax.fori_loop(0, EDGE // TOP_CHUNK, coarse_top, best)
    gmax[...] = jnp.max(best, axis=0, keepdims=True)

    def slot(ref, p):
        return ref.at[pl.ds(pl.multiple_of(p * ROWS, ROWS), ROWS)]

    def part(ref, p, rows):
        return ref.at[pl.ds(pl.multiple_of(p * ROWS, ROWS), rows)]

    def out1(k):
        p = target(k)
        return pltpu.make_async_remote_copy(
            src_ref=part(send1, p, 3 * CAP), dst_ref=part(recv1, me, 3 * CAP), send_sem=s1_sem,
            recv_sem=r1_sem.at[k // (peers - 1)], device_id=(p, mg), device_id_type=MESH,
        )

    def out2(p):
        return pltpu.make_async_remote_copy(
            src_ref=part(send2, p, 2 * CAP), dst_ref=part(recv2, me, 2 * CAP), send_sem=sent_sem,
            recv_sem=r2_sem, device_id=(p, mg), device_id_type=MESH,
        )

    def outg(g):
        return pltpu.make_async_remote_copy(
            src_ref=gmax, dst_ref=gmax_in.at[pl.ds(mg, 1)], send_sem=sent_sem,
            recv_sem=rg_sem, device_id=(me, g), device_id_type=MESH,
        )

    def outt(p):
        return pltpu.make_async_remote_copy(
            src_ref=tops.at[pl.ds(me, 1)], dst_ref=tops.at[pl.ds(me, 1)], send_sem=sent_sem,
            recv_sem=rt_sem, device_id=(p, mg), device_id_type=MESH,
        )

    def drain(ref, sem, rows):
        whole = ref.at[pl.ds(0, rows)]
        pltpu.make_async_copy(whole, whole, sem).wait()

    def hand_over(p):
        return pltpu.make_async_remote_copy(
            src_ref=part(send1, p, 3 * CAP), dst_ref=part(relayed, p, 3 * CAP), send_sem=s1_sem,
            recv_sem=bundle_sem.at[min(peers - 1 - p, 2)], device_id=(1, mg), device_id_type=MESH,
        )

    def out_relay(p):
        return pltpu.make_async_remote_copy(
            src_ref=part(relayed, p, 3 * CAP), dst_ref=part(recv1, 0, 3 * CAP), send_sem=s1_sem,
            recv_sem=r1_sem.at[p // (peers - 1)], device_id=(p, mg), device_id_type=MESH,
        )

    def send_all():
        each_step(1, peers, lambda k, _: (out1(k).start(), 0)[1])

    def send_group():
        each_group(lambda g: outg(g).start())


    @pl.when(me >= early)
    def _():
        pl.semaphore_wait(barrier, greeted)
        send_group()

    listed.wait()

    half_lane = 32 * (row16 % 4)
    index_r = (half_lane + 2 * k8, 2 * k8, half_lane)
    target_r = (jnp.zeros_like(lane), row16, k8)

    def pair_edges(r):
        base = pairs[r, 0] * SPAN
        fine_put(emf_p, r * SPAN, fine_edges(fine_read(fb, base), fine_read(fv, base)))

    def pair_restrict(r):
        d = pairs[r, 1]
        index, target = by_axis(d, index_r), by_axis(d, target_r)
        upper = lane >= jnp.where(d == 1, LANES, 64)
        for which in range(2):
            axis = jnp.where(d == 0, 1, 0) if which == 0 else jnp.where(d == 2, 1, 2)
            base = r * SPAN + axis * TILES
            got = []
            for h in range(2):
                here = emf_p[pl.ds(base + h, ROWS, stride=4), :]
                if which == 0:
                    there = jnp.where(
                        d == 0, roll(here, -EDGE), emf_p[pl.ds(base + h + 2, ROWS, stride=4), :]
                    )
                else:
                    there = jnp.where(d == 2, roll(here, -EDGE), roll(here, -1))
                got.append(take(0.5 * (here + there), index))
            value = jnp.where(upper, got[1], got[0])
            rows1[pl.ds(4 * r + which, 1), :] = sum_rows(jnp.where(sub == target, value, 0.0))
        code = (pairs[r, 3] * 6 + d * 2 + pairs[r, 4]).astype(jnp.float32)
        key = jnp.where((lane[:1] // HALF) % 2 == pairs[r, 5], code, -1.0)
        rows1[pl.ds(4 * r + 2, 1), :] = key

    def each_pair(body):
        if pair_count <= 4:
            for r in range(pair_count):
                body(r)
        else:
            lax.fori_loop(0, pair_count, lambda r, _: (body(r), 0)[1], 0)

    each_pair(pair_edges)
    each_pair(pair_restrict)

    slot_of = [pairs[r, 0] for r in range(pair_count)]
    face_of = [pairs[r, 1] for r in range(pair_count)]
    owner_of = [pairs[r, 2] for r in range(pair_count)]
    rank_of = []
    for r in range(pair_count):
        rank = jnp.int32(0)
        for q in range(r):
            rank = rank + jnp.where(owner_of[q] == owner_of[r], 1, 0)
        rank_of.append(rank)

    def build(p, carry):
        message = jnp.full((ROWS, LANES), -1.0, jnp.float32)
        for r in range(pair_count):
            here = jnp.where(owner_of[r] == p, rank_of[r], ROWS)
            for n, row in enumerate((2 * here, 2 * here + 1, 2 * CAP + here)):
                message = jnp.where(
                    sub == row, jnp.broadcast_to(rows1[4 * r + n : 4 * r + n + 1, :], (ROWS, LANES)), message
                )
        slot(send1, p)[...] = message
        return carry

    lax.fori_loop(0, peers, build, 0, unroll=few)

    if relay:

        @pl.when(me == 0)
        def _():
            pl.semaphore_wait(barrier, 1)
            for p in range(peers - 1, 1, -1):
                hand_over(p).start()
            out1(1).start()

        @pl.when(me == 1)
        def _():
            pl.semaphore_wait(barrier, greeted + groups - 1 + peers - 2)
            pl.semaphore_signal(go_sem, inc=1, device_id=(0, mg), device_id_type=MESH)
            for p in range(peers - 1, 1, -1):
                n = peers - 1 - p
                if n < 2:
                    drain(relayed, bundle_sem.at[n], 3 * CAP)
                elif n == 2:
                    drain(relayed, bundle_sem.at[2], (p - 1) * 3 * CAP)
                out_relay(p).start()
                out1(p ^ 1).start()
            out1(1).start()

        @pl.when(jnp.logical_and(me > 1, me < early))
        def _():
            pl.semaphore_wait(barrier, greeted)

        @pl.when(me > 1)
        def _():
            send_all()


        @pl.when(me == 0)
        def _():
            pl.semaphore_wait(go_sem, 1)

        @pl.when(me < early)
        def _():
            send_group()

    else:
        send_all()


    def coarse_step(t, parts):
        parts = list(parts)

        def last(i, g):
            part_x = tuple(halfway[at(0, i, g, h), :] for h in range(2))
            blocked_put(emf_c, g)(0, i, add(part_x, back_z(part_x)))

        def first(i, g):
            put = blocked_put(emf_c, g)
            c = [tuple(centred[at(n, i, g, h), :] for h in range(2)) for n in range(3)]
            cell = cells([blocked(cv, g)(n, i) for n in range(3)], c)
            part_x = add(cell[0], back_y(cell[0]))
            part_y = add(cell[1], back_z(cell[1]))
            part_z = add(cell[2], back_y(cell[2]))
            for h in range(2):
                halfway[at(0, i, g, h), :] = part_x[h]
            put(1, i, add(part_y, parts[g][0]))
            put(2, i, add(part_z, parts[g][1]))
            parts[g] = (part_y, part_z)

        each_plane(lax.rem(t + CHUNKS - 1, CHUNKS), CHUNK, last)
        each_plane(lax.rem(t, CHUNKS), CHUNK, first)
        return tuple(parts)

    nothing = ((zero, zero), (zero, zero))
    lax.fori_loop(0, CHUNKS + 1, coarse_step, (nothing,) * coarse_groups)


    def packed(read, c, d, q1):
        if d == 0:
            return read(c, 0)[q1]
        out = zero
        for m in range(HALF):
            tiles = read(c, q1 * HALF + m)
            if d == 1:
                out = jnp.where(row16 == m, roll(tiles[0], EDGE * m), out)
            else:
                for q2 in range(2):
                    out = jnp.where(k_of == HALF * q2 + m, roll(tiles[q2], HALF * q2 + m), out)
        return out

    def plane_slot(n, g):
        at = (n * coarse_groups + g) * ROWS
        return slice(at, at + ROWS)

    for g in range(coarse_groups):
        for d in range(3):
            for q1 in range(2):
                plane_b[plane_slot(2 * d + q1, g), :] = packed(blocked(cb, g), d, d, q1)
                for which in range(2):
                    plane_e[plane_slot(4 * d + 2 * which + q1, g), :] = packed(
                        blocked(emf_c, g), TANGENT[d][which], d, q1
                    )

    fine_step = largest_step(fine_count, FINE_STEP)

    def fine_bulk(n, carry):
        for u in range(fine_step):
            base = (n * fine_step + u) * SPAN
            fine_put(curl_f, base, fine_curl(fine_edges(fine_read(fb, base), fine_read(fv, base))))
        return carry

    def fine_all():
        lax.fori_loop(0, fine_count // fine_step, fine_bulk, 0)

    @pl.when(me < early)
    def _():
        fine_all()

    def row_of(ref, n):
        return jnp.broadcast_to(ref[pl.ds(n, 1), :], (ROWS, LANES))

    base_code = [((sub + ROWS * g) * 6).astype(jnp.float32) for g in range(coarse_groups)]
    empty = jnp.full((ROWS, LANES), EMPTY, jnp.float32)

    def collect(p, held):
        held = list(held)
        for c in range(CAP):
            key = row_of(recv1, p * ROWS + 2 * CAP + c)
            values = [row_of(recv1, p * ROWS + 2 * c + which) for which in range(2)]
            for g in range(coarse_groups):
                code = key - base_code[g]
                held[g] = tuple(
                    jnp.where(code == float(2 * (n // 4) + n % 2), values[n // 2 % 2], held[g][n])
                    for n in range(12)
                )
        return tuple(held)

    drain(gmax_in, rg_sem, groups - 1)
    best = gmax[...]
    for k in range(1, groups):
        best = jnp.maximum(best, gmax_in[pl.ds(lax.rem(mg + k, groups), 1), :])
    tops[pl.ds(me, 1), :] = jnp.broadcast_to(jnp.max(best, axis=1, keepdims=True), (1, LANES))
    each_peer(lambda p: outt(p).start())
    slot(recv1, me)[...] = slot(send1, me)[...]
    drain(recv1, r1_sem.at[0], (peers - 2) * 3 * CAP)
    held = collect(me, ((empty,) * 12,) * coarse_groups)
    held = each_step(1, peers - 1, lambda k, held: collect(source(k), held), held)
    for g in range(coarse_groups):
        for n in range(12):
            held_ref[plane_slot(n, g), :] = held[g][n]
    drain(recv1, r1_sem.at[1], 3 * CAP)
    held = tuple(
        tuple(held_ref[plane_slot(n, g), :] for n in range(12)) for g in range(coarse_groups)
    )
    held = collect(source(jnp.int32(peers - 1)), held)
    spread = row16
    squeeze = EDGE * k8
    upper8 = k_of >= HALF

    def known(v):
        return v < BIG

    def chosen(v, other):
        return jnp.where(known(v), v, other)

    for g in range(coarse_groups):
        for n in range(12):
            held_ref[plane_slot(n, g), :] = held[g][n]
        sent = [[[held[g][4 * d + 2 * w + q] for q in range(2)] for w in range(2)] for d in range(3)]
        base = [
            [
                [chosen(sent[d][w][q], plane_e[plane_slot(4 * d + 2 * w + q, g), :]) for q in range(2)]
                for w in range(2)
            ]
            for d in range(3)
        ]
        now = [[list(base[d][w]) for w in range(2)] for d in range(3)]
        ahead = [[[None] * 2 for w in range(2)] for d in range(3)]
        for q in range(2):
            over = roll(sent[2][1][0], -HALF * q)
            now[0][0][q] = jnp.where(first_z, chosen(over, base[0][0][q]), base[0][0][q])
            wrap = chosen(roll(sent[2][1][0], EDGE - 1 - HALF * q), roll(base[0][0][q], EDGE - 1))
            ahead[0][0][q] = jnp.where(last_z, wrap, roll(base[0][0][q], -1))

            over = take(sent[2][0][q], spread)
            now[1][0][q] = jnp.where(first_z, chosen(over, base[1][0][q]), base[1][0][q])
            wrap = chosen(over, roll(base[1][0][q], EDGE - 1))
            ahead[1][0][q] = jnp.where(last_z, wrap, roll(base[1][0][q], -1))

            under = take(sent[1][0][q], squeeze)
            free = known(under) & (sent[2][0][q] >= BIG) & (lane < HALF)
            now[2][0][q] = jnp.where(free, under, base[2][0][q])
            free = known(under) & (roll(sent[2][0][q], LANES - HALF) >= BIG)
            wrap = jnp.where(free, under, roll(base[2][0][q], LANES - HALF))
            wrap = jnp.where(upper8, wrap, roll(base[2][0][q], LANES - EDGE - HALF))
            ahead[2][0][q] = jnp.where(last_y, wrap, roll(base[2][0][q], -EDGE))

        over, under = sent[1][1][0], sent[0][1][0]
        now[0][1][0] = jnp.where(first_y, chosen(over, base[0][1][0]), base[0][1][0])
        free = known(under) & (over >= BIG) & first_y
        now[1][1][0] = jnp.where(free, under, base[1][1][0])
        over, under = roll(over, -EDGE), roll(under, -EDGE)
        turned = [[roll(base[d][1][q], -EDGE) for q in range(2)] for d in range(2)]
        wrap = (chosen(over, turned[0][0]), jnp.where(known(under) & (over >= BIG), under, turned[1][0]))
        for d in range(2):
            ahead[d][1] = [
                jnp.where(last_y, turned[d][1], turned[d][0]),
                jnp.where(last_y, wrap[d], turned[d][1]),
            ]

        under = jnp.where(upper8, roll(sent[0][0][1], HALF), sent[0][0][0])
        free = known(under) & (sent[2][1][0] >= BIG) & (k8 == 0)
        now[2][1][0] = jnp.where(free, under, base[2][1][0])
        under = jnp.where(upper8, roll(sent[0][0][1], EDGE - 1), roll(sent[0][0][0], HALF - 1))
        free = known(under) & (roll(sent[2][1][0], HALF - 1) >= BIG)
        turned = [roll(base[2][1][q], HALF - 1) for q in range(2)]
        wrap = (turned[1], jnp.where(free, under, turned[0]))
        for q in range(2):
            ahead[2][1][q] = jnp.where(k8 == HALF - 1, wrap[q], roll(base[2][1][q], -1))

        for d in range(3):
            left, right = sub2(ahead[d][1], now[d][1]), sub2(ahead[d][0], now[d][0])
            curl = sub2(right, left) if d == 1 else sub2(left, right)
            for q in range(2):
                plane_n[plane_slot(2 * d + q, g), :] = curl[q]


    def answer(p):
        rows = zero
        for c in range(CAP):
            key = row_of(recv1, p * ROWS + 2 * CAP + c)
            curl_acc, field_acc = zero, zero
            for g in range(coarse_groups):
                code = key - base_code[g]
                for n in range(6):
                    hit = code == float(n)
                    curl_acc = jnp.where(hit, plane_n[plane_slot(n, g), :], curl_acc)
                    field_acc = jnp.where(hit, plane_b[plane_slot(n, g), :], field_acc)
            rows = jnp.where(sub == c, sum_rows(curl_acc), rows)
            rows = jnp.where(sub == CAP + c, sum_rows(field_acc), rows)
        slot(send2, p)[...] = rows

    def reply(k, carry):
        answer(target(k))
        out2(target(k)).start()
        return carry

    each_step(1, peers, reply)
    answer(me)
    for g in range(coarse_groups):
        for d in range(3):
            for which in range(2):
                axis = TANGENT[d][which]
                for q1 in range(2):
                    value = held_ref[plane_slot(4 * d + 2 * which + q1, g), :]

                    def patch(tile, shift, mask, value=value, axis=axis, g=g):
                        where = (axis, slice(ROWS * g, ROWS * g + ROWS), slice(tile * LANES, tile * LANES + LANES))
                        turned = roll(value, shift)
                        put = turned < BIG
                        if mask is not None:
                            put = put & mask
                        emf_c[where] = jnp.where(put, turned, emf_c[where])

                    if d == 0:
                        patch(q1, 0, None)
                        continue
                    for m in range(HALF):
                        tile = 2 * (q1 * HALF + m)
                        if d == 1:
                            patch(tile, -EDGE * m, first_y)
                        else:
                            for q2 in range(2):
                                patch(tile + q2, -(HALF * q2 + m), first_z)


    def curl_step(n, carry):
        for u in range(4):
            i = 4 * n + u
            after = lax.rem(i + 1, EDGE)
            for g in range(coarse_groups):
                read, put = blocked(emf_c, g), blocked_put(curl_c, g)
                e_x, e_y, e_z = read(0, i), read(1, i), read(2, i)
                put(0, i, sub2(sub2(ahead_y(e_z), e_z), sub2(ahead_z(e_y), e_y)))
                put(1, i, sub2(sub2(ahead_z(e_x), e_x), sub2(read(2, after), e_z)))
                put(2, i, sub2(sub2(read(1, after), e_y), sub2(ahead_y(e_x), e_x)))
        return carry

    lax.fori_loop(0, EDGE // 4, curl_step, 0)


    @pl.when(me >= early)
    def _():
        fine_all()

    index_n = (lane, k_of, EDGE * k8)
    target_n = (jnp.zeros_like(lane), row16, row16)

    def pair_normal(r):
        d = pairs[r, 1]
        base = pairs[r, 0] * SPAN + d * TILES
        index, target = by_axis(d, index_n), by_axis(d, target_n)
        upper = k_of >= jnp.where(d == 2, HALF, EDGE)
        for n, ref in enumerate((fb, curl_f)):
            for h in range(2):
                start = base + jnp.where(d == 0, h, 2 * HALF * h)
                got = [take(ref[pl.ds(start + s, ROWS, stride=2), :], index) for s in range(2)]
                value = jnp.where(upper, got[1], got[0])
                picked[pl.ds((2 * n + h) * pair_rows + r, 1), :] = sum_rows(
                    jnp.where(sub == target, value, 0.0)
                )

    each_pair(pair_normal)

    for s in range(0, pair_count, ROWS):
        turned, column_of = jnp.zeros_like(lane), jnp.zeros_like(lane)
        for r in range(s, min(s + ROWS, pair_count)):
            turned = jnp.where(sub == r - s, face_of[r], turned)
            column_of = jnp.where(sub == r - s, pairs[r, 5], column_of)
        for h in range(2):
            m, n = 4 * h + lane // 32, k_of // 2
            index_out[h * pair_rows + s : h * pair_rows + s + ROWS, :] = (
                jnp.where(turned == 2, EDGE * n + m, EDGE * m + n) + HALF * column_of
            )

    drain(tops, rt_sem, peers - 1)
    by = jnp.broadcast_to(
        0.125 * (0.2 / jnp.max(tops[...], axis=0, keepdims=True)), (ROWS, LANES)
    )
    step_out[...] = by

    for c in range(3):
        curl_c[c] = cb[c] - by[:1, :1] * curl_c[c]
    twice = 2.0 * by
    tiles = largest_step(fine_count * SPAN // ROWS, 36)

    def finish_fine(n, carry):
        for u in range(tiles):
            rows = pl.ds(pl.multiple_of((n * tiles + u) * ROWS, ROWS), ROWS)
            curl_f[rows, :] = fb[rows, :] - twice * curl_f[rows, :]
        return carry

    lax.fori_loop(0, fine_count * SPAN // ROWS // tiles, finish_fine, 0)
    for n in range(0, 2 * pair_rows, ROWS):
        far = slice(2 * pair_rows + n, 2 * pair_rows + n + ROWS)
        fine_face[n : n + ROWS, :] = picked[n : n + ROWS, :] - twice * picked[far, :]
    slot(recv2, me)[...] = slot(send2, me)[...]
    drain(recv2, r2_sem, (peers - 1) * 2 * CAP)
    for r in range(pair_count):
        row = owner_of[r] * ROWS + rank_of[r]
        own_a[r : r + 1, :] = recv2[pl.ds(row, 1), :]
        own_b[r : r + 1, :] = recv2[pl.ds(row + CAP, 1), :]
    drain(fb, sent_sem, (peers - 1) * (2 * CAP + 1) + groups - 1)
    if relay:

        @pl.when(me == 1)
        def _():
            drain(fb, s1_sem, (2 * peers - 3) * 3 * CAP)

        @pl.when(me != 1)
        def _():
            drain(fb, s1_sem, (peers - 1) * 3 * CAP)

    else:
        drain(fb, s1_sem, (peers - 1) * 3 * CAP)


def store(new_c, new_f, fine_face, own_a, own_b, index, step, out_c, out_f, out_j, new_j, sems):
    copies = [
        pltpu.make_async_copy(src, dst, sems.at[n])
        for n, (src, dst) in enumerate(((new_c, out_c), (new_f, out_f)))
    ]
    for copy in copies:
        copy.start()
    count, pair_rows = out_j.shape[0], own_a.shape[0]
    for s in range(0, count, ROWS):
        coarse = own_b[s : s + ROWS, :] - step[...] * own_a[s : s + ROWS, :]
        for h in range(2):
            here = slice(h * pair_rows + s, h * pair_rows + s + ROWS)
            new_j[s : s + ROWS, h * LANES : (h + 1) * LANES] = fine_face[here, :] - take(
                coarse, index[here, :]
            )
    copies.append(pltpu.make_async_copy(new_j.at[pl.ds(0, count)], out_j, sems.at[2]))
    copies[-1].start()
    for copy in copies:
        copy.wait()


def on_device(peers, groups, coarse_field, coarse_velocity, fine_field, fine_velocity, pairs):
    coarse_count, fine_count = coarse_field.shape[1], fine_field.shape[1]
    pair_count = pairs.shape[1]
    cells = EDGE**3
    flat_rows = fine_count * SPAN

    def coarse_view(x):
        return jnp.transpose(x[0], (1, 0, 2))

    def fine_view(x):
        return x.reshape(flat_rows, LANES)

    pair_rows = ROWS * -(-pair_count // ROWS)
    operands = [
        pltpu.with_memory_space_constraint(x, pltpu.HBM)
        for x in (
            pairs[0],
            coarse_view(coarse_field),
            coarse_view(coarse_velocity),
            fine_view(fine_field),
            fine_view(fine_velocity),
        )
    ]
    f32 = jnp.float32
    dma = pltpu.SemaphoreType.DMA
    vmem = pltpu.VMEM
    anywhere = pl.BlockSpec(memory_space=pltpu.HBM)
    inside = pl.BlockSpec(memory_space=pltpu.VMEM)
    coarse_shape, fine_shape = (3, coarse_count, cells), (flat_rows, LANES)
    shapes = (
        coarse_shape,
        fine_shape,
        (2 * pair_rows, LANES),
        (pair_rows, LANES),
        (pair_rows, LANES),
        (2 * pair_rows, LANES),
        (ROWS, LANES),
    )
    kinds = [f32] * 5 + [jnp.int32, f32]
    results = pl.pallas_call(
        functools.partial(kernel, peers, groups, coarse_count, fine_count, pair_count),
        out_shape=tuple(jax.ShapeDtypeStruct(s, k) for s, k in zip(shapes, kinds)),
        in_specs=[anywhere] * 5,
        out_specs=(inside,) * len(shapes),
        scratch_shapes=[
            pltpu.SMEM(pairs.shape[1:], jnp.int32),
            vmem(coarse_shape, f32),
            vmem(coarse_shape, f32),
            vmem(fine_shape, f32),
            vmem(fine_shape, f32),
            vmem(coarse_shape, f32),
            vmem((pair_count * SPAN, LANES), f32),
            vmem((6 * EDGE * coarse_count, LANES), f32),
            vmem((2 * EDGE * coarse_count, LANES), f32),
            vmem((12 * coarse_count, LANES), f32),
            vmem((6 * coarse_count, LANES), f32),
            vmem((6 * coarse_count, LANES), f32),
            vmem((12 * coarse_count, LANES), f32),
            vmem((4 * pair_rows, LANES), f32),
            vmem((peers, LANES), f32),
            vmem((4 * pair_rows, LANES), f32),
            vmem((peers * ROWS, LANES), f32),
            vmem((peers * ROWS, LANES), f32),
            vmem((peers * ROWS, LANES), f32),
            vmem((peers * ROWS, LANES), f32),
            vmem((peers * ROWS, LANES), f32),
            vmem((1, LANES), f32),
            vmem((groups, LANES), f32),
            dma((5,)),
            dma,
            dma,
            dma((3,)),
            pltpu.SemaphoreType.REGULAR,
            dma((2,)),
            dma,
            dma,
            dma,
        ],
        compiler_params=pltpu.CompilerParams(
            collective_id=0, has_side_effects=True, vmem_limit_bytes=32 * 1024 * 1024
        ),
    )(*operands)
    coarse_out, fine_out, jump = pl.pallas_call(
        store,
        out_shape=(
            jax.ShapeDtypeStruct(coarse_shape, f32),
            jax.ShapeDtypeStruct(fine_shape, f32),
            jax.ShapeDtypeStruct((pair_count, EDGE * EDGE), f32),
        ),
        in_specs=[inside] * len(shapes),
        out_specs=(anywhere,) * 3,
        scratch_shapes=[
            vmem((pair_rows, EDGE * EDGE), f32),
            dma((3,)),
        ],
    )(*(pltpu.with_memory_space_constraint(x, pltpu.VMEM) for x in results))
    return (
        jnp.transpose(coarse_out, (1, 0, 2))[None],
        fine_out.reshape(1, fine_count, 3, cells),
        jump[None],
    )


def solution(mesh):
    spec = P("gz", "blocks", None, None)
    flat = P("gz", "blocks", None)
    return jax.shard_map(
        functools.partial(on_device, mesh.shape["blocks"], mesh.shape["gz"]),
        mesh=mesh,
        in_specs=(spec, spec, spec, spec, flat),
        out_specs=(spec, spec, flat),
        check_vma=False,
    )
```

```python
import functools

import jax
import jax.numpy as jnp
from jax import lax
from jax.experimental import pallas as pl
from jax.experimental.pallas import tpu as pltpu
from jax.sharding import PartitionSpec as P

EDGE = 16
HALF = 8
CAP = 2
LANES = 128
ROWS = 8
TILES = EDGE**3 // LANES
SPAN = 3 * TILES
TINY = 1.2e-38
BIG = 1e30
EMPTY = 3e38
TANGENT = ((1, 2), (0, 2), (0, 1))
MESH = pl.DeviceIdType.MESH
TOP_CHUNK = 8
CHUNK = 4
CHUNKS = EDGE // CHUNK
FINE_STEP = 4
SPEED_STEP = 6


def take(values, index):
    return jnp.take_along_axis(values, index, axis=1, mode="promise_in_bounds")


def largest_step(count, most):
    return max(n for n in range(1, most + 1) if count % n == 0)


def kernel(
    peers,
    groups,
    coarse_count,
    fine_count,
    pair_count,
    pairs_hbm,
    cb_hbm,
    cv_hbm,
    fb_hbm,
    fv_hbm,
    cb,
    curl_c,
    fb,
    curl_f,
    fine_face,
    own_a,
    own_b,
    index_out,
    step_out,
    pairs,
    cv,
    fv,
    emf_c,
    emf_p,
    centred,
    halfway,
    plane_e,
    plane_b,
    plane_n,
    held_ref,
    picked,
    tops,
    rows1,
    send1,
    recv1,
    relayed,
    send2,
    recv2,
    gmax,
    gmax_in,
    sent_sem,
    bundle_sem,
    go_sem,
    r1_sem,
    r2_sem,
    rg_sem,
    rt_sem,
):
    me = lax.axis_index("blocks")
    mg = lax.axis_index("gz")
    few = peers <= 8
    coarse_groups = coarse_count // ROWS
    pair_rows = ROWS * -(-pair_count // ROWS)

    paired = peers & (peers - 1) == 0
    flips = []
    for n in range(peers.bit_length() - 1):
        bit = 1 << n
        flips.append((bit, bit * (1 - 2 * lax.rem(lax.div(me, bit), 2))))

    def target(k):
        if not paired:
            return lax.rem(me + k, peers)
        return sum((lax.rem(lax.div(k, bit), 2) * flip for bit, flip in flips), me)

    def source(k):
        return target(k) if paired else lax.rem(me + peers - k, peers)

    def each_step(first, last, body, carry=0):
        if few:
            for k in range(last - 1, first - 1, -1):
                carry = body(k, carry)
            return carry
        return lax.fori_loop(0, last - first, lambda n, c: body(last - 1 - n, c), carry)

    def each_peer(body):
        each_step(1, peers, lambda k, _: (body(target(k)), 0)[1])

    def each_group(body):
        for k in range(1, groups):
            body(lax.rem(mg + k, groups))

    barrier = pltpu.get_barrier_semaphore()
    relay = paired and few and peers > 2
    near = max(peers - 3, 1)
    early = peers // 2 if relay else 0
    greeted = peers - 1 + groups - 1

    def greet(p):
        at = jnp.where(jnp.logical_and(p == 0, me > 1), 1, p) if relay else p
        pl.semaphore_signal(barrier, inc=1, device_id=(at, mg), device_id_type=MESH)

    each_peer(greet)
    lane = lax.broadcasted_iota(jnp.int32, (ROWS, LANES), 1)
    sub = lax.broadcasted_iota(jnp.int32, (ROWS, LANES), 0)
    zero = jnp.zeros((ROWS, LANES), jnp.float32)
    row16 = lane // EDGE
    k_of = lane % EDGE
    k8 = lane % HALF
    first_y = lane < EDGE
    last_y = lane >= LANES - EDGE
    first_z = k_of == 0
    last_z = k_of == EDGE - 1
    first_x = sub == 0
    last_x = sub == ROWS - 1

    def roll(v, shift):
        return v if shift % LANES == 0 else pltpu.roll(v, shift % LANES, 1)

    def back_y(pair):
        low, high = roll(pair[0], EDGE), roll(pair[1], EDGE)
        return jnp.where(first_y, high, low), jnp.where(first_y, low, high)

    def ahead_y(pair):
        low, high = roll(pair[0], -EDGE), roll(pair[1], -EDGE)
        return jnp.where(last_y, high, low), jnp.where(last_y, low, high)

    def back_z(pair):
        return tuple(jnp.where(first_z, roll(v, 1 - EDGE), roll(v, 1)) for v in pair)

    def ahead_z(pair):
        return tuple(jnp.where(last_z, roll(v, EDGE - 1), roll(v, -1)) for v in pair)

    def add(a, b):
        return tuple(x + y for x, y in zip(a, b))

    def sub2(a, b):
        return tuple(x - y for x, y in zip(a, b))

    def mul(a, b):
        return tuple(x * y for x, y in zip(a, b))

    def quad(f):
        return lambda q: f(q[:2]) + f(q[2:])

    def back_x(q):
        r = [pltpu.roll(v, 1, 0) for v in q]
        return tuple(jnp.where(first_x, r[n ^ 2], r[n]) for n in range(4))

    def ahead_x(q):
        r = [pltpu.roll(v, ROWS - 1, 0) for v in q]
        return tuple(jnp.where(last_x, r[n ^ 2], r[n]) for n in range(4))

    def top_of(v, c):
        out = []
        for n in range(len(v[0])):
            vv = (v[0][n] * v[0][n] + v[1][n] * v[1][n]) + v[2][n] * v[2][n]
            cc = (c[0][n] * c[0][n] + c[1][n] * c[1][n]) + c[2][n] * c[2][n]
            root_v = vv * lax.rsqrt(jnp.maximum(vv, TINY))
            root_c = cc * lax.rsqrt(jnp.maximum(cc, TINY))
            out.append(root_v + 0.5 * root_c)
        return functools.reduce(jnp.maximum, out)

    def cells(v, c):
        return (
            sub2(mul(v[2], c[1]), mul(v[1], c[2])),
            sub2(mul(v[0], c[2]), mul(v[2], c[0])),
            sub2(mul(v[1], c[0]), mul(v[0], c[1])),
        )

    def fine_read(ref, base):
        return tuple(
            tuple(
                ref[pl.ds(base + c * TILES + 2 * HALF * ih + h, ROWS, stride=2), :]
                for ih in range(2)
                for h in range(2)
            )
            for c in range(3)
        )

    def fine_put(ref, base, values):
        for c in range(3):
            for ih in range(2):
                for h in range(2):
                    ref[pl.ds(base + c * TILES + 2 * HALF * ih + h, ROWS, stride=2), :] = values[c][
                        2 * ih + h
                    ]

    def fine_centre(b):
        return (add(b[0], ahead_x(b[0])), add(b[1], quad(ahead_y)(b[1])), add(b[2], quad(ahead_z)(b[2])))

    def fine_edges(b, v):
        cell = cells(v, fine_centre(b))
        part_x = add(cell[0], quad(back_y)(cell[0]))
        part_y = add(cell[1], quad(back_z)(cell[1]))
        part_z = add(cell[2], quad(back_y)(cell[2]))
        return (
            add(part_x, quad(back_z)(part_x)),
            add(part_y, back_x(part_y)),
            add(part_z, back_x(part_z)),
        )

    def fine_curl(e):
        return (
            sub2(sub2(quad(ahead_y)(e[2]), e[2]), sub2(quad(ahead_z)(e[1]), e[1])),
            sub2(sub2(quad(ahead_z)(e[0]), e[0]), sub2(ahead_x(e[2]), e[2])),
            sub2(sub2(ahead_x(e[1]), e[1]), sub2(quad(ahead_y)(e[0]), e[0])),
        )

    def by_axis(d, values):
        return jnp.where(d == 0, values[0], jnp.where(d == 1, values[1], values[2]))

    def sum_rows(v):
        return jnp.sum(v, axis=0, keepdims=True)

    def column(tile):
        return pl.ds(pl.multiple_of(tile * LANES, LANES), LANES)

    def blocked(ref, g):
        def read(c, i):
            return tuple(ref[c, ROWS * g : ROWS * g + ROWS, column(2 * i + h)] for h in range(2))

        return read

    def blocked_put(ref, g):
        def put(c, i, pair):
            for h in range(2):
                ref[c, ROWS * g : ROWS * g + ROWS, column(2 * i + h)] = pair[h]

        return put

    speed_step = largest_step(fine_count, SPEED_STEP)
    fine_parts = fine_count // speed_step
    def at(n, i, g, h):
        row = (((n * coarse_groups + g) * EDGE + i) * 2 + h) * ROWS
        return pl.ds(row if isinstance(row, int) else pl.multiple_of(row, ROWS), ROWS)

    def each_plane(chunk, planes, body):
        for u in range(planes):
            for g in range(coarse_groups):
                body(chunk * planes + u, g)

    def front(load_sem):
        loads = []

        def load(src, dst):
            loads.append(pltpu.make_async_copy(src, dst, load_sem.at[1 + len(loads)]))

        for n in range(fine_parts):
            rows = pl.ds(n * speed_step * SPAN, speed_step * SPAN)
            load(fb_hbm.at[rows], fb.at[rows])
            load(fv_hbm.at[rows], fv.at[rows])
        for g in range(coarse_groups):
            rows = pl.ds(g * ROWS, ROWS)
            load(cb_hbm.at[:, rows], cb.at[:, rows])
            load(cv_hbm.at[:, rows], cv.at[:, rows])
        listed = pltpu.make_async_copy(pairs_hbm, pairs, load_sem.at[0])
        listed.start()
        for copy in loads:
            copy.start()
        me_or_one = jnp.where(me == 0, 1, me) if relay else me
        each_group(
            lambda g: pl.semaphore_signal(barrier, inc=1, device_id=(me_or_one, g), device_id_type=MESH)
        )

        best = zero
        for n in range(fine_parts):
            loads[2 * n].wait()
            loads[2 * n + 1].wait()
            for u in range(speed_step):
                base = (n * speed_step + u) * SPAN
                best = jnp.maximum(best, top_of(fine_read(fv, base), fine_centre(fine_read(fb, base))))


        def coarse_top(n, best, g):
            tops = []
            for u in range(TOP_CHUNK):
                i = n * TOP_CHUNK + u
                field = blocked(cb, g)
                b = [field(c, i) for c in range(3)]
                c = (
                    add(b[0], field(0, lax.rem(i + 1, EDGE))),
                    add(b[1], ahead_y(b[1])),
                    add(b[2], ahead_z(b[2])),
                )
                for k in range(3):
                    for h in range(2):
                        centred[at(k, i, g, h), :] = c[k][h]
                tops.append(top_of([blocked(cv, g)(k, i) for k in range(3)], c))
            return functools.reduce(jnp.maximum, tops, best)

        for g in range(coarse_groups):
            loads[2 * fine_parts + 2 * g].wait()
            loads[2 * fine_parts + 2 * g + 1].wait()
            best = lax.fori_loop(0, EDGE // TOP_CHUNK, functools.partial(coarse_top, g=g), best)
        gmax[...] = jnp.max(best, axis=0, keepdims=True)
        listed.wait()


    pl.run_scoped(front, pltpu.SemaphoreType.DMA((1 + 2 * (fine_parts + coarse_groups),)))

    def slot(ref, p):
        return ref.at[pl.ds(pl.multiple_of(p * ROWS, ROWS), ROWS)]

    def part(ref, p, rows):
        return ref.at[pl.ds(pl.multiple_of(p * ROWS, ROWS), rows)]

    def out1(k):
        p = target(k)
        return pltpu.make_async_remote_copy(
            src_ref=part(send1, p, 3 * CAP), dst_ref=part(recv1, me, 3 * CAP), send_sem=sent_sem,
            recv_sem=r1_sem.at[k // (near + 1)], device_id=(p, mg), device_id_type=MESH,
        )

    def out2(p):
        return pltpu.make_async_remote_copy(
            src_ref=part(send2, p, 2 * CAP), dst_ref=part(recv2, me, 2 * CAP), send_sem=sent_sem,
            recv_sem=r2_sem, device_id=(p, mg), device_id_type=MESH,
        )

    def outg(g):
        return pltpu.make_async_remote_copy(
            src_ref=gmax, dst_ref=gmax_in.at[pl.ds(mg, 1)], send_sem=sent_sem,
            recv_sem=rg_sem, device_id=(me, g), device_id_type=MESH,
        )

    def outt(p):
        return pltpu.make_async_remote_copy(
            src_ref=tops.at[pl.ds(me, 1)], dst_ref=tops.at[pl.ds(me, 1)], send_sem=sent_sem,
            recv_sem=rt_sem, device_id=(p, mg), device_id_type=MESH,
        )

    def drain(ref, sem, rows):
        whole = ref.at[pl.ds(0, rows)]
        pltpu.make_async_copy(whole, whole, sem).wait()

    def hand_over(p):
        return pltpu.make_async_remote_copy(
            src_ref=part(send1, p, 3 * CAP), dst_ref=part(relayed, p, 3 * CAP), send_sem=sent_sem,
            recv_sem=bundle_sem.at[min(peers - 1 - p, 2)], device_id=(1, mg), device_id_type=MESH,
        )

    def out_relay(p):
        return pltpu.make_async_remote_copy(
            src_ref=part(relayed, p, 3 * CAP), dst_ref=part(recv1, 0, 3 * CAP), send_sem=sent_sem,
            recv_sem=r1_sem.at[p // (near + 1)], device_id=(p, mg), device_id_type=MESH,
        )

    def send_all():
        each_step(1, peers, lambda k, _: (out1(k).start(), 0)[1])

    def send_group():
        each_group(lambda g: outg(g).start())


    @pl.when(me >= early)
    def _():
        pl.semaphore_wait(barrier, greeted)
        send_group()

    half_lane = 32 * (row16 % 4)
    index_r = (half_lane + 2 * k8, 2 * k8, half_lane)
    target_r = (jnp.zeros_like(lane), row16, k8)

    def pair_edges(r):
        base = pairs[r, 0] * SPAN
        fine_put(emf_p, r * SPAN, fine_edges(fine_read(fb, base), fine_read(fv, base)))

    def pair_restrict(r):
        d = pairs[r, 1]
        index, target = by_axis(d, index_r), by_axis(d, target_r)
        upper = lane >= jnp.where(d == 1, LANES, 64)
        for which in range(2):
            axis = jnp.where(d == 0, 1, 0) if which == 0 else jnp.where(d == 2, 1, 2)
            base = r * SPAN + axis * TILES
            got = []
            for h in range(2):
                here = emf_p[pl.ds(base + h, ROWS, stride=4), :]
                if which == 0:
                    there = jnp.where(
                        d == 0, roll(here, -EDGE), emf_p[pl.ds(base + h + 2, ROWS, stride=4), :]
                    )
                else:
                    there = jnp.where(d == 2, roll(here, -EDGE), roll(here, -1))
                got.append(take(0.5 * (here + there), index))
            value = jnp.where(upper, got[1], got[0])
            rows1[pl.ds(4 * r + which, 1), :] = sum_rows(jnp.where(sub == target, value, 0.0))
        code = (pairs[r, 3] * 6 + d * 2 + pairs[r, 4]).astype(jnp.float32)
        key = jnp.where((lane[:1] // HALF) % 2 == pairs[r, 5], code, -1.0)
        rows1[pl.ds(4 * r + 2, 1), :] = key

    def each_pair(body):
        if pair_count <= 4:
            for r in range(pair_count):
                body(r)
        else:
            lax.fori_loop(0, pair_count, lambda r, _: (body(r), 0)[1], 0)

    each_pair(pair_edges)
    each_pair(pair_restrict)

    slot_of = [pairs[r, 0] for r in range(pair_count)]
    face_of = [pairs[r, 1] for r in range(pair_count)]
    owner_of = [pairs[r, 2] for r in range(pair_count)]
    rank_of = []
    for r in range(pair_count):
        rank = jnp.int32(0)
        for q in range(r):
            rank = rank + jnp.where(owner_of[q] == owner_of[r], 1, 0)
        rank_of.append(rank)

    def build(p, carry):
        message = jnp.full((ROWS, LANES), -1.0, jnp.float32)
        for r in range(pair_count):
            here = jnp.where(owner_of[r] == p, rank_of[r], ROWS)
            for n, row in enumerate((2 * here, 2 * here + 1, 2 * CAP + here)):
                message = jnp.where(
                    sub == row, jnp.broadcast_to(rows1[4 * r + n : 4 * r + n + 1, :], (ROWS, LANES)), message
                )
        slot(send1, p)[...] = message
        return carry

    lax.fori_loop(0, peers, build, 0, unroll=few)

    if relay:

        @pl.when(me == 0)
        def _():
            pl.semaphore_wait(barrier, 1)
            for p in range(peers - 1, 1, -1):
                hand_over(p).start()
            out1(1).start()

        @pl.when(me == 1)
        def _():
            pl.semaphore_wait(barrier, greeted + groups - 1 + peers - 2)
            pl.semaphore_signal(go_sem, inc=1, device_id=(0, mg), device_id_type=MESH)
            for p in range(peers - 1, 1, -1):
                n = peers - 1 - p
                if n < 2:
                    drain(relayed, bundle_sem.at[n], 3 * CAP)
                elif n == 2:
                    drain(relayed, bundle_sem.at[2], (p - 1) * 3 * CAP)
                out_relay(p).start()
                out1(p ^ 1).start()
            out1(1).start()

        @pl.when(jnp.logical_and(me > 1, me < early))
        def _():
            pl.semaphore_wait(barrier, greeted)

        @pl.when(me > 1)
        def _():
            send_all()


        @pl.when(me == 0)
        def _():
            pl.semaphore_wait(go_sem, 1)

        @pl.when(me < early)
        def _():
            send_group()

    else:
        send_all()


    def coarse_step(t, parts):
        parts = list(parts)

        def last(i, g):
            part_x = tuple(halfway[at(0, i, g, h), :] for h in range(2))
            blocked_put(emf_c, g)(0, i, add(part_x, back_z(part_x)))

        def first(i, g):
            put = blocked_put(emf_c, g)
            c = [tuple(centred[at(n, i, g, h), :] for h in range(2)) for n in range(3)]
            cell = cells([blocked(cv, g)(n, i) for n in range(3)], c)
            part_x = add(cell[0], back_y(cell[0]))
            part_y = add(cell[1], back_z(cell[1]))
            part_z = add(cell[2], back_y(cell[2]))
            for h in range(2):
                halfway[at(0, i, g, h), :] = part_x[h]
            put(1, i, add(part_y, parts[g][0]))
            put(2, i, add(part_z, parts[g][1]))
            parts[g] = (part_y, part_z)

        each_plane(lax.rem(t + CHUNKS - 1, CHUNKS), CHUNK, last)
        each_plane(lax.rem(t, CHUNKS), CHUNK, first)
        return tuple(parts)

    nothing = ((zero, zero), (zero, zero))
    lax.fori_loop(0, CHUNKS + 1, coarse_step, (nothing,) * coarse_groups)


    def packed(read, c, d, q1):
        if d == 0:
            return read(c, 0)[q1]
        out = zero
        for m in range(HALF):
            tiles = read(c, q1 * HALF + m)
            if d == 1:
                out = jnp.where(row16 == m, roll(tiles[0], EDGE * m), out)
            else:
                for q2 in range(2):
                    out = jnp.where(k_of == HALF * q2 + m, roll(tiles[q2], HALF * q2 + m), out)
        return out

    def plane_slot(n, g):
        at = (n * coarse_groups + g) * ROWS
        return slice(at, at + ROWS)

    for g in range(coarse_groups):
        for d in range(3):
            for q1 in range(2):
                plane_b[plane_slot(2 * d + q1, g), :] = packed(blocked(cb, g), d, d, q1)
                for which in range(2):
                    plane_e[plane_slot(4 * d + 2 * which + q1, g), :] = packed(
                        blocked(emf_c, g), TANGENT[d][which], d, q1
                    )

    fine_step = largest_step(fine_count, FINE_STEP)

    def fine_bulk(n, carry):
        for u in range(fine_step):
            base = (n * fine_step + u) * SPAN
            fine_put(curl_f, base, fine_curl(fine_edges(fine_read(fb, base), fine_read(fv, base))))
        return carry

    def fine_all():
        lax.fori_loop(0, fine_count // fine_step, fine_bulk, 0)

    @pl.when(me < early)
    def _():
        fine_all()

    def row_of(ref, n):
        return jnp.broadcast_to(ref[pl.ds(n, 1), :], (ROWS, LANES))

    base_code = [((sub + ROWS * g) * 6).astype(jnp.float32) for g in range(coarse_groups)]
    empty = jnp.full((ROWS, LANES), EMPTY, jnp.float32)

    def collect(p, held):
        held = list(held)
        for c in range(CAP):
            key = row_of(recv1, p * ROWS + 2 * CAP + c)
            values = [row_of(recv1, p * ROWS + 2 * c + which) for which in range(2)]
            for g in range(coarse_groups):
                code = key - base_code[g]
                held[g] = tuple(
                    jnp.where(code == float(2 * (n // 4) + n % 2), values[n // 2 % 2], held[g][n])
                    for n in range(12)
                )
        return tuple(held)

    drain(gmax_in, rg_sem, groups - 1)
    best = gmax[...]
    for k in range(1, groups):
        best = jnp.maximum(best, gmax_in[pl.ds(lax.rem(mg + k, groups), 1), :])
    tops[pl.ds(me, 1), :] = jnp.broadcast_to(jnp.max(best, axis=1, keepdims=True), (1, LANES))
    each_peer(lambda p: outt(p).start())
    slot(recv1, me)[...] = slot(send1, me)[...]
    drain(recv1, r1_sem.at[0], near * 3 * CAP)
    held = collect(me, ((empty,) * 12,) * coarse_groups)
    held = each_step(1, near + 1, lambda k, held: collect(source(k), held), held)
    for g in range(coarse_groups):
        for n in range(12):
            held_ref[plane_slot(n, g), :] = held[g][n]
    drain(recv1, r1_sem.at[1], (peers - 1 - near) * 3 * CAP)
    held = tuple(
        tuple(held_ref[plane_slot(n, g), :] for n in range(12)) for g in range(coarse_groups)
    )
    held = each_step(near + 1, peers, lambda k, held: collect(source(k), held), held)
    spread = row16
    squeeze = EDGE * k8
    upper8 = k_of >= HALF

    def known(v):
        return v < BIG

    def chosen(v, other):
        return jnp.where(known(v), v, other)

    for g in range(coarse_groups):
        for n in range(12):
            held_ref[plane_slot(n, g), :] = held[g][n]
        sent = [[[held[g][4 * d + 2 * w + q] for q in range(2)] for w in range(2)] for d in range(3)]
        base = [
            [
                [chosen(sent[d][w][q], plane_e[plane_slot(4 * d + 2 * w + q, g), :]) for q in range(2)]
                for w in range(2)
            ]
            for d in range(3)
        ]
        now = [[list(base[d][w]) for w in range(2)] for d in range(3)]
        ahead = [[[None] * 2 for w in range(2)] for d in range(3)]
        for q in range(2):
            over = roll(sent[2][1][0], -HALF * q)
            now[0][0][q] = jnp.where(first_z, chosen(over, base[0][0][q]), base[0][0][q])
            wrap = chosen(roll(sent[2][1][0], EDGE - 1 - HALF * q), roll(base[0][0][q], EDGE - 1))
            ahead[0][0][q] = jnp.where(last_z, wrap, roll(base[0][0][q], -1))

            over = take(sent[2][0][q], spread)
            now[1][0][q] = jnp.where(first_z, chosen(over, base[1][0][q]), base[1][0][q])
            wrap = chosen(over, roll(base[1][0][q], EDGE - 1))
            ahead[1][0][q] = jnp.where(last_z, wrap, roll(base[1][0][q], -1))

            under = take(sent[1][0][q], squeeze)
            free = known(under) & (sent[2][0][q] >= BIG) & (lane < HALF)
            now[2][0][q] = jnp.where(free, under, base[2][0][q])
            free = known(under) & (roll(sent[2][0][q], LANES - HALF) >= BIG)
            wrap = jnp.where(free, under, roll(base[2][0][q], LANES - HALF))
            wrap = jnp.where(upper8, wrap, roll(base[2][0][q], LANES - EDGE - HALF))
            ahead[2][0][q] = jnp.where(last_y, wrap, roll(base[2][0][q], -EDGE))

        over, under = sent[1][1][0], sent[0][1][0]
        now[0][1][0] = jnp.where(first_y, chosen(over, base[0][1][0]), base[0][1][0])
        free = known(under) & (over >= BIG) & first_y
        now[1][1][0] = jnp.where(free, under, base[1][1][0])
        over, under = roll(over, -EDGE), roll(under, -EDGE)
        turned = [[roll(base[d][1][q], -EDGE) for q in range(2)] for d in range(2)]
        wrap = (chosen(over, turned[0][0]), jnp.where(known(under) & (over >= BIG), under, turned[1][0]))
        for d in range(2):
            ahead[d][1] = [
                jnp.where(last_y, turned[d][1], turned[d][0]),
                jnp.where(last_y, wrap[d], turned[d][1]),
            ]

        under = jnp.where(upper8, roll(sent[0][0][1], HALF), sent[0][0][0])
        free = known(under) & (sent[2][1][0] >= BIG) & (k8 == 0)
        now[2][1][0] = jnp.where(free, under, base[2][1][0])
        under = jnp.where(upper8, roll(sent[0][0][1], EDGE - 1), roll(sent[0][0][0], HALF - 1))
        free = known(under) & (roll(sent[2][1][0], HALF - 1) >= BIG)
        turned = [roll(base[2][1][q], HALF - 1) for q in range(2)]
        wrap = (turned[1], jnp.where(free, under, turned[0]))
        for q in range(2):
            ahead[2][1][q] = jnp.where(k8 == HALF - 1, wrap[q], roll(base[2][1][q], -1))

        for d in range(3):
            left, right = sub2(ahead[d][1], now[d][1]), sub2(ahead[d][0], now[d][0])
            curl = sub2(right, left) if d == 1 else sub2(left, right)
            for q in range(2):
                plane_n[plane_slot(2 * d + q, g), :] = curl[q]


    def answer(p):
        rows = zero
        for c in range(CAP):
            key = row_of(recv1, p * ROWS + 2 * CAP + c)
            curl_acc, field_acc = zero, zero
            for g in range(coarse_groups):
                code = key - base_code[g]
                for n in range(6):
                    hit = code == float(n)
                    curl_acc = jnp.where(hit, plane_n[plane_slot(n, g), :], curl_acc)
                    field_acc = jnp.where(hit, plane_b[plane_slot(n, g), :], field_acc)
            rows = jnp.where(sub == c, sum_rows(curl_acc), rows)
            rows = jnp.where(sub == CAP + c, sum_rows(field_acc), rows)
        slot(send2, p)[...] = rows

    def reply(k, carry):
        answer(target(k))
        out2(target(k)).start()
        return carry

    each_step(1, peers, reply)
    answer(me)
    for g in range(coarse_groups):
        for d in range(3):
            for which in range(2):
                axis = TANGENT[d][which]
                for q1 in range(2):
                    value = held_ref[plane_slot(4 * d + 2 * which + q1, g), :]

                    def patch(tile, shift, mask, value=value, axis=axis, g=g):
                        where = (axis, slice(ROWS * g, ROWS * g + ROWS), slice(tile * LANES, tile * LANES + LANES))
                        turned = roll(value, shift)
                        put = turned < BIG
                        if mask is not None:
                            put = put & mask
                        emf_c[where] = jnp.where(put, turned, emf_c[where])

                    if d == 0:
                        patch(q1, 0, None)
                        continue
                    for m in range(HALF):
                        tile = 2 * (q1 * HALF + m)
                        if d == 1:
                            patch(tile, -EDGE * m, first_y)
                        else:
                            for q2 in range(2):
                                patch(tile + q2, -(HALF * q2 + m), first_z)


    def curl_step(n, carry):
        for u in range(4):
            i = 4 * n + u
            after = lax.rem(i + 1, EDGE)
            for g in range(coarse_groups):
                read, put = blocked(emf_c, g), blocked_put(curl_c, g)
                e_x, e_y, e_z = read(0, i), read(1, i), read(2, i)
                put(0, i, sub2(sub2(ahead_y(e_z), e_z), sub2(ahead_z(e_y), e_y)))
                put(1, i, sub2(sub2(ahead_z(e_x), e_x), sub2(read(2, after), e_z)))
                put(2, i, sub2(sub2(read(1, after), e_y), sub2(ahead_y(e_x), e_x)))
        return carry

    lax.fori_loop(0, EDGE // 4, curl_step, 0)


    @pl.when(me >= early)
    def _():
        fine_all()

    index_n = (lane, k_of, EDGE * k8)
    target_n = (jnp.zeros_like(lane), row16, row16)

    def pair_normal(r):
        d = pairs[r, 1]
        base = pairs[r, 0] * SPAN + d * TILES
        index, target = by_axis(d, index_n), by_axis(d, target_n)
        upper = k_of >= jnp.where(d == 2, HALF, EDGE)
        for n, ref in enumerate((fb, curl_f)):
            for h in range(2):
                start = base + jnp.where(d == 0, h, 2 * HALF * h)
                got = [take(ref[pl.ds(start + s, ROWS, stride=2), :], index) for s in range(2)]
                value = jnp.where(upper, got[1], got[0])
                picked[pl.ds((2 * n + h) * pair_rows + r, 1), :] = sum_rows(
                    jnp.where(sub == target, value, 0.0)
                )

    each_pair(pair_normal)

    for s in range(0, pair_count, ROWS):
        turned, column_of = jnp.zeros_like(lane), jnp.zeros_like(lane)
        for r in range(s, min(s + ROWS, pair_count)):
            turned = jnp.where(sub == r - s, face_of[r], turned)
            column_of = jnp.where(sub == r - s, pairs[r, 5], column_of)
        for h in range(2):
            m, n = 4 * h + lane // 32, k_of // 2
            index_out[h * pair_rows + s : h * pair_rows + s + ROWS, :] = (
                jnp.where(turned == 2, EDGE * n + m, EDGE * m + n) + HALF * column_of
            )

    drain(tops, rt_sem, peers - 1)
    by = jnp.broadcast_to(
        0.125 * (0.2 / jnp.max(tops[...], axis=0, keepdims=True)), (ROWS, LANES)
    )
    step_out[...] = by

    curl_c[0] = cb[0] - by[:1, :1] * curl_c[0]
    twice = 2.0 * by
    for n in range(0, 2 * pair_rows, ROWS):
        far = slice(2 * pair_rows + n, 2 * pair_rows + n + ROWS)
        fine_face[n : n + ROWS, :] = picked[n : n + ROWS, :] - twice * picked[far, :]
    slot(recv2, me)[...] = slot(send2, me)[...]
    drain(recv2, r2_sem, (peers - 1) * 2 * CAP)
    for r in range(pair_count):
        row = owner_of[r] * ROWS + rank_of[r]
        own_a[r : r + 1, :] = recv2[pl.ds(row, 1), :]
        own_b[r : r + 1, :] = recv2[pl.ds(row + CAP, 1), :]
    other = (peers - 1) * (2 * CAP + 1) + groups - 1
    if relay:

        @pl.when(me == 1)
        def _():
            drain(fb, sent_sem, other + (2 * peers - 3) * 3 * CAP)

        @pl.when(me != 1)
        def _():
            drain(fb, sent_sem, other + (peers - 1) * 3 * CAP)

    else:
        drain(fb, sent_sem, other + (peers - 1) * 3 * CAP)


def store(
    cb, curl_c, fb, curl_f, fine_face, own_a, own_b, index, step, out_c, out_f, out_j, new_c, new_f, new_j, sems
):
    by = step[0:1, 0:1]
    copies = []

    def send(src, dst):
        copies.append(pltpu.make_async_copy(src, dst, sems.at[len(copies)]))
        copies[-1].start()

    send(curl_c.at[0], out_c.at[0])
    for c in range(1, 3):
        new_c[c - 1] = cb[c] - by * curl_c[c]
        send(new_c.at[c - 1], out_c.at[c])
    new_f[...] = fb[...] - (2.0 * by) * curl_f[...]
    send(new_f, out_f)
    count, pair_rows = out_j.shape[0], own_a.shape[0]
    for s in range(0, count, ROWS):
        coarse = own_b[s : s + ROWS, :] - step[...] * own_a[s : s + ROWS, :]
        for h in range(2):
            here = slice(h * pair_rows + s, h * pair_rows + s + ROWS)
            new_j[s : s + ROWS, h * LANES : (h + 1) * LANES] = fine_face[here, :] - take(
                coarse, index[here, :]
            )
    send(new_j.at[pl.ds(0, count)], out_j)
    for copy in copies:
        copy.wait()


def on_device(peers, groups, coarse_field, coarse_velocity, fine_field, fine_velocity, pairs):
    coarse_count, fine_count = coarse_field.shape[1], fine_field.shape[1]
    pair_count = pairs.shape[1]
    cells = EDGE**3
    flat_rows = fine_count * SPAN

    def coarse_view(x):
        return jnp.transpose(x[0], (1, 0, 2))

    def fine_view(x):
        return x.reshape(flat_rows, LANES)

    pair_rows = ROWS * -(-pair_count // ROWS)
    operands = [
        pltpu.with_memory_space_constraint(x, pltpu.HBM)
        for x in (
            pairs[0],
            coarse_view(coarse_field),
            coarse_view(coarse_velocity),
            fine_view(fine_field),
            fine_view(fine_velocity),
        )
    ]
    f32 = jnp.float32
    dma = pltpu.SemaphoreType.DMA
    vmem = pltpu.VMEM
    anywhere = pl.BlockSpec(memory_space=pltpu.HBM)
    inside = pl.BlockSpec(memory_space=pltpu.VMEM)
    coarse_shape, fine_shape = (3, coarse_count, cells), (flat_rows, LANES)
    shapes = (
        coarse_shape,
        coarse_shape,
        fine_shape,
        fine_shape,
        (2 * pair_rows, LANES),
        (pair_rows, LANES),
        (pair_rows, LANES),
        (2 * pair_rows, LANES),
        (ROWS, LANES),
    )
    kinds = [f32] * 7 + [jnp.int32, f32]
    results = pl.pallas_call(
        functools.partial(kernel, peers, groups, coarse_count, fine_count, pair_count),
        out_shape=tuple(jax.ShapeDtypeStruct(s, k) for s, k in zip(shapes, kinds)),
        in_specs=[anywhere] * 5,
        out_specs=(inside,) * len(shapes),
        scratch_shapes=[
            pltpu.SMEM(pairs.shape[1:], jnp.int32),
            vmem(coarse_shape, f32),
            vmem(fine_shape, f32),
            vmem(coarse_shape, f32),
            vmem((pair_count * SPAN, LANES), f32),
            vmem((6 * EDGE * coarse_count, LANES), f32),
            vmem((2 * EDGE * coarse_count, LANES), f32),
            vmem((12 * coarse_count, LANES), f32),
            vmem((6 * coarse_count, LANES), f32),
            vmem((6 * coarse_count, LANES), f32),
            vmem((12 * coarse_count, LANES), f32),
            vmem((4 * pair_rows, LANES), f32),
            vmem((peers, LANES), f32),
            vmem((4 * pair_rows, LANES), f32),
            vmem((peers * ROWS, LANES), f32),
            vmem((peers * ROWS, LANES), f32),
            vmem((peers * ROWS, LANES), f32),
            vmem((peers * ROWS, LANES), f32),
            vmem((peers * ROWS, LANES), f32),
            vmem((1, LANES), f32),
            vmem((groups, LANES), f32),
            dma,
            dma((3,)),
            pltpu.SemaphoreType.REGULAR,
            dma((2,)),
            dma,
            dma,
            dma,
        ],
        compiler_params=pltpu.CompilerParams(
            collective_id=0, has_side_effects=True, vmem_limit_bytes=32 * 1024 * 1024
        ),
    )(*operands)
    coarse_out, fine_out, jump = pl.pallas_call(
        store,
        out_shape=(
            jax.ShapeDtypeStruct(coarse_shape, f32),
            jax.ShapeDtypeStruct(fine_shape, f32),
            jax.ShapeDtypeStruct((pair_count, EDGE * EDGE), f32),
        ),
        in_specs=[inside] * len(shapes),
        out_specs=(anywhere,) * 3,
        scratch_shapes=[
            vmem((2, coarse_count, cells), f32),
            vmem(fine_shape, f32),
            vmem((pair_rows, EDGE * EDGE), f32),
            dma((5,)),
        ],
    )(*(pltpu.with_memory_space_constraint(x, pltpu.VMEM) for x in results))
    return (
        jnp.transpose(coarse_out, (1, 0, 2))[None],
        fine_out.reshape(1, fine_count, 3, cells),
        jump[None],
    )


def solution(mesh):
    spec = P("gz", "blocks", None, None)
    flat = P("gz", "blocks", None)
    return jax.shard_map(
        functools.partial(on_device, mesh.shape["blocks"], mesh.shape["gz"]),
        mesh=mesh,
        in_specs=(spec, spec, spec, spec, flat),
        out_specs=(spec, spec, flat),
        check_vma=False,
    )
```
